512 devices in a mesh: gx: 32 (over z_hi, x, core), gy: 16 (over y, z_lo).
Axes of the slice: x: 4, y: 8, z: 8 (z_hi: 4, z_lo: 2; z = z_hi * 2 + z_lo), core: 2. Of those that a mesh axis runs over, the one named last changes fastest.
Arguments:
- populations: float32 [19, 256, 256, 128], P(None, 'gx', 'gy')
- anchor: int32 [32, 16, 1024], P('gx', 'gy'), may hold values from 0 to 20606, as said below
- offsets: float32 [32, 16, 3, 1024], P('gx', 'gy'), may hold values from 0 to 0.999
- heading: float32 [32, 16, 2, 1024], P('gx', 'gy'), may hold values from -3.140625 to 3.140625
- velocity: float32 [32, 16, 3, 1024], P('gx', 'gy'), may hold values from -0.6 to 0.6
- live_count: int32 [32, 16], P('gx', 'gy'), may hold values from 1 to 1024, as said below
Outputs:
- populations_next: float32 [19, 256, 256, 128], P(None, 'gx', 'gy')
- swimmer_force: float32 [32, 16, 3, 1024], P('gx', 'gy')
The draws below stay inside these ranges and needn't reach their ends.
Inputs may be any that keep to these rules, and one draw needn't show every extreme that they name: The anchor is (ax (18) + ay) * 128 + az with 0 <= ax <= 8, 0 <= ay <= 16, 0 <= az <= 126. Live swimmers fill slots 0 to live_count - 1 of their device; some device holds 1024.
All inputs are finite; a program needn't handle non-finite values.
Results may differ from the reference program's by a relative error of at most 0.0003.
Values sent between devices are 32-bit elements; how exact they have to be, the bound alone decides.
A program may use at most 64 MiB of HBM per device.

```python
import jax
import jax.numpy as jnp
from jax import lax

CX = 8
CY = 16
NZ = 128
SW_DEV = 1024
N_GX = 32
N_GY = 16


def draw_populations(key, part):
    weight = jnp.asarray((1.0 / 3.0,) + (1.0 / 18.0,) * 6 + (1.0 / 36.0,) * 12, jnp.float32)
    spread = jax.random.uniform(key, (19, CX * N_GX, CY * N_GY, NZ), jnp.float32)
    factor = 0.6 + 0.8 * spread
    return weight[:, None, None, None] * factor


def draw_anchor(key, part):
    first, second, third = jax.random.split(jax.random.fold_in(key, 11), 3)
    shape = (N_GX, N_GY, SW_DEV)
    cell_x = jax.random.randint(first, shape, 0, CX + 1)
    cell_y = jax.random.randint(second, shape, 0, CY + 1)
    cell_z = jax.random.randint(third, shape, 0, NZ - 1)
    return ((cell_x * (CY + 2) + cell_y) * NZ + cell_z).astype(jnp.int32)


def draw_live_count(key, part):
    first, second = jax.random.split(jax.random.fold_in(key, 23))
    lowest = max(1, SW_DEV // 8)
    counts = jax.random.randint(first, (N_GX, N_GY), lowest, SW_DEV // 2 + 1)
    chosen = jax.random.randint(second, (), 0, N_GX * N_GY)
    places = jnp.arange(N_GX * N_GY, dtype=jnp.int32).reshape(N_GX, N_GY)
    return jnp.where(places == chosen, SW_DEV, counts).astype(jnp.int32)


def shard_levels(stream_key, extent, cuts, low, top_value):
    factor_of = 1.0
    for position, shards_of in cuts:
        heights = jax.random.uniform(jax.random.fold_in(jax.random.fold_in(stream_key, 6), position), (shards_of,), jnp.float32, low / len(cuts), top_value / len(cuts))
        factor_of = factor_of * jnp.repeat(jnp.exp(heights), extent[position] // shards_of).reshape((-1,) + (1,) * (len(extent) - 1 - position))
    return factor_of


def normal_values(key, shape, scale, bound, shards=(), held_as=jnp.bfloat16):
    drawn = scale * jax.random.normal(key, shape, jnp.float32)
    if shards:
        drawn = drawn * shard_levels(key, shape, shards, -0.22, 0.18)
    return jnp.clip(drawn, -bound, bound).astype(held_as)


def setup_inputs(seed: int = 0) -> dict:
    keys = jax.random.split(jax.random.key(seed), 7)
    populations = draw_populations(jax.random.fold_in(keys[6], 71), 0)
    anchor = draw_anchor(jax.random.fold_in(keys[6], 71), 0)
    offsets = jnp.clip(0.999 * jax.random.uniform(keys[2], (N_GX, N_GY, 3, SW_DEV), jnp.float32) ** shard_levels(keys[2], (N_GX, N_GY, 3, SW_DEV), ((0, 32), (1, 16)), -0.2, 0.2), 0.0, 0.999)
    heading = jnp.clip(jax.random.uniform(keys[3], (N_GX, N_GY, 2, SW_DEV), jnp.float32, -3.140625, 3.140625), -3.140625, 3.140625)
    velocity = normal_values(keys[4], (N_GX, N_GY, 3, SW_DEV), 0.1, 0.6, ((0, 32), (1, 16)), jnp.float32)
    live_count = draw_live_count(jax.random.fold_in(keys[6], 71), 0)
    return dict(populations=populations, anchor=anchor, offsets=offsets, heading=heading, velocity=velocity, live_count=live_count)


lattice_dirs = ((0, 0, 0), (1, 0, 0), (-1, 0, 0), (0, 1, 0), (0, -1, 0), (0, 0, 1), (0, 0, -1),
                (1, 1, 0), (-1, -1, 0), (1, -1, 0), (-1, 1, 0), (1, 0, 1), (-1, 0, -1),
                (1, 0, -1), (-1, 0, 1), (0, 1, 1), (0, -1, -1), (0, 1, -1), (0, -1, 1))
lattice_weights = (1.0 / 3.0,) + (1.0 / 18.0,) * 6 + (1.0 / 36.0,) * 12
relax_time = 0.8
friction = 2.0
propulsion = 0.5
wca_energy = 0.01
floor_square = 0.8
cutoff_square = 2.0 ** (1.0 / 3.0)


def moments(fluid):
    dirs = jnp.asarray(lattice_dirs, jnp.float32)
    density = jnp.sum(fluid, axis=0)
    momentum = jnp.einsum("qc,qxyz->cxyz", dirs, fluid, precision=lax.Precision.HIGHEST)
    return density, momentum


def collide(fluid, forcing):
    dirs = jnp.asarray(lattice_dirs, jnp.float32)
    density, momentum = moments(fluid)
    speed = (momentum + 0.5 * forcing) / density
    along = jnp.einsum("qc,cxyz->qxyz", dirs, speed, precision=lax.Precision.HIGHEST)
    pushed = jnp.einsum("qc,cxyz->qxyz", dirs, forcing, precision=lax.Precision.HIGHEST)
    square = jnp.sum(speed * speed, axis=0)
    dotted = jnp.sum(speed * forcing, axis=0)
    weight = jnp.asarray(lattice_weights, jnp.float32)[:, None, None, None]
    balance = weight * density * (1.0 + 3.0 * along + 4.5 * along * along - 1.5 * square)
    source = (1.0 - 0.5 / relax_time) * weight * (3.0 * (pushed - dotted) + 9.0 * along * pushed)
    return fluid - (fluid - balance) / relax_time + source


def stencil(root, offsets, stride_x, stride_y):
    indices = []
    shares = []
    for step_x in (0, 1):
        for step_y in (0, 1):
            for step_z in (0, 1):
                part_x = offsets[..., 0, :] if step_x else 1.0 - offsets[..., 0, :]
                part_y = offsets[..., 1, :] if step_y else 1.0 - offsets[..., 1, :]
                part_z = offsets[..., 2, :] if step_z else 1.0 - offsets[..., 2, :]
                indices.append(root + step_x * stride_x + step_y * stride_y + step_z)
                shares.append(part_x * part_y * part_z)
    return indices, shares


def direction(heading):
    first = heading[..., 0, :]
    second = heading[..., 1, :]
    return jnp.stack([jnp.cos(first) * jnp.cos(second), jnp.sin(first) * jnp.cos(second), jnp.sin(second)], axis=-2)


def pair_force(own, ghosts, depth):
    delta = own[:3, :, None] - ghosts[:3, None, :]
    along_z = delta[2]
    along_z = jnp.where(along_z > 0.5 * depth, along_z - depth, jnp.where(along_z < -0.5 * depth, along_z + depth, along_z))
    delta = jnp.stack([delta[0], delta[1], along_z])
    raw = jnp.sum(delta * delta, axis=0)
    square = jnp.maximum(raw, floor_square)
    inverse = 1.0 / square
    sixth = inverse * inverse * inverse
    magnitude = 24.0 * wca_energy * (2.0 * sixth * sixth - sixth) * inverse
    keep = jnp.where(raw < cutoff_square, ghosts[3][None, :], 0.0)
    return jnp.sum(delta * (magnitude * keep)[None], axis=2)


def reference(populations, anchor, offsets, heading, velocity, live_count):
    grid_x = CX * N_GX
    grid_y = CY * N_GY
    density, momentum = moments(populations)
    speed = momentum / density
    framed = jnp.pad(speed, ((0, 0), (1, 1), (1, 1), (0, 0)), mode="wrap").reshape(3, -1)
    block_row = (CY + 2) * NZ
    cell_x = anchor // block_row
    rest = anchor % block_row
    cell_y = rest // NZ
    cell_z = rest % NZ
    dev_x = jnp.arange(N_GX, dtype=jnp.int32)[:, None, None]
    dev_y = jnp.arange(N_GY, dtype=jnp.int32)[None, :, None]
    root = ((dev_x * CX + cell_x) * (grid_y + 2) + dev_y * CY + cell_y) * NZ + cell_z
    indices, shares = stencil(root, offsets, (grid_y + 2) * NZ, NZ)
    sampled = jnp.zeros(velocity.shape, jnp.float32)
    for index, share in zip(indices, shares):
        sampled = sampled + share[:, :, None, :] * jnp.moveaxis(framed[:, index], 0, 2)
    slots = jnp.arange(SW_DEV, dtype=jnp.int32)
    live = (slots[None, None, :] < live_count[:, :, None]).astype(jnp.float32)
    drag = friction * (sampled - velocity)
    push = propulsion * direction(heading)
    reaction = -(drag + push) * live[:, :, None, :]
    spread = jnp.zeros((3, (grid_x + 2) * (grid_y + 2) * NZ), jnp.float32)
    for index, share in zip(indices, shares):
        spread = spread.at[:, index.reshape(-1)].add(jnp.moveaxis(reaction * share[:, :, None, :], 2, 0).reshape(3, -1))
    spread = spread.reshape(3, grid_x + 2, grid_y + 2, NZ)
    inner = spread[:, 1:grid_x + 1]
    inner = inner.at[:, 0].add(spread[:, grid_x + 1]).at[:, grid_x - 1].add(spread[:, 0])
    forcing = inner[:, :, 1:grid_y + 1]
    forcing = forcing.at[:, :, 0].add(inner[:, :, grid_y + 1]).at[:, :, grid_y - 1].add(inner[:, :, 0])
    post = collide(populations, forcing)
    moved = jnp.stack([jnp.roll(post[q], lattice_dirs[q], axis=(0, 1, 2)) for q in range(19)])
    place_x = cell_x.astype(jnp.float32) - 1.0 + offsets[:, :, 0]
    place_y = cell_y.astype(jnp.float32) - 1.0 + offsets[:, :, 1]
    place_z = cell_z.astype(jnp.float32) + offsets[:, :, 2]
    own = jnp.stack([place_x, place_y, place_z, live], axis=2)
    seen = []
    for step_a in (-1, 0, 1):
        for step_b in (-1, 0, 1):
            rolled = jnp.roll(own, (-step_a, -step_b), axis=(0, 1))
            moved_by = jnp.asarray([step_a * CX, step_b * CY, 0, 0], jnp.float32)[:, None]
            seen.append(rolled + moved_by)
    ghosts = jnp.concatenate(seen, axis=3)
    depth = jnp.float32(NZ)
    pairs = lax.map(lambda item: pair_force(item[0], item[1], depth),
                    (own.reshape(-1, 4, SW_DEV), ghosts.reshape(-1, 4, 9 * SW_DEV)))
    pairs = pairs.reshape(N_GX, N_GY, 3, SW_DEV)
    force = (pairs + drag + push) * live[:, :, None, :]
    return moved, force
```

```python
import functools

import jax
import jax.numpy as jnp
import numpy as np
from jax import lax
from jax.experimental import pallas as pl
from jax.experimental.pallas import tpu as pltpu
from jax.sharding import PartitionSpec as P

DIRS = (
    (0, 0, 0), (1, 0, 0), (-1, 0, 0), (0, 1, 0), (0, -1, 0), (0, 0, 1), (0, 0, -1),
    (1, 1, 0), (-1, -1, 0), (1, -1, 0), (-1, 1, 0), (1, 0, 1), (-1, 0, -1),
    (1, 0, -1), (-1, 0, 1), (0, 1, 1), (0, -1, -1), (0, 1, -1), (0, -1, 1),
)
WEIGHTS = (1.0 / 3.0,) + (1.0 / 18.0,) * 6 + (1.0 / 36.0,) * 12
CUTOFF = 2.0 ** (1.0 / 3.0)
REACH = 1.125
FAR = 1.0e9
F32 = jnp.float32
BF16 = jnp.bfloat16
MESH = pl.DeviceIdType.MESH

CX, CY, NZ, SW = 8, 16, 128, 1024
ROWS = CX * CY
LANE_TILES = SW // 128

SIDES = ((-1, 0), (1, 0), (0, -1), (0, 1), (-1, -1), (-1, 1), (1, -1), (1, 1))
RANGES = ((0, 4, 7), (1, 0, 3), (2, 2, 5), (3, 6, 8), (3, 0, 1), (4, 4, 5), (5, 6, 7), (6, 2, 3), (7, 0, 1))


def facing(axis, sign):
    return [q for q in range(19) if DIRS[q][axis] == sign]


def corner_q(sx, sy):
    return DIRS.index((-sx, -sy, 0))


def split2(v):
    hi = v.astype(BF16)
    return hi, (v - hi.astype(F32)).astype(BF16)


def split3(v):
    hi = v.astype(BF16)
    rest = v - hi.astype(F32)
    mid = rest.astype(BF16)
    return hi, mid, (rest - mid.astype(F32)).astype(BF16)


def dot(a, b):
    return lax.dot_general(a, b, (((1,), (0,)), ((), ())), preferred_element_type=F32)


def dot_t(a, b):
    return lax.dot_general(a, b, (((1,), (1,)), ((), ())), preferred_element_type=F32)


def tent(d):
    return jnp.maximum(1.0 - jnp.abs(d), 0.0)


def moments(load):
    rho = None
    mom = [None, None, None]
    for q in range(19):
        f = load(q)
        rho = f if rho is None else rho + f
        for c in range(3):
            s = DIRS[q][c]
            if s:
                if mom[c] is None:
                    mom[c] = f if s > 0 else -f
                else:
                    mom[c] = mom[c] + f if s > 0 else mom[c] - f
    return rho, mom


def pair_terms(ox, oy, oz, px, py, pz):
    dx = ox - px
    dy = oy - py
    dz = oz - pz
    dz = dz - NZ * jnp.round(dz * (1.0 / NZ))
    raw = dx * dx + dy * dy + dz * dz
    inv = 1.0 / jnp.maximum(raw, 0.8)
    sixth = inv * inv * inv
    mag = (sixth + sixth - 1.0) * (sixth * inv)
    mag = jnp.where(raw < CUTOFF, mag, 0.0)
    return mag * dx, mag * dy, mag * dz


def exchange_kernel(n_gx, n_gy, pops, anchor, offsets, heading, velocity, count,
                    halo_x, halo_y, halo_c, lists, starts_out, own_out, pair_out,
                    pv, msg_x, msg_y, msg_c, msg_l, msg_s, mom, cols, pop_sem, send_sem, recv_sem):
    gx = lax.axis_index("gx")
    gy = lax.axis_index("gy")

    def device(side):
        return (lax.rem(gx + side[0] + n_gx, n_gx), lax.rem(gy + side[1] + n_gy, n_gy))

    loads = [pltpu.make_async_copy(pops.at[q], pv.at[q], pop_sem.at[q]) for q in range(19)]
    for c in loads:
        c.start()
    barrier = pltpu.get_barrier_semaphore()
    for side in SIDES:
        pl.semaphore_signal(barrier, inc=1, device_id=device(side), device_id_type=MESH)

    root = anchor[0]
    bx = lax.shift_right_logical(root, 7)
    cz = root & (NZ - 1)
    bxf = bx.astype(F32)
    cxf = jnp.floor(bxf * (1.0 / (CY + 2)) + 0.01)
    cyf = bxf - cxf * (CY + 2)
    off = offsets[0, 0]
    x = cxf - 1.0 + off[0:1]
    y = cyf - 1.0 + off[1:2]
    z = cz.astype(F32) + off[2:3]
    slot = lax.broadcasted_iota(jnp.int32, (1, SW), 1)
    live = (slot < count[0, 0]).astype(F32)
    ang = heading[0, 0]
    cs, sn = jnp.cos(ang), jnp.sin(ang)
    vel = velocity[0, 0]
    c1 = cs[1:2]
    w = [2.0 * vel[0:1] - 0.5 * (cs[0:1] * c1),
         2.0 * vel[1:2] - 0.5 * (sn[0:1] * c1),
         2.0 * vel[2:3] - 0.5 * sn[1:2]]
    zero = jnp.zeros((1, SW), F32)
    table = jnp.concatenate([x, y, z, w[0], w[1], w[2], live, zero], axis=0)
    own_out[...] = table

    xl, xh = x < REACH, x > CX - 1 - REACH
    yl, yh = y < REACH, y > CY - 1 - REACH
    yc = jnp.where(yl, 0.0, jnp.where(yh, 2.0, 1.0))
    kind = jnp.where(xl, yc, jnp.where(xh, 6.0 - yc, jnp.where(yl, 7.0, jnp.where(yh, 3.0, 8.0))))
    kind = jnp.where(live > 0.0, kind, 9.0)
    krow = lax.broadcasted_iota(jnp.int32, (16, SW), 0).astype(F32)
    member = (krow == kind).astype(F32)
    stack = jnp.concatenate([member[:, t * 128:(t + 1) * 128] for t in range(LANE_TILES)], axis=0).astype(BF16)
    ri = lax.broadcasted_iota(jnp.int32, (128, 256), 0)
    ci = lax.broadcasted_iota(jnp.int32, (128, 256), 1)
    upper = ((ri < ci) | (ci >= 128)).astype(F32).astype(BF16)
    pre = dot(stack, upper)
    base = jnp.zeros((16, 128), F32)
    within = []
    for t in range(LANE_TILES):
        blk = pre[t * 16:(t + 1) * 16]
        within.append(blk[:, :128] + base)
        base = base + blk[:, 128:]
    acc = jnp.zeros((1, 128), F32)
    starts = []
    for k in range(10):
        starts.append(acc)
        acc = acc + base[k:k + 1]
    first = jnp.concatenate(starts + [acc] * 6, axis=0)
    ranks = [jnp.sum(member[:, t * 128:(t + 1) * 128] * (within[t] + first), axis=0, keepdims=True)
             for t in range(LANE_TILES)]
    lane = lax.broadcasted_iota(jnp.int32, (1, 128), 1)
    row = jnp.zeros((1, 128), F32)
    for k in range(10):
        row = jnp.where(lane == k, first[k:k + 1], row)
    msg_s[...] = jnp.broadcast_to(row, (8, 128))

    parts = jnp.concatenate(split3(table), axis=0)
    dst = lax.broadcasted_iota(jnp.int32, (SW, 128), 0).astype(F32)
    total = jnp.zeros((24, SW), F32)
    for t in range(0, LANE_TILES, 2):
        hot = jnp.concatenate([(dst == ranks[t]).astype(F32).astype(BF16),
                               (dst == ranks[t + 1]).astype(F32).astype(BF16)], axis=1)
        total = total + dot_t(parts[:, t * 128:(t + 2) * 128], hot)
    ordered = total[0:8] + total[8:16] + total[16:24]
    for t in range(LANE_TILES):
        msg_l[t] = ordered[:, t * 128:(t + 1) * 128]

    for c in loads:
        c.wait()
    rho, m = moments(lambda q: pv[q])
    inv = 1.0 / rho
    mom[0] = rho
    for c in range(3):
        mom[1 + c] = m[c] * inv
    for s, (adj, far) in enumerate(((0, 1), (CX - 1, CX - 2))):
        for c in range(4):
            msg_x[s, c] = mom[c, adj * CY:(adj + 1) * CY]
        for c in range(3):
            msg_x[s, 4 + c] = mom[1 + c, far * CY:(far + 1) * CY]
        for k, q in enumerate(facing(0, 2 * s - 1)):
            msg_x[s, 7 + k] = pv[q, adj * CY:(adj + 1) * CY]
    for s, (adj, far) in enumerate(((0, 1), (CY - 1, CY - 2))):
        for c in range(4):
            msg_y[s, c] = mom[c, pl.ds(adj, CX, stride=CY)]
        for c in range(3):
            msg_y[s, 4 + c] = mom[1 + c, pl.ds(far, CX, stride=CY)]
        for k, q in enumerate(facing(1, 2 * s - 1)):
            msg_y[s, 7 + k] = pv[q, pl.ds(adj, CX, stride=CY)]
    for i in range(4):
        sx, sy = SIDES[4 + i]
        ax, fx = (0, 1) if sx < 0 else (CX - 1, CX - 2)
        ay, fy = (0, 1) if sy < 0 else (CY - 1, CY - 2)
        msg_c[i] = jnp.zeros((16, 128), F32)
        for c in range(4):
            msg_c[i, c:c + 1] = mom[c, ax * CY + ay:ax * CY + ay + 1]
        for j, (nx, ny) in enumerate(((ax, fy), (fx, ay), (fx, fy))):
            for c in range(3):
                msg_c[i, 5 + 3 * j + c:6 + 3 * j + c] = mom[1 + c, nx * CY + ny:nx * CY + ny + 1]
        q = DIRS.index((sx, sy, 0))
        msg_c[i, 4:5] = pv[q, ax * CY + ay:ax * CY + ay + 1]

    pl.semaphore_wait(barrier, 8)
    copies = []
    for d, side in enumerate(SIDES):
        o = SIDES.index((-side[0], -side[1]))
        if side[1] == 0:
            src, out = msg_x.at[d], halo_x.at[o]
        elif side[0] == 0:
            src, out = msg_y.at[d - 2], halo_y.at[o - 2]
        else:
            src, out = msg_c.at[d - 4], halo_c.at[o - 4]
        for k, (a, b) in enumerate(((src, out), (msg_l, lists.at[o]), (msg_s, starts_out.at[o]))):
            copies.append(pltpu.make_async_remote_copy(
                src_ref=a, dst_ref=b, send_sem=send_sem.at[3 * d + k], recv_sem=recv_sem.at[3 * o + k],
                device_id=device(side), device_id_type=MESH))
    for c in copies:
        c.start()

    place = jnp.concatenate([jnp.where(live > 0.0, x, FAR), y, z, zero, zero, zero, zero, zero], axis=0)
    for t in range(LANE_TILES):
        cols_t = jnp.transpose(place[:, t * 128:(t + 1) * 128])
        for c in range(3):
            cols[c, t * 128:(t + 1) * 128] = jnp.broadcast_to(cols_t[:, c:c + 1], (128, 128))
    width = 512
    for h in range(SW // width):
        own = [jnp.broadcast_to(v[:, h * width:(h + 1) * width], (8, width)) for v in (x, y, z)]

        def step(g, carry, own=own):
            at = pl.multiple_of(g * 8, 8)
            p = [jnp.concatenate([cols[c, pl.ds(at, 8)]] * (width // 128), axis=1) for c in range(3)]
            f = pair_terms(*own, *p)
            return tuple(a + b for a, b in zip(carry, f))

        init = tuple(jnp.zeros((8, width), F32) for _ in range(3))
        got = lax.fori_loop(0, SW // 8, step, init)
        for c in range(3):
            pair_out[c:c + 1, h * width:(h + 1) * width] = jnp.sum(got[c], axis=0, keepdims=True)

    for c in copies:
        c.wait()


ADJ_ROWS = 192
ALL_ROWS = 240
BLOCK = 256
GHOST_TILES = 8 * LANE_TILES + 4


def fluid_kernel(pops, own, pair, halo_x, halo_y, halo_c, lists, starts_hbm, next_out, force_out,
                 pv, out_v, starts, node, ucat, force, plane, ghosts, cols, pop_sem, out_sem, start_sem):
    loads = [pltpu.make_async_copy(pops.at[q], pv.at[q], pop_sem.at[q]) for q in range(19)]
    start_copy = pltpu.make_async_copy(starts_hbm, starts, start_sem)
    start_copy.start()
    for c in loads:
        c.start()

    start_copy.wait()
    ghosts[...] = jnp.zeros(ghosts.shape, F32)
    lane = lax.broadcasted_iota(jnp.int32, (8, 128), 1)
    sub = lax.broadcasted_iota(jnp.int32, (8, 128), 0)
    total = jnp.int32(0)
    for d, lo, hi in RANGES:
        a = starts[d, 0, lo].astype(jnp.int32)
        b = starts[d, 0, hi].astype(jnp.int32)
        base = total
        sx, sy = SIDES[d]
        moved = jnp.where(sub == 0, float(sx * CX), jnp.where(sub == 1, float(sy * CY), 0.0))

        def put(t, carry, d=d, a=a, b=b, base=base, moved=moved):
            to = base - a + t * 128 + 128 * 8
            by = to & 127
            tile = lax.shift_right_logical(to, 7) - 8
            at = t * 128 + lane
            v = jnp.where((at >= a) & (at < b), lists[d, t] + moved, 0.0)
            v = pltpu.roll(v, by, 1)
            upper = lane >= by
            low = jnp.maximum(tile, 0)
            ghosts[low] = ghosts[low] + jnp.where(upper & (tile >= 0), v, 0.0)
            ghosts[tile + 1] = ghosts[tile + 1] + jnp.where(upper, 0.0, v)
            return carry

        @pl.when(b > a)
        def _(a=a, b=b, put=put):
            lax.fori_loop(lax.shift_right_logical(a, 7), lax.shift_right_logical(b + 127, 7), put, 0)

        total = total + (b - a)

    for c in loads:
        c.wait()
    rho, m = moments(lambda q: pv[q])
    inv = 1.0 / rho
    node[0] = rho
    node[1] = inv
    for c in range(3):
        u = m[c] * inv
        node[2 + c] = u
        corner = []
        for i in range(4):
            for j in range(4):
                sx, sy = (0 if i < 2 else 1), (0 if j < 2 else 1)
                fx, fy = i in (0, 3), j in (0, 3)
                k = 2 * sx + sy
                r = (11 if fy else 8) if fx else (5 if fy else 1)
                corner.append(halo_c[k, r + c:r + c + 1])
        rows = jnp.concatenate(
            [u, halo_x[0, 1 + c], halo_x[1, 1 + c], halo_y[0, 1 + c], halo_y[1, 1 + c]] + corner
            + [halo_x[0, 4 + c], halo_x[1, 4 + c], halo_y[0, 4 + c], halo_y[1, 4 + c]], axis=0)
        hi, lo = split2(rows)
        ucat[c * ALL_ROWS:(c + 1) * ALL_ROWS, 0:128] = hi
        ucat[c * ALL_ROWS:(c + 1) * ALL_ROWS, 128:256] = lo

    force[...] = jnp.zeros(force.shape, F32)
    zi = lax.broadcasted_iota(jnp.int32, (NZ, 1), 0).astype(F32)
    x8 = lax.broadcasted_iota(jnp.int32, (CX, 1), 0).astype(F32)
    y16 = lax.broadcasted_iota(jnp.int32, (CY, 1), 0).astype(F32)
    ki = lax.broadcasted_iota(jnp.int32, (16, 1), 0)
    ii, jj = lax.shift_right_logical(ki, 2), ki & 3
    xd = jnp.where(ii < 2, ii - 2, ii + CX - 2).astype(F32)
    yd = jnp.where(jj < 2, jj - 2, jj + CY - 2).astype(F32)

    def block(vals, live):
        px, py, pz = vals[0:1], vals[1:2], vals[2:3]
        tz = tent(zi - pz)
        zh, zl = split2(tz)
        tx, ty = tent(x8 - px), tent(y16 - py)
        parts = [tx[i:i + 1] * ty for i in range(CX)]
        parts += [tent(-1.0 - px) * ty, tent(CX - px) * ty, tent(-1.0 - py) * tx, tent(CY - py) * tx]
        parts += [tent(xd - px) * tent(yd - py)]
        parts += [tent(-2.0 - px) * ty, tent(CX + 1.0 - px) * ty, tent(-2.0 - py) * tx, tent(CY + 1.0 - py) * tx]
        plane[...] = jnp.concatenate(parts, axis=0)
        zz = jnp.concatenate([zh, zh], axis=0)
        zhl = jnp.concatenate([zh, zl], axis=0)
        sampled = []
        for c in range(3):
            uc = ucat[c * ALL_ROWS:(c + 1) * ALL_ROWS]
            got = dot(uc, zz) + dot(uc[:, :128], zl)
            sampled.append(jnp.sum(got * plane[...], axis=0, keepdims=True))
        for c in range(3):
            react = (vals[3 + c:4 + c] - 2.0 * sampled[c]) * live
            wh, wl = split2(plane[0:ADJ_ROWS] * react)
            both = dot_t(wh, zhl)
            force[c] = force[c] + (both[:, :128] + both[:, 128:] + dot_t(wl, zh))
        return sampled

    for s in range(SW // BLOCK):
        cut = slice(s * BLOCK, (s + 1) * BLOCK)
        vals = own[:, cut]
        got = block(vals, vals[6:7])
        for c in range(3):
            force_out[c:c + 1, cut] = 2.0 * got[c] - vals[3 + c:4 + c] + 0.24 * pair[c:c + 1, cut]

    slot = lax.broadcasted_iota(jnp.int32, (1, BLOCK), 1)

    def ghost_block(i, carry):
        vals = jnp.concatenate([ghosts[2 * i], ghosts[2 * i + 1]], axis=1)
        live = (slot + i * BLOCK < total).astype(F32)
        block(vals, live)
        return carry

    lax.fori_loop(0, lax.shift_right_logical(total + BLOCK - 1, 8), ghost_block, 0)

    slot1 = lax.broadcasted_iota(jnp.int32, (8, 128), 1)

    def ghost_pairs(t, carry):
        g = ghosts[t]
        g = jnp.where((sub == 0) & (slot1 + t * 128 >= total), FAR, g)
        gt = jnp.transpose(g)
        for c in range(3):
            cols[c] = jnp.broadcast_to(gt[:, c:c + 1], (128, 128))
        groups = jnp.minimum(lax.shift_right_logical(total - t * 128 + 7, 3), 16)
        width = 512
        for h in range(SW // width):
            cut = slice(h * width, (h + 1) * width)
            mine = [jnp.broadcast_to(own[c:c + 1, cut], (8, width)) for c in range(3)]

            def step(n, acc, mine=mine):
                at = pl.multiple_of(n * 8, 8)
                p = [jnp.concatenate([cols[c, pl.ds(at, 8)]] * (width // 128), axis=1) for c in range(3)]
                f = pair_terms(*mine, *p)
                return tuple(a + b for a, b in zip(acc, f))

            init = tuple(jnp.zeros((8, width), F32) for _ in range(3))
            got = lax.fori_loop(0, groups, step, init)
            for c in range(3):
                force_out[c:c + 1, cut] = force_out[c:c + 1, cut] + 0.24 * jnp.sum(got[c], axis=0, keepdims=True)
        return carry

    lax.fori_loop(0, lax.shift_right_logical(total + 127, 7), ghost_pairs, 0)
    force_out[...] = force_out[...] * own[6:7]

    def prepare(rho, u0, half, g):
        u = [u0[c] + half * g[c] for c in range(3)]
        uu = u[0] * u[0] + u[1] * u[1] + u[2] * u[2]
        ug = u[0] * g[0] + u[1] * g[1] + u[2] * g[2]
        k0 = 1.25 * rho * (1.0 - 1.5 * uu) - 1.125 * ug
        return k0, 3.75 * rho, 5.625 * rho, u, [1.125 * v for v in g]

    def along(q, v):
        out = None
        for c in range(3):
            s = DIRS[q][c]
            if s:
                out = (v[c] if s > 0 else -v[c]) if out is None else (out + v[c] if s > 0 else out - v[c])
        return out

    def post(q, f, prep):
        k0, r1, r2, u, g = prep
        if q == 0:
            return -0.25 * f + WEIGHTS[0] * k0
        a, p = along(q, u), along(q, g)
        return -0.25 * f + WEIGHTS[q] * (k0 + a * (r1 + r2 * a + 3.0 * p) + p)

    def side_prep(rho, u0, lo, n):
        g = [force[c, lo:lo + n] for c in range(3)]
        return prepare(rho, u0, 0.5 / rho, g)

    inner = side_prep(node[0], [node[2 + c] for c in range(3)], 0, ROWS)
    k0, r1, r2, u, g = inner
    node[1] = k0
    for c in range(3):
        node[2 + c] = u[c]
        node[5 + c] = g[c]
    xs = [side_prep(halo_x[s, 0], [halo_x[s, 1 + c] for c in range(3)], ROWS + s * CY, CY) for s in range(2)]
    ys = [side_prep(halo_y[s, 0], [halo_y[s, 1 + c] for c in range(3)], ROWS + 2 * CY + s * CX, CX)
          for s in range(2)]
    cs = []
    for i in range(4):
        sx, sy = SIDES[4 + i]
        r = ADJ_ROWS - 16 + (1 if sx < 0 else 2) * 4 + (1 if sy < 0 else 2)
        cs.append(side_prep(halo_c[i, 0:1], [halo_c[i, 1 + c:2 + c] for c in range(3)], r, 1))
    stores = []
    for q in range(19):
        dx, dy, dz = DIRS[q]
        rho_q = node[0]
        prep = (node[1], 3.75 * rho_q, 5.625 * rho_q, [node[2 + c] for c in range(3)], [node[5 + c] for c in range(3)])

        def turned(v, dz=dz):
            return pltpu.roll(v, dz % NZ, 1) if dz else v

        v = turned(post(q, pv[q], prep))
        if dy:
            v = pltpu.roll(v, dy % ROWS, 0)
        if dx == 0:
            out_v[q] = v
        else:
            s = 0 if dx > 0 else 1
            e = turned(post(q, halo_x[s, 7 + facing(0, dx).index(q)], xs[s]))
            if dy:
                e = pltpu.roll(e, dy % CY, 0)
            if dx > 0:
                out_v[q, CY:ROWS] = v[0:ROWS - CY]
                out_v[q, 0:CY] = e
            else:
                out_v[q, 0:ROWS - CY] = v[CY:ROWS]
                out_v[q, ROWS - CY:ROWS] = e
        if dy:
            s = 0 if dy > 0 else 1
            at = 0 if dy > 0 else CY - 1
            e = turned(post(q, halo_y[s, 7 + facing(1, dy).index(q)], ys[s]))
            if dx:
                e = pltpu.roll(e, dx % CX, 0)
            out_v[q, pl.ds(at, CX, stride=CY)] = e
            if dx:
                i = SIDES.index((-dx, -dy)) - 4
                r = at + (0 if dx > 0 else (CX - 1) * CY)
                out_v[q, r:r + 1] = post(q, halo_c[i, 4:5], cs[i])
        c = pltpu.make_async_copy(out_v.at[q], next_out.at[q], out_sem.at[q])
        c.start()
        stores.append(c)
    for c in stores:
        c.wait()


def body(n_gx, n_gy, populations, anchor, offsets, heading, velocity, live_count):
    pops = populations.reshape(19, ROWS, NZ)
    vmem = pl.BlockSpec(memory_space=pltpu.VMEM)
    smem = pl.BlockSpec(memory_space=pltpu.SMEM)
    hbm = pl.BlockSpec(memory_space=pl.ANY)
    dma = pltpu.SemaphoreType.DMA
    halo = (
        jax.ShapeDtypeStruct((2, 12, CY, 128), F32),
        jax.ShapeDtypeStruct((2, 12, CX, 128), F32),
        jax.ShapeDtypeStruct((4, 16, 128), F32),
        jax.ShapeDtypeStruct((8, LANE_TILES, 8, 128), F32),
        jax.ShapeDtypeStruct((8, 8, 128), F32),
        jax.ShapeDtypeStruct((8, SW), F32),
        jax.ShapeDtypeStruct((3, SW), F32),
    )
    halo_x, halo_y, halo_c, lists, starts, own, pair = pl.pallas_call(
        functools.partial(exchange_kernel, n_gx, n_gy),
        out_shape=halo,
        in_specs=[hbm, vmem, vmem, vmem, vmem, smem],
        out_specs=[vmem] * 7,
        scratch_shapes=[
            pltpu.VMEM((19, ROWS, NZ), F32),
            pltpu.VMEM((2, 12, CY, 128), F32),
            pltpu.VMEM((2, 12, CX, 128), F32),
            pltpu.VMEM((4, 16, 128), F32),
            pltpu.VMEM((LANE_TILES, 8, 128), F32),
            pltpu.VMEM((8, 128), F32),
            pltpu.VMEM((4, ROWS, NZ), F32),
            pltpu.VMEM((3, SW, 128), F32),
            dma((19,)), dma((24,)), dma((24,)),
        ],
        compiler_params=pltpu.CompilerParams(collective_id=0, has_side_effects=True),
        name="exchange",
    )(pops, anchor, offsets, heading, velocity, live_count)
    moved, force = pl.pallas_call(
        fluid_kernel,
        out_shape=(jax.ShapeDtypeStruct((19, ROWS, NZ), F32), jax.ShapeDtypeStruct((3, SW), F32)),
        in_specs=[hbm, vmem, vmem, vmem, vmem, vmem, vmem, hbm],
        out_specs=[hbm, vmem],
        scratch_shapes=[
            pltpu.VMEM((19, ROWS, NZ), F32),
            pltpu.VMEM((19, ROWS, NZ), F32),
            pltpu.SMEM((8, 8, 128), F32),
            pltpu.VMEM((8, ROWS, NZ), F32),
            pltpu.VMEM((3 * ALL_ROWS, 256), BF16),
            pltpu.VMEM((3, ADJ_ROWS, NZ), F32),
            pltpu.VMEM((ALL_ROWS, BLOCK), F32),
            pltpu.VMEM((GHOST_TILES, 8, 128), F32),
            pltpu.VMEM((3, 128, 128), F32),
            dma((19,)), dma((19,)), dma,
        ],
        name="fluid",
    )(pops, own, pair, halo_x, halo_y, halo_c, lists, starts)
    return (moved.reshape(populations.shape), force.reshape(1, 1, 3, SW))


def solution(mesh):
    return jax.shard_map(
        functools.partial(body, mesh.shape["gx"], mesh.shape["gy"]),
        mesh=mesh,
        in_specs=(
            P(None, "gx", "gy", None),
            P("gx", "gy", None),
            P("gx", "gy", None, None),
            P("gx", "gy", None, None),
            P("gx", "gy", None, None),
            P("gx", "gy"),
        ),
        out_specs=(P(None, "gx", "gy", None), P("gx", "gy", None, None)),
        check_vma=False,
    )
```

```python
import functools

import jax
import jax.numpy as jnp
import numpy as np
from jax import lax
from jax.experimental import pallas as pl
from jax.experimental.pallas import tpu as pltpu
from jax.sharding import PartitionSpec as P

DIRS = (
    (0, 0, 0), (1, 0, 0), (-1, 0, 0), (0, 1, 0), (0, -1, 0), (0, 0, 1), (0, 0, -1),
    (1, 1, 0), (-1, -1, 0), (1, -1, 0), (-1, 1, 0), (1, 0, 1), (-1, 0, -1),
    (1, 0, -1), (-1, 0, 1), (0, 1, 1), (0, -1, -1), (0, 1, -1), (0, -1, 1),
)
WEIGHTS = (1.0 / 3.0,) + (1.0 / 18.0,) * 6 + (1.0 / 36.0,) * 12
CUTOFF = 2.0 ** (1.0 / 3.0)
REACH = 1.125
FAR = 1.0e9
F32 = jnp.float32
BF16 = jnp.bfloat16
MESH = pl.DeviceIdType.MESH

CX, CY, NZ, SW = 8, 16, 128, 1024
ROWS = CX * CY
LANE_TILES = SW // 128

SIDES = ((-1, 0), (1, 0), (0, -1), (0, 1), (-1, -1), (-1, 1), (1, -1), (1, 1))
RANGES = ((0, 4, 7), (1, 0, 3), (2, 2, 5), (3, 6, 8), (3, 0, 1), (4, 4, 5), (5, 6, 7), (6, 2, 3), (7, 0, 1))


def facing(axis, sign):
    return [q for q in range(19) if DIRS[q][axis] == sign]


def corner_q(sx, sy):
    return DIRS.index((-sx, -sy, 0))


def split2(v):
    hi = v.astype(BF16)
    return hi, (v - hi.astype(F32)).astype(BF16)


def split3(v):
    hi = v.astype(BF16)
    rest = v - hi.astype(F32)
    mid = rest.astype(BF16)
    return hi, mid, (rest - mid.astype(F32)).astype(BF16)


def dot(a, b):
    return lax.dot_general(a, b, (((1,), (0,)), ((), ())), preferred_element_type=F32)


def dot_t(a, b):
    return lax.dot_general(a, b, (((1,), (1,)), ((), ())), preferred_element_type=F32)


def tent(d):
    return jnp.maximum(1.0 - jnp.abs(d), 0.0)


def moments(load):
    rho = None
    mom = [None, None, None]
    for q in range(19):
        f = load(q)
        rho = f if rho is None else rho + f
        for c in range(3):
            s = DIRS[q][c]
            if s:
                if mom[c] is None:
                    mom[c] = f if s > 0 else -f
                else:
                    mom[c] = mom[c] + f if s > 0 else mom[c] - f
    return rho, mom


def pair_terms(ox, oy, oz, px, py, pz):
    dx = ox - px
    dy = oy - py
    dz = oz - pz
    dz = dz - NZ * jnp.round(dz * (1.0 / NZ))
    raw = dx * dx + dy * dy + dz * dz
    inv = 1.0 / jnp.maximum(raw, 0.8)
    sixth = inv * inv * inv
    mag = (sixth + sixth - 1.0) * (sixth * inv)
    mag = jnp.where(raw < CUTOFF, mag, 0.0)
    return mag * dx, mag * dy, mag * dz


def classes(x, y, live):
    xl, xh = x < REACH, x > CX - 1 - REACH
    yl, yh = y < REACH, y > CY - 1 - REACH
    yc = jnp.where(yl, 0.0, jnp.where(yh, 2.0, 1.0))
    kind = jnp.where(xl, yc, jnp.where(xh, 6.0 - yc, jnp.where(yl, 7.0, jnp.where(yh, 3.0, 8.0))))
    return jnp.where(live > 0.0, kind, 9.0)


def sort_ranks(kind):
    krow = lax.broadcasted_iota(jnp.int32, (16, SW), 0).astype(F32)
    member = (krow == kind).astype(F32)
    stack = jnp.concatenate([member[:, t * 128:(t + 1) * 128] for t in range(LANE_TILES)], axis=0).astype(BF16)
    ri = lax.broadcasted_iota(jnp.int32, (128, 256), 0)
    ci = lax.broadcasted_iota(jnp.int32, (128, 256), 1)
    upper = ((ri < ci) | (ci >= 128)).astype(F32).astype(BF16)
    pre = dot(stack, upper)
    base = jnp.zeros((16, 128), F32)
    within = []
    for t in range(LANE_TILES):
        blk = pre[t * 16:(t + 1) * 16]
        within.append(blk[:, :128] + base)
        base = base + blk[:, 128:]
    acc = jnp.zeros((1, 128), F32)
    starts = []
    for k in range(10):
        starts.append(acc)
        acc = acc + base[k:k + 1]
    first = jnp.concatenate(starts + [acc] * 6, axis=0)
    ranks = [jnp.sum(member[:, t * 128:(t + 1) * 128] * (within[t] + first), axis=0, keepdims=True)
             for t in range(LANE_TILES)]
    lane = lax.broadcasted_iota(jnp.int32, (1, 128), 1)
    row = jnp.zeros((1, 128), F32)
    for k in range(10):
        row = jnp.where(lane == k, first[k:k + 1], row)
    return ranks, row


def plane_weights(px, py, far):
    x8 = lax.broadcasted_iota(jnp.int32, (CX, 1), 0).astype(F32)
    y16 = lax.broadcasted_iota(jnp.int32, (CY, 1), 0).astype(F32)
    ki = lax.broadcasted_iota(jnp.int32, (16, 1), 0)
    ii, jj = lax.shift_right_logical(ki, 2), ki & 3
    xd = jnp.where(ii < 2, ii - 2, ii + CX - 2).astype(F32)
    yd = jnp.where(jj < 2, jj - 2, jj + CY - 2).astype(F32)
    tx, ty = tent(x8 - px), tent(y16 - py)
    parts = [tx[i:i + 1] * ty for i in range(CX)]
    parts += [tent(-1.0 - px) * ty, tent(CX - px) * ty, tent(-1.0 - py) * tx, tent(CY - py) * tx]
    parts += [tent(xd - px) * tent(yd - py)]
    if far:
        parts += [tent(-2.0 - px) * ty, tent(CX + 1.0 - px) * ty, tent(-2.0 - py) * tx, tent(CY + 1.0 - py) * tx]
    return jnp.concatenate(parts, axis=0)


def z_weights(pz):
    zi = lax.broadcasted_iota(jnp.int32, (NZ, 1), 0).astype(F32)
    return split2(tent(zi - pz))


def widen(v):
    hi, lo = split2(v)
    return jnp.concatenate([hi, lo], axis=1)


def sample(u, zh, zl):
    return dot(u, jnp.concatenate([zh, zh], axis=0)) + dot(u[:, :128], zl)


def columns(cols, at, place):
    turned = jnp.transpose(place)
    for c in range(3):
        cols[c, at:at + 128] = jnp.broadcast_to(turned[:, c:c + 1], (128, 128))


def pair_step(cols, mine, width):
    def step(n, acc):
        at = pl.multiple_of(n * 8, 8)
        p = [jnp.concatenate([cols[c, pl.ds(at, 8)]] * (width // 128), axis=1) for c in range(3)]
        return tuple(a + b for a, b in zip(acc, pair_terms(*mine, *p)))

    return step


def exchange_kernel(n_gx, n_gy, pops, anchor, offsets, heading, velocity, count,
                    halo_x, halo_y, halo_c, lists, starts_out, own_out, base_out, mom, inner, zhl, plane,
                    msg_x, msg_y, msg_c, msg_l, msg_s, cols, send_sem, recv_sem):
    gx = lax.axis_index("gx")
    gy = lax.axis_index("gy")

    def device(side):
        return (lax.rem(gx + side[0] + n_gx, n_gx), lax.rem(gy + side[1] + n_gy, n_gy))

    barrier = pltpu.get_barrier_semaphore()
    for side in SIDES:
        pl.semaphore_signal(barrier, inc=1, device_id=device(side), device_id_type=MESH)

    rho, m = moments(lambda q: pops[q])
    inv = 1.0 / rho
    mom[0] = rho
    for c in range(3):
        mom[1 + c] = m[c] * inv
    for s, (adj, far) in enumerate(((0, 1), (CX - 1, CX - 2))):
        for c in range(4):
            msg_x[s, c] = mom[c, adj * CY:(adj + 1) * CY]
        for c in range(3):
            msg_x[s, 4 + c] = mom[1 + c, far * CY:(far + 1) * CY]
        for k, q in enumerate(facing(0, 2 * s - 1)):
            msg_x[s, 7 + k] = pops[q, adj * CY:(adj + 1) * CY]
    for s, (adj, far) in enumerate(((0, 1), (CY - 1, CY - 2))):
        for c in range(4):
            msg_y[s, c] = mom[c, pl.ds(adj, CX, stride=CY)]
        for c in range(3):
            msg_y[s, 4 + c] = mom[1 + c, pl.ds(far, CX, stride=CY)]
        for k, q in enumerate(facing(1, 2 * s - 1)):
            msg_y[s, 7 + k] = pops[q, pl.ds(adj, CX, stride=CY)]
    for i in range(4):
        sx, sy = SIDES[4 + i]
        ax, fx = (0, 1) if sx < 0 else (CX - 1, CX - 2)
        ay, fy = (0, 1) if sy < 0 else (CY - 1, CY - 2)
        msg_c[i] = jnp.zeros((16, 128), F32)
        for c in range(4):
            msg_c[i, c:c + 1] = mom[c, ax * CY + ay:ax * CY + ay + 1]
        for j, (nx, ny) in enumerate(((ax, fy), (fx, ay), (fx, fy))):
            for c in range(3):
                msg_c[i, 5 + 3 * j + c:6 + 3 * j + c] = mom[1 + c, nx * CY + ny:nx * CY + ny + 1]
        q = DIRS.index((sx, sy, 0))
        msg_c[i, 4:5] = pops[q, ax * CY + ay:ax * CY + ay + 1]

    def send(k, a, b, side, o):
        d = SIDES.index(side)
        return pltpu.make_async_remote_copy(
            src_ref=a, dst_ref=b, send_sem=send_sem.at[3 * d + k], recv_sem=recv_sem.at[3 * o + k],
            device_id=device(side), device_id_type=MESH)

    fluid, swimmers = [], []
    for d, side in enumerate(SIDES):
        o = SIDES.index((-side[0], -side[1]))
        if side[1] == 0:
            fluid.append(send(0, msg_x.at[d], halo_x.at[o], side, o))
        elif side[0] == 0:
            fluid.append(send(0, msg_y.at[d - 2], halo_y.at[o - 2], side, o))
        else:
            fluid.append(send(0, msg_c.at[d - 4], halo_c.at[o - 4], side, o))
        swimmers.append(send(1, msg_s, starts_out.at[o], side, o))
        swimmers.append(send(2, msg_l.at[:, pl.ds(0, 6)], lists.at[o, :, pl.ds(0, 6)], side, o))
    pl.semaphore_wait(barrier, 8)
    for c in fluid:
        c.start()

    root = anchor[0]
    bxf = lax.shift_right_logical(root, 7).astype(F32)
    cxf = jnp.floor(bxf * (1.0 / (CY + 2)) + 0.01)
    cyf = bxf - cxf * (CY + 2)
    x = cxf - 1.0 + offsets[0]
    y = cyf - 1.0 + offsets[1]
    z = (root & (NZ - 1)).astype(F32) + offsets[2]
    slot = lax.broadcasted_iota(jnp.int32, (1, SW), 1)
    live = (slot < count[...]).astype(F32)
    ranks, row = sort_ranks(classes(x, y, live))
    msg_s[...] = row
    starts_out[8] = row
    ang = heading[0, 0]
    cs, sn = jnp.cos(ang), jnp.sin(ang)
    c1 = cs[1:2]
    w = [2.0 * velocity[0] - 0.5 * (cs[0:1] * c1),
         2.0 * velocity[1] - 0.5 * (sn[0:1] * c1),
         2.0 * velocity[2] - 0.5 * sn[1:2]]
    zero = jnp.zeros((1, SW), F32)
    table = jnp.concatenate([x, y, z, w[0], w[1], w[2], live, zero], axis=0)
    parts = jnp.concatenate(split3(table), axis=0)
    dst = lax.broadcasted_iota(jnp.int32, (SW, 128), 0).astype(F32)
    total = jnp.zeros((24, SW), F32)
    for t in range(0, LANE_TILES, 2):
        hot = jnp.concatenate([(dst == ranks[t]).astype(F32).astype(BF16),
                               (dst == ranks[t + 1]).astype(F32).astype(BF16)], axis=1)
        total = total + dot_t(parts[:, t * 128:(t + 2) * 128], hot)
    ordered = total[0:8] + total[8:16] + total[16:24]
    for t in range(LANE_TILES):
        msg_l[t] = ordered[:, t * 128:(t + 1) * 128]
    for c in swimmers:
        c.start()

    for c in range(3):
        inner[c * ROWS:(c + 1) * ROWS] = widen(mom[1 + c])
    for i in range(BLOCKS):
        cut = slice(i * BLOCK, (i + 1) * BLOCK)
        zh, zl = z_weights(z[:, cut])
        zhl[i, 0:NZ] = zh
        zhl[i, NZ:2 * NZ] = zl
        plane[i] = plane_weights(x[:, cut], y[:, cut], False)
        got = sample(inner[...], zh, zl)
        own_out[i, 0:3] = table[0:3, cut]
        own_out[i, 6:8] = table[6:8, cut]
        for c in range(3):
            s = jnp.sum(got[c * ROWS:(c + 1) * ROWS] * plane[i, 0:ROWS], axis=0, keepdims=True)
            own_out[i, 3 + c:4 + c] = (w[c][:, cut] - 2.0 * s) * live[:, cut]

    place = jnp.concatenate([jnp.where(live > 0.0, x, FAR), y, z, zero, zero, zero, zero, zero], axis=0)
    for t in range(LANE_TILES):
        columns(cols, t * 128, place[:, t * 128:(t + 1) * 128])
    for i in range(0, BLOCKS, 2):
        width = 2 * BLOCK
        mine = [jnp.broadcast_to(v[:, i * BLOCK:i * BLOCK + width], (8, width)) for v in (x, y, z)]
        init = tuple(jnp.zeros((8, width), F32) for _ in range(3))
        got = lax.fori_loop(0, SW // 8, pair_step(cols, mine, width), init)
        for c in range(3):
            total_c = 0.24 * jnp.sum(got[c], axis=0, keepdims=True)
            for j in range(2):
                cut = slice((i + j) * BLOCK, (i + j + 1) * BLOCK)
                base_out[i + j, c:c + 1] = (total_c[:, j * BLOCK:(j + 1) * BLOCK] * live[:, cut]
                                            - own_out[i + j, 3 + c:4 + c])

    for c in fluid + swimmers:
        c.wait()


ADJ = 64
FAR_ROWS = 48
ADJ_ROWS = ROWS + ADJ
BLOCK = 256
BLOCKS = SW // BLOCK
GHOST_TILES = 8 * LANE_TILES + 4


def fluid_kernel(pops, own, base, halo_x, halo_y, halo_c, lists, starts_in, mom, inner, zhl, plane,
                 next_out, force_out,
                 acc, out_v, starts, node, near, outer, force, ghosts, cols, out_sem, start_sem):
    start_copy = pltpu.make_async_copy(starts_in, starts, start_sem)
    start_copy.start()
    acc[...] = base[...]
    ghosts[...] = jnp.zeros(ghosts.shape, F32)
    force[...] = jnp.zeros(force.shape, F32)
    for c in range(3):
        corner = []
        for i in range(4):
            for j in range(4):
                sx, sy = (0 if i < 2 else 1), (0 if j < 2 else 1)
                fx, fy = i in (0, 3), j in (0, 3)
                k = 2 * sx + sy
                r = (11 if fy else 8) if fx else (5 if fy else 1)
                corner.append(halo_c[k, r + c:r + c + 1])
        near[c * ADJ:(c + 1) * ADJ] = widen(jnp.concatenate(
            [halo_x[0, 1 + c], halo_x[1, 1 + c], halo_y[0, 1 + c], halo_y[1, 1 + c]] + corner, axis=0))
        outer[c * FAR_ROWS:(c + 1) * FAR_ROWS] = widen(jnp.concatenate(
            [halo_x[0, 4 + c], halo_x[1, 4 + c], halo_y[0, 4 + c], halo_y[1, 4 + c]], axis=0))
    start_copy.wait()
    lane = lax.broadcasted_iota(jnp.int32, (8, 128), 1)
    sub = lax.broadcasted_iota(jnp.int32, (8, 128), 0)
    total = jnp.int32(0)
    for d, lo, hi in RANGES:
        a = starts[d, 0, lo].astype(jnp.int32)
        b = starts[d, 0, hi].astype(jnp.int32)
        sx, sy = SIDES[d]
        moved = jnp.where(sub == 0, float(sx * CX), jnp.where(sub == 1, float(sy * CY), 0.0))

        def put(t, carry, d=d, a=a, b=b, base=total, moved=moved):
            to = base - a + t * 128 + 128 * 8
            by = to & 127
            tile = lax.shift_right_logical(to, 7) - 8
            src = jnp.minimum(t, LANE_TILES - 1)
            at = t * 128 + lane
            v = jnp.where((at >= a) & (at < b), lists[d, src] + moved, 0.0)
            v = pltpu.roll(v, by, 1)
            upper = lane >= by
            low = jnp.maximum(tile, 0)
            ghosts[low] = ghosts[low] + jnp.where(upper & (tile >= 0), v, 0.0)
            ghosts[tile + 1] = ghosts[tile + 1] + jnp.where(upper, 0.0, v)
            return carry

        t0 = lax.shift_right_logical(a, 7)
        put(t0, 0)
        put(t0 + 1, 0)
        lax.fori_loop(t0 + 2, lax.shift_right_logical(b + 127, 7), put, 0)
        total = total + (b - a)

    def spread(weights, react, zz):
        zh = zz[0:NZ]
        for c in range(3):
            wh, wl = split2(weights * react[c])
            both = dot_t(wh, zz)
            force[c] = force[c] + (both[:, :128] + both[:, 128:] + dot_t(wl, zh))

    n_own = starts[8, 0, 9].astype(jnp.int32)

    def own_block(i, carry):
        zz = zhl[i]
        got = sample(near[...], zz[0:NZ], zz[NZ:2 * NZ])
        live = own[i, 6:7]
        react = []
        for c in range(3):
            s = jnp.sum(got[c * ADJ:(c + 1) * ADJ] * plane[i, ROWS:ADJ_ROWS], axis=0, keepdims=True)
            s = 2.0 * s * live
            react.append(own[i, 3 + c:4 + c] - s)
            acc[i, c:c + 1] = acc[i, c:c + 1] + s
        spread(plane[i], react, zz)
        return carry

    lax.fori_loop(0, lax.shift_right_logical(n_own + BLOCK - 1, 8), own_block, 0)
    slot = lax.broadcasted_iota(jnp.int32, (1, BLOCK), 1)

    def ghost_block(i, carry):
        vals = jnp.concatenate([ghosts[2 * i], ghosts[2 * i + 1]], axis=1)
        live = (slot + i * BLOCK < total).astype(F32)
        zh, zl = z_weights(vals[2:3])
        weights = plane_weights(vals[0:1], vals[1:2], True)
        gi = sample(inner[...], zh, zl)
        gn = sample(near[...], zh, zl)
        gf = sample(outer[...], zh, zl)
        react = []
        for c in range(3):
            s = (jnp.sum(gi[c * ROWS:(c + 1) * ROWS] * weights[0:ROWS], axis=0, keepdims=True)
                 + jnp.sum(gn[c * ADJ:(c + 1) * ADJ] * weights[ROWS:ADJ_ROWS], axis=0, keepdims=True)
                 + jnp.sum(gf[c * FAR_ROWS:(c + 1) * FAR_ROWS] * weights[ADJ_ROWS:], axis=0, keepdims=True))
            react.append((vals[3 + c:4 + c] - 2.0 * s) * live)
        spread(weights[0:ADJ_ROWS], react, jnp.concatenate([zh, zl], axis=0))
        return carry

    lax.fori_loop(0, lax.shift_right_logical(total + BLOCK - 1, 8), ghost_block, 0)

    tiles = lax.shift_right_logical(total + 127, 7)

    def ghost_columns(t, carry):
        g = jnp.where((sub == 0) & (lane + t * 128 >= total), FAR, ghosts[t])
        turned = jnp.transpose(g)
        at = pl.multiple_of(t * 128, 128)
        for c in range(3):
            cols[c, pl.ds(at, 128)] = jnp.broadcast_to(turned[:, c:c + 1], (128, 128))
        return carry

    lax.fori_loop(0, tiles, ghost_columns, 0)

    def ghost_pairs(i, carry):
        mine = [jnp.broadcast_to(own[i, c:c + 1], (8, BLOCK)) for c in range(3)]
        one = pair_step(cols, mine, BLOCK)
        init = tuple(jnp.zeros((8, BLOCK), F32) for _ in range(3))
        got = lax.fori_loop(0, lax.shift_right_logical(total + 15, 4),
                            lambda n, acc: one(2 * n + 1, one(2 * n, acc)), init)
        live = own[i, 6:7]
        for c in range(3):
            acc[i, c:c + 1] = acc[i, c:c + 1] + 0.24 * live * jnp.sum(got[c], axis=0, keepdims=True)
        return carry

    lax.fori_loop(0, lax.shift_right_logical(n_own + BLOCK - 1, 8), ghost_pairs, 0)
    for i in range(BLOCKS):
        for c in range(3):
            force_out[c, :, i * BLOCK:(i + 1) * BLOCK] = acc[i, c:c + 1]

    def prepare(rho, u0, half, g):
        u = [u0[c] + half * g[c] for c in range(3)]
        uu = u[0] * u[0] + u[1] * u[1] + u[2] * u[2]
        ug = u[0] * g[0] + u[1] * g[1] + u[2] * g[2]
        k0 = 1.25 * rho * (1.0 - 1.5 * uu) - 1.125 * ug
        return k0, 3.75 * rho, 5.625 * rho, u, [1.125 * v for v in g]

    def along(q, v):
        out = None
        for c in range(3):
            s = DIRS[q][c]
            if s:
                out = (v[c] if s > 0 else -v[c]) if out is None else (out + v[c] if s > 0 else out - v[c])
        return out

    def post(q, f, prep):
        k0, r1, r2, u, g = prep
        if q == 0:
            return -0.25 * f + WEIGHTS[0] * k0
        a, p = along(q, u), along(q, g)
        return -0.25 * f + WEIGHTS[q] * (k0 + a * (r1 + r2 * a + 3.0 * p) + p)

    def side_prep(rho, u0, lo, n):
        g = [force[c, lo:lo + n] for c in range(3)]
        return prepare(rho, u0, 0.5 / rho, g)

    k0, r1, r2, u, g = side_prep(mom[0], [mom[1 + c] for c in range(3)], 0, ROWS)
    node[0] = k0
    for c in range(3):
        node[1 + c] = u[c]
        node[4 + c] = g[c]
    xs = [side_prep(halo_x[s, 0], [halo_x[s, 1 + c] for c in range(3)], ROWS + s * CY, CY) for s in range(2)]
    ys = [side_prep(halo_y[s, 0], [halo_y[s, 1 + c] for c in range(3)], ROWS + 2 * CY + s * CX, CX)
          for s in range(2)]
    cs = []
    for i in range(4):
        sx, sy = SIDES[4 + i]
        r = ADJ_ROWS - 16 + (1 if sx < 0 else 2) * 4 + (1 if sy < 0 else 2)
        cs.append(side_prep(halo_c[i, 0:1], [halo_c[i, 1 + c:2 + c] for c in range(3)], r, 1))
    stores = []
    for q in range(19):
        dx, dy, dz = DIRS[q]
        rho_q = mom[0]
        prep = (node[0], 3.75 * rho_q, 5.625 * rho_q, [node[1 + c] for c in range(3)], [node[4 + c] for c in range(3)])

        def turned(v, dz=dz):
            return pltpu.roll(v, dz % NZ, 1) if dz else v

        v = turned(post(q, pops[q], prep))
        if dy:
            v = pltpu.roll(v, dy % ROWS, 0)
        if dx == 0:
            out_v[q] = v
        else:
            s = 0 if dx > 0 else 1
            e = turned(post(q, halo_x[s, 7 + facing(0, dx).index(q)], xs[s]))
            if dy:
                e = pltpu.roll(e, dy % CY, 0)
            if dx > 0:
                out_v[q, CY:ROWS] = v[0:ROWS - CY]
                out_v[q, 0:CY] = e
            else:
                out_v[q, 0:ROWS - CY] = v[CY:ROWS]
                out_v[q, ROWS - CY:ROWS] = e
        if dy:
            s = 0 if dy > 0 else 1
            at = 0 if dy > 0 else CY - 1
            e = turned(post(q, halo_y[s, 7 + facing(1, dy).index(q)], ys[s]))
            if dx:
                e = pltpu.roll(e, dx % CX, 0)
            out_v[q, pl.ds(at, CX, stride=CY)] = e
            if dx:
                i = SIDES.index((-dx, -dy)) - 4
                r = at + (0 if dx > 0 else (CX - 1) * CY)
                out_v[q, r:r + 1] = post(q, halo_c[i, 4:5], cs[i])
        c = pltpu.make_async_copy(out_v.at[q], next_out.at[q], out_sem.at[q])
        c.start()
        stores.append(c)
    for c in stores:
        c.wait()


def body(n_gx, n_gy, populations, anchor, offsets, heading, velocity, live_count):
    pops = populations.reshape(19, ROWS, NZ)
    vmem = pl.BlockSpec(memory_space=pltpu.VMEM)
    hbm = pl.BlockSpec(memory_space=pl.ANY)
    dma = pltpu.SemaphoreType.DMA
    held = (
        pltpu.VMEM((2, 12, CY, 128), F32),
        pltpu.VMEM((2, 12, CX, 128), F32),
        pltpu.VMEM((4, 16, 128), F32),
        pltpu.VMEM((8, LANE_TILES, 8, 128), F32),
        pltpu.VMEM((9, 1, 128), F32),
        pltpu.VMEM((BLOCKS, 8, BLOCK), F32),
        pltpu.VMEM((BLOCKS, 8, BLOCK), F32),
        pltpu.VMEM((4, ROWS, NZ), F32),
        pltpu.VMEM((3 * ROWS, 2 * NZ), BF16),
        pltpu.VMEM((BLOCKS, 2 * NZ, BLOCK), BF16),
        pltpu.VMEM((BLOCKS, ADJ_ROWS, BLOCK), F32),
    )
    halo_x, halo_y, halo_c, lists, starts, own, base, mom, inner, zhl, plane = pl.pallas_call(
        functools.partial(exchange_kernel, n_gx, n_gy),
        out_shape=held,
        in_specs=[vmem] * 6,
        out_specs=[vmem] * 11,
        scratch_shapes=[
            pltpu.VMEM((2, 12, CY, 128), F32),
            pltpu.VMEM((2, 12, CX, 128), F32),
            pltpu.VMEM((4, 16, 128), F32),
            pltpu.VMEM((LANE_TILES, 8, 128), F32),
            pltpu.VMEM((1, 128), F32),
            pltpu.VMEM((3, SW, 128), F32),
            dma((24,)), dma((24,)),
        ],
        compiler_params=pltpu.CompilerParams(collective_id=0, has_side_effects=True, vmem_limit_bytes=20 << 20),
        name="exchange",
    )(pops, anchor, jnp.swapaxes(offsets, 1, 2).reshape(3, 1, SW), heading,
      jnp.swapaxes(velocity, 1, 2).reshape(3, 1, SW), live_count)
    moved, force = pl.pallas_call(
        fluid_kernel,
        out_shape=(jax.ShapeDtypeStruct((19, ROWS, NZ), F32), jax.ShapeDtypeStruct((3, 1, SW), F32)),
        in_specs=[vmem] * 12,
        out_specs=[hbm, vmem],
        scratch_shapes=[
            pltpu.VMEM((BLOCKS, 8, BLOCK), F32),
            pltpu.VMEM((19, ROWS, NZ), F32),
            pltpu.SMEM((9, 1, 128), F32),
            pltpu.VMEM((7, ROWS, NZ), F32),
            pltpu.VMEM((3 * ADJ, 2 * NZ), BF16),
            pltpu.VMEM((3 * FAR_ROWS, 2 * NZ), BF16),
            pltpu.VMEM((3, ADJ_ROWS, NZ), F32),
            pltpu.VMEM((GHOST_TILES, 8, 128), F32),
            pltpu.VMEM((3, GHOST_TILES * 128, 128), F32),
            dma((19,)), dma,
        ],
        compiler_params=pltpu.CompilerParams(vmem_limit_bytes=32 << 20),
        name="fluid",
    )(pops, own, base, halo_x, halo_y, halo_c, lists, starts, mom, inner, zhl, plane)
    return (moved.reshape(populations.shape), jnp.swapaxes(force.reshape(1, 3, 1, SW), 1, 2))


def solution(mesh):
    return jax.shard_map(
        functools.partial(body, mesh.shape["gx"], mesh.shape["gy"]),
        mesh=mesh,
        in_specs=(
            P(None, "gx", "gy", None),
            P("gx", "gy", None),
            P("gx", "gy", None, None),
            P("gx", "gy", None, None),
            P("gx", "gy", None, None),
            P("gx", "gy"),
        ),
        out_specs=(P(None, "gx", "gy", None), P("gx", "gy", None, None)),
        check_vma=False,
    )
```

```python
import functools

import jax
import jax.numpy as jnp
import numpy as np
from jax import lax
from jax.experimental import pallas as pl
from jax.experimental.pallas import tpu as pltpu
from jax.sharding import PartitionSpec as P

DIRS = (
    (0, 0, 0), (1, 0, 0), (-1, 0, 0), (0, 1, 0), (0, -1, 0), (0, 0, 1), (0, 0, -1),
    (1, 1, 0), (-1, -1, 0), (1, -1, 0), (-1, 1, 0), (1, 0, 1), (-1, 0, -1),
    (1, 0, -1), (-1, 0, 1), (0, 1, 1), (0, -1, -1), (0, 1, -1), (0, -1, 1),
)
WEIGHTS = (1.0 / 3.0,) + (1.0 / 18.0,) * 6 + (1.0 / 36.0,) * 12
CUTOFF = 2.0 ** (1.0 / 3.0)
REACH = 1.125
FAR = 1.0e9
F32 = jnp.float32
BF16 = jnp.bfloat16
MESH = pl.DeviceIdType.MESH

CX, CY, NZ, SW = 8, 16, 128, 1024
ROWS = CX * CY
LANE_TILES = SW // 128

SIDES = ((-1, 0), (1, 0), (0, -1), (0, 1), (-1, -1), (-1, 1), (1, -1), (1, 1))
RANGES = ((0, 4, 7), (1, 0, 3), (2, 2, 5), (3, 6, 8), (3, 0, 1), (4, 4, 5), (5, 6, 7), (6, 2, 3), (7, 0, 1))


def facing(axis, sign):
    return [q for q in range(19) if DIRS[q][axis] == sign]


def corner_q(sx, sy):
    return DIRS.index((-sx, -sy, 0))


def split2(v):
    hi = v.astype(BF16)
    return hi, (v - hi.astype(F32)).astype(BF16)


def split3(v):
    hi = v.astype(BF16)
    rest = v - hi.astype(F32)
    mid = rest.astype(BF16)
    return hi, mid, (rest - mid.astype(F32)).astype(BF16)


def dot(a, b):
    return lax.dot_general(a, b, (((1,), (0,)), ((), ())), preferred_element_type=F32)


def dot_t(a, b):
    return lax.dot_general(a, b, (((1,), (1,)), ((), ())), preferred_element_type=F32)


def tent(d):
    return jnp.maximum(1.0 - jnp.abs(d), 0.0)


def moments(load):
    rho = None
    mom = [None, None, None]
    for q in range(19):
        f = load(q)
        rho = f if rho is None else rho + f
        for c in range(3):
            s = DIRS[q][c]
            if s:
                if mom[c] is None:
                    mom[c] = f if s > 0 else -f
                else:
                    mom[c] = mom[c] + f if s > 0 else mom[c] - f
    return rho, mom


def pair_terms(ox, oy, oz, px, py, pz):
    dx = ox - px
    dy = oy - py
    dz = oz - pz
    dz = dz - NZ * jnp.round(dz * (1.0 / NZ))
    raw = dx * dx + dy * dy + dz * dz
    inv = 1.0 / jnp.maximum(raw, 0.8)
    sixth = inv * inv * inv
    mag = (sixth + sixth - 1.0) * (sixth * inv)
    mag = jnp.where(raw < CUTOFF, mag, 0.0)
    return mag * dx, mag * dy, mag * dz


def classes(x, y, live):
    xl, xh = x < REACH, x > CX - 1 - REACH
    yl, yh = y < REACH, y > CY - 1 - REACH
    yc = jnp.where(yl, 0.0, jnp.where(yh, 2.0, 1.0))
    kind = jnp.where(xl, yc, jnp.where(xh, 6.0 - yc, jnp.where(yl, 7.0, jnp.where(yh, 3.0, 8.0))))
    return jnp.where(live > 0.0, kind, 9.0)


def sort_ranks(kind):
    masks = [(kind == k).astype(F32) for k in range(10)]
    ri = lax.broadcasted_iota(jnp.int32, (128, 256), 0)
    ci = lax.broadcasted_iota(jnp.int32, (128, 256), 1)
    upper = ((ri < ci) | (ci >= 128)).astype(F32).astype(BF16)
    pre = dot(jnp.concatenate(masks, axis=0).astype(BF16), upper)
    within, tile_sum = pre[:, :128], pre[:, 128:]
    place = lax.broadcasted_iota(jnp.int32, (80, 128), 0) & 7
    upto = tile_sum
    for by in (1, 2, 4):
        upto = upto + jnp.where(place >= by, pltpu.roll(upto, by, 0), 0.0)
    lane = lax.broadcasted_iota(jnp.int32, (1, 128), 1)
    rank = jnp.zeros((8, 128), F32)
    row = jnp.zeros((1, 128), F32)
    first = jnp.zeros((1, 128), F32)
    for k in range(10):
        cut = slice(8 * k, 8 * k + 8)
        row = jnp.where(lane == k, first, row)
        rank = rank + masks[k] * (within[cut] + (upto[cut] - tile_sum[cut]) + first)
        first = first + upto[8 * k + 7:8 * k + 8]
    return rank, row


def plane_weights(px, py, far):
    x8 = lax.broadcasted_iota(jnp.int32, (CX, 1), 0).astype(F32)
    y16 = lax.broadcasted_iota(jnp.int32, (CY, 1), 0).astype(F32)
    ki = lax.broadcasted_iota(jnp.int32, (16, 1), 0)
    ii, jj = lax.shift_right_logical(ki, 2), ki & 3
    xd = jnp.where(ii < 2, ii - 2, ii + CX - 2).astype(F32)
    yd = jnp.where(jj < 2, jj - 2, jj + CY - 2).astype(F32)
    tx, ty = tent(x8 - px), tent(y16 - py)
    parts = [tx[i:i + 1] * ty for i in range(CX)]
    parts += [tent(-1.0 - px) * ty, tent(CX - px) * ty, tent(-1.0 - py) * tx, tent(CY - py) * tx]
    parts += [tent(xd - px) * tent(yd - py)]
    if far:
        parts += [tent(-2.0 - px) * ty, tent(CX + 1.0 - px) * ty, tent(-2.0 - py) * tx, tent(CY + 1.0 - py) * tx]
    return jnp.concatenate(parts, axis=0)


def z_weights(pz):
    zi = lax.broadcasted_iota(jnp.int32, (NZ, 1), 0).astype(F32)
    return split2(tent(zi - pz))


def widen(v):
    hi, lo = split2(v)
    return jnp.concatenate([hi, lo], axis=1)


def sample(u, zh, zl):
    return dot(u, jnp.concatenate([zh, zh], axis=0)) + dot(u[:, :128], zl)


def columns(cols, at, place):
    turned = jnp.transpose(place)
    for c in range(3):
        cols[c, at:at + 128] = jnp.broadcast_to(turned[:, c:c + 1], (128, 128))


def pair_step(cols, mine, width):
    def step(n, acc):
        at = pl.multiple_of(n * 8, 8)
        p = [jnp.concatenate([cols[c, pl.ds(at, 8)]] * (width // 128), axis=1) for c in range(3)]
        return tuple(a + b for a, b in zip(acc, pair_terms(*mine, *p)))

    return step


def exchange_kernel(n_gx, n_gy, pops_hbm, anchor_hbm, offsets_hbm, heading_hbm, velocity_hbm, count,
                    pops, halo_x, halo_y, halo_c, lists, starts_out, own_out, base_out, mom, inner, zhl, plane,
                    anchor, offsets, heading, velocity, table,
                    msg_x, msg_y, msg_c, msg_l, msg_s, cols, load_sem, send_sem, recv_sem):
    gx = lax.axis_index("gx")
    gy = lax.axis_index("gy")

    def device(side):
        return (lax.rem(gx + side[0] + n_gx, n_gx), lax.rem(gy + side[1] + n_gy, n_gy))

    loads = [pltpu.make_async_copy(a, b, load_sem.at[k]) for k, (a, b) in enumerate((
        (anchor_hbm, anchor), (offsets_hbm, offsets), (heading_hbm, heading), (velocity_hbm, velocity)))]
    loads += [pltpu.make_async_copy(pops_hbm.at[pl.ds(q, n)], pops.at[pl.ds(q, n)], load_sem.at[4 + k])
              for k, (q, n) in enumerate(((0, 5), (5, 5), (10, 5), (15, 4)))]
    for c in loads:
        c.start()
    barrier = pltpu.get_barrier_semaphore()
    for side in SIDES:
        pl.semaphore_signal(barrier, inc=1, device_id=device(side), device_id_type=MESH)
    for c in loads:
        c.wait()

    root = anchor[...]
    bxf = lax.shift_right_logical(root, 7).astype(F32)
    cxf = jnp.floor(bxf * (1.0 / (CY + 2)) + 0.01)
    x = cxf - 1.0 + offsets[0:8]
    y = bxf - cxf * (CY + 2) - 1.0 + offsets[8:16]
    z = (root & (NZ - 1)).astype(F32) + offsets[16:24]
    lane = lax.broadcasted_iota(jnp.int32, (8, 128), 1)
    sub = lax.broadcasted_iota(jnp.int32, (8, 128), 0)
    live = (sub * 128 + lane < count[0, 0]).astype(F32)
    first, second = heading[pl.ds(0, 8, stride=2)], heading[pl.ds(1, 8, stride=2)]
    c1 = jnp.cos(second)
    w = [2.0 * velocity[0:8] - 0.5 * (jnp.cos(first) * c1),
         2.0 * velocity[8:16] - 0.5 * (jnp.sin(first) * c1),
         2.0 * velocity[16:24] - 0.5 * jnp.sin(second)]
    for k, v in enumerate((x, y, z, *w, live, jnp.zeros((8, 128), F32))):
        table[pl.ds(k, 8, stride=8)] = v
    rank, row = sort_ranks(classes(x, y, live))
    msg_s[...] = row
    starts_out[8] = row
    to_tile = jnp.floor(rank * (1.0 / 128.0))
    to_lane = rank - 128.0 * to_tile
    split = [v.astype(F32) for v in split3(table[...])]
    dst = lax.broadcasted_iota(jnp.int32, (128, 128), 0).astype(F32)
    ordered = jnp.zeros((24 * LANE_TILES, 128), F32)
    for t in range(0, LANE_TILES, 2):
        hot, rows = [], []
        for j in (t, t + 1):
            hot.append((dst == to_lane[j:j + 1]).astype(F32).astype(BF16))
            part = jnp.concatenate([v[8 * j:8 * j + 8] for v in split], axis=0)
            rows.append(jnp.concatenate(
                [jnp.where(to_tile[j:j + 1] == float(k), part, 0.0) for k in range(LANE_TILES)],
                axis=0).astype(BF16))
        ordered = ordered + dot_t(jnp.concatenate(rows, axis=1), jnp.concatenate(hot, axis=1))
    for t in range(LANE_TILES):
        at = 24 * t
        msg_l[t] = ordered[at:at + 8] + ordered[at + 8:at + 16] + ordered[at + 16:at + 24]

    rho, m = moments(lambda q: pops[q])
    inv = 1.0 / rho
    mom[0] = rho
    for c in range(3):
        mom[1 + c] = m[c] * inv
    for s, (adj, far) in enumerate(((0, 1), (CX - 1, CX - 2))):
        for c in range(4):
            msg_x[s, c] = mom[c, adj * CY:(adj + 1) * CY]
        for c in range(3):
            msg_x[s, 4 + c] = mom[1 + c, far * CY:(far + 1) * CY]
        for k, q in enumerate(facing(0, 2 * s - 1)):
            msg_x[s, 7 + k] = pops[q, adj * CY:(adj + 1) * CY]
    for s, (adj, far) in enumerate(((0, 1), (CY - 1, CY - 2))):
        for c in range(4):
            msg_y[s, c] = mom[c, pl.ds(adj, CX, stride=CY)]
        for c in range(3):
            msg_y[s, 4 + c] = mom[1 + c, pl.ds(far, CX, stride=CY)]
        for k, q in enumerate(facing(1, 2 * s - 1)):
            msg_y[s, 7 + k] = pops[q, pl.ds(adj, CX, stride=CY)]
    for i in range(4):
        sx, sy = SIDES[4 + i]
        ax, fx = (0, 1) if sx < 0 else (CX - 1, CX - 2)
        ay, fy = (0, 1) if sy < 0 else (CY - 1, CY - 2)
        msg_c[i] = jnp.zeros((16, 128), F32)
        for c in range(4):
            msg_c[i, c:c + 1] = mom[c, ax * CY + ay:ax * CY + ay + 1]
        for j, (nx, ny) in enumerate(((ax, fy), (fx, ay), (fx, fy))):
            for c in range(3):
                msg_c[i, 5 + 3 * j + c:6 + 3 * j + c] = mom[1 + c, nx * CY + ny:nx * CY + ny + 1]
        q = DIRS.index((sx, sy, 0))
        msg_c[i, 4:5] = pops[q, ax * CY + ay:ax * CY + ay + 1]

    def send(k, a, b, side, o):
        d = SIDES.index(side)
        return pltpu.make_async_remote_copy(
            src_ref=a, dst_ref=b, send_sem=send_sem.at[3 * d + k], recv_sem=recv_sem.at[3 * o + k],
            device_id=device(side), device_id_type=MESH)

    fluid, swimmers = [], []
    for d, side in enumerate(SIDES):
        o = SIDES.index((-side[0], -side[1]))
        if side[1] == 0:
            fluid.append(send(0, msg_x.at[d], halo_x.at[o], side, o))
        elif side[0] == 0:
            fluid.append(send(0, msg_y.at[d - 2], halo_y.at[o - 2], side, o))
        else:
            fluid.append(send(0, msg_c.at[d - 4], halo_c.at[o - 4], side, o))
        swimmers.append(send(1, msg_s, starts_out.at[o], side, o))
        swimmers.append(send(2, msg_l.at[:, pl.ds(0, 6)], lists.at[o, :, pl.ds(0, 6)], side, o))
    pl.semaphore_wait(barrier, 8)
    for c in fluid + swimmers:
        c.start()

    for c in range(3):
        inner[c * ROWS:(c + 1) * ROWS] = widen(mom[1 + c])
    for i in range(BLOCKS):
        vals = jnp.concatenate([table[16 * i:16 * i + 8], table[16 * i + 8:16 * i + 16]], axis=1)
        zh, zl = z_weights(vals[2:3])
        zhl[i, 0:NZ] = zh
        zhl[i, NZ:2 * NZ] = zl
        plane[i] = plane_weights(vals[0:1], vals[1:2], False)
        got = sample(inner[...], zh, zl)
        own_out[i] = vals
        for c in range(3):
            s = jnp.sum(got[c * ROWS:(c + 1) * ROWS] * plane[i, 0:ROWS], axis=0, keepdims=True)
            own_out[i, 3 + c:4 + c] = (vals[3 + c:4 + c] - 2.0 * s) * vals[6:7]

    for t in range(LANE_TILES):
        v = table[8 * t:8 * t + 8]
        columns(cols, t * 128, jnp.where((sub == 0) & (v[6:7] == 0.0), FAR, v))
    for i in range(0, BLOCKS, 2):
        width = 2 * BLOCK
        mine = [jnp.broadcast_to(jnp.concatenate([own_out[i, c:c + 1], own_out[i + 1, c:c + 1]], axis=1), (8, width))
                for c in range(3)]
        init = tuple(jnp.zeros((8, width), F32) for _ in range(3))
        got = lax.fori_loop(0, SW // 8, pair_step(cols, mine, width), init)
        for c in range(3):
            pairs = 0.24 * jnp.sum(got[c], axis=0, keepdims=True)
            for j in range(2):
                base_out[i + j, c:c + 1] = (pairs[:, j * BLOCK:(j + 1) * BLOCK] * own_out[i + j, 6:7]
                                            - own_out[i + j, 3 + c:4 + c])
    for i in range(BLOCKS):
        base_out[i, 3:8] = jnp.zeros((5, BLOCK), F32)

    for c in fluid + swimmers:
        c.wait()


ADJ = 64
FAR_ROWS = 48
ADJ_ROWS = ROWS + ADJ
BLOCK = 256
BLOCKS = SW // BLOCK
GHOST_TILES = 8 * LANE_TILES + 4


def fluid_kernel(pops, own, base, halo_x, halo_y, halo_c, lists, starts_in, mom, inner, zhl, plane,
                 next_out, force_out,
                 acc, out_v, starts, node, near, outer, force, ghosts, cols, out_sem, start_sem):
    start_copy = pltpu.make_async_copy(starts_in, starts, start_sem)
    start_copy.start()
    acc[...] = base[...]
    ghosts[...] = jnp.zeros(ghosts.shape, F32)
    force[...] = jnp.zeros(force.shape, F32)
    for c in range(3):
        corner = []
        for i in range(4):
            for j in range(4):
                sx, sy = (0 if i < 2 else 1), (0 if j < 2 else 1)
                fx, fy = i in (0, 3), j in (0, 3)
                k = 2 * sx + sy
                r = (11 if fy else 8) if fx else (5 if fy else 1)
                corner.append(halo_c[k, r + c:r + c + 1])
        near[c * ADJ:(c + 1) * ADJ] = widen(jnp.concatenate(
            [halo_x[0, 1 + c], halo_x[1, 1 + c], halo_y[0, 1 + c], halo_y[1, 1 + c]] + corner, axis=0))
        outer[c * FAR_ROWS:(c + 1) * FAR_ROWS] = widen(jnp.concatenate(
            [halo_x[0, 4 + c], halo_x[1, 4 + c], halo_y[0, 4 + c], halo_y[1, 4 + c]], axis=0))
    start_copy.wait()
    lane = lax.broadcasted_iota(jnp.int32, (8, 128), 1)
    sub = lax.broadcasted_iota(jnp.int32, (8, 128), 0)
    total = jnp.int32(0)
    for d, lo, hi in RANGES:
        a = starts[d, 0, lo].astype(jnp.int32)
        b = starts[d, 0, hi].astype(jnp.int32)
        sx, sy = SIDES[d]
        moved = jnp.where(sub == 0, float(sx * CX), jnp.where(sub == 1, float(sy * CY), 0.0))

        def put(t, carry, d=d, a=a, b=b, base=total, moved=moved):
            to = base - a + t * 128 + 128 * 8
            by = to & 127
            tile = lax.shift_right_logical(to, 7) - 8
            src = jnp.minimum(t, LANE_TILES - 1)
            at = t * 128 + lane
            v = jnp.where((at >= a) & (at < b), lists[d, src] + moved, 0.0)
            v = pltpu.roll(v, by, 1)
            upper = lane >= by
            low = jnp.maximum(tile, 0)
            ghosts[low] = ghosts[low] + jnp.where(upper & (tile >= 0), v, 0.0)
            ghosts[tile + 1] = ghosts[tile + 1] + jnp.where(upper, 0.0, v)
            return carry

        t0 = lax.shift_right_logical(a, 7)
        put(t0, 0)
        put(t0 + 1, 0)
        lax.fori_loop(t0 + 2, lax.shift_right_logical(b + 127, 7), put, 0)
        total = total + (b - a)

    def spread(weights, react, zz):
        zh = zz[0:NZ]
        for c in range(3):
            wh, wl = split2(weights * react[c])
            both = dot_t(wh, zz)
            force[c] = force[c] + (both[:, :128] + both[:, 128:] + dot_t(wl, zh))

    n_own = starts[8, 0, 9].astype(jnp.int32)

    def own_block(i, carry):
        zz = zhl[i]
        got = sample(near[...], zz[0:NZ], zz[NZ:2 * NZ])
        live = own[i, 6:7]
        react = []
        for c in range(3):
            s = jnp.sum(got[c * ADJ:(c + 1) * ADJ] * plane[i, ROWS:ADJ_ROWS], axis=0, keepdims=True)
            s = 2.0 * s * live
            react.append(own[i, 3 + c:4 + c] - s)
            acc[i, c:c + 1] = acc[i, c:c + 1] + s
        spread(plane[i], react, zz)
        return carry

    lax.fori_loop(0, lax.shift_right_logical(n_own + BLOCK - 1, 8), own_block, 0)
    slot = lax.broadcasted_iota(jnp.int32, (1, BLOCK), 1)

    def ghost_block(i, carry):
        vals = jnp.concatenate([ghosts[2 * i], ghosts[2 * i + 1]], axis=1)
        live = (slot + i * BLOCK < total).astype(F32)
        zh, zl = z_weights(vals[2:3])
        weights = plane_weights(vals[0:1], vals[1:2], True)
        gi = sample(inner[...], zh, zl)
        gn = sample(near[...], zh, zl)
        gf = sample(outer[...], zh, zl)
        react = []
        for c in range(3):
            s = (jnp.sum(gi[c * ROWS:(c + 1) * ROWS] * weights[0:ROWS], axis=0, keepdims=True)
                 + jnp.sum(gn[c * ADJ:(c + 1) * ADJ] * weights[ROWS:ADJ_ROWS], axis=0, keepdims=True)
                 + jnp.sum(gf[c * FAR_ROWS:(c + 1) * FAR_ROWS] * weights[ADJ_ROWS:], axis=0, keepdims=True))
            react.append((vals[3 + c:4 + c] - 2.0 * s) * live)
        spread(weights[0:ADJ_ROWS], react, jnp.concatenate([zh, zl], axis=0))
        return carry

    lax.fori_loop(0, lax.shift_right_logical(total + BLOCK - 1, 8), ghost_block, 0)

    tiles = lax.shift_right_logical(total + 127, 7)

    def ghost_columns(t, carry):
        g = jnp.where((sub == 0) & (lane + t * 128 >= total), FAR, ghosts[t])
        turned = jnp.transpose(g)
        at = pl.multiple_of(t * 128, 128)
        for c in range(3):
            cols[c, pl.ds(at, 128)] = jnp.broadcast_to(turned[:, c:c + 1], (128, 128))
        return carry

    lax.fori_loop(0, tiles, ghost_columns, 0)

    def ghost_pairs(i, carry):
        mine = [jnp.broadcast_to(own[i, c:c + 1], (8, BLOCK)) for c in range(3)]
        one = pair_step(cols, mine, BLOCK)
        init = tuple(jnp.zeros((8, BLOCK), F32) for _ in range(3))
        got = lax.fori_loop(0, lax.shift_right_logical(total + 15, 4),
                            lambda n, acc: one(2 * n + 1, one(2 * n, acc)), init)
        live = own[i, 6:7]
        for c in range(3):
            acc[i, c:c + 1] = acc[i, c:c + 1] + 0.24 * live * jnp.sum(got[c], axis=0, keepdims=True)
        return carry

    lax.fori_loop(0, lax.shift_right_logical(n_own + BLOCK - 1, 8), ghost_pairs, 0)
    for i in range(BLOCKS):
        for c in range(3):
            for j in range(2):
                r = c * LANE_TILES + 2 * i + j
                force_out[r:r + 1] = acc[i, c:c + 1, j * 128:(j + 1) * 128]

    def prepare(rho, u0, half, g):
        u = [u0[c] + half * g[c] for c in range(3)]
        uu = u[0] * u[0] + u[1] * u[1] + u[2] * u[2]
        ug = u[0] * g[0] + u[1] * g[1] + u[2] * g[2]
        k0 = 1.25 * rho * (1.0 - 1.5 * uu) - 1.125 * ug
        return k0, 3.75 * rho, 5.625 * rho, u, [1.125 * v for v in g]

    def along(q, v):
        out = None
        for c in range(3):
            s = DIRS[q][c]
            if s:
                out = (v[c] if s > 0 else -v[c]) if out is None else (out + v[c] if s > 0 else out - v[c])
        return out

    def post(q, f, prep):
        k0, r1, r2, u, g = prep
        if q == 0:
            return -0.25 * f + WEIGHTS[0] * k0
        a, p = along(q, u), along(q, g)
        return -0.25 * f + WEIGHTS[q] * (k0 + a * (r1 + r2 * a + 3.0 * p) + p)

    def side_prep(rho, u0, lo, n):
        g = [force[c, lo:lo + n] for c in range(3)]
        return prepare(rho, u0, 0.5 / rho, g)

    k0, r1, r2, u, g = side_prep(mom[0], [mom[1 + c] for c in range(3)], 0, ROWS)
    node[0] = k0
    for c in range(3):
        node[1 + c] = u[c]
        node[4 + c] = g[c]
    xs = [side_prep(halo_x[s, 0], [halo_x[s, 1 + c] for c in range(3)], ROWS + s * CY, CY) for s in range(2)]
    ys = [side_prep(halo_y[s, 0], [halo_y[s, 1 + c] for c in range(3)], ROWS + 2 * CY + s * CX, CX)
          for s in range(2)]
    cs = []
    for i in range(4):
        sx, sy = SIDES[4 + i]
        r = ADJ_ROWS - 16 + (1 if sx < 0 else 2) * 4 + (1 if sy < 0 else 2)
        cs.append(side_prep(halo_c[i, 0:1], [halo_c[i, 1 + c:2 + c] for c in range(3)], r, 1))
    stores = []
    for q in range(19):
        dx, dy, dz = DIRS[q]
        rho_q = mom[0]
        prep = (node[0], 3.75 * rho_q, 5.625 * rho_q, [node[1 + c] for c in range(3)], [node[4 + c] for c in range(3)])

        def turned(v, dz=dz):
            return pltpu.roll(v, dz % NZ, 1) if dz else v

        v = turned(post(q, pops[q], prep))
        if dy:
            v = pltpu.roll(v, dy % ROWS, 0)
        if dx == 0:
            out_v[q] = v
        else:
            s = 0 if dx > 0 else 1
            e = turned(post(q, halo_x[s, 7 + facing(0, dx).index(q)], xs[s]))
            if dy:
                e = pltpu.roll(e, dy % CY, 0)
            if dx > 0:
                out_v[q, CY:ROWS] = v[0:ROWS - CY]
                out_v[q, 0:CY] = e
            else:
                out_v[q, 0:ROWS - CY] = v[CY:ROWS]
                out_v[q, ROWS - CY:ROWS] = e
        if dy:
            s = 0 if dy > 0 else 1
            at = 0 if dy > 0 else CY - 1
            e = turned(post(q, halo_y[s, 7 + facing(1, dy).index(q)], ys[s]))
            if dx:
                e = pltpu.roll(e, dx % CX, 0)
            out_v[q, pl.ds(at, CX, stride=CY)] = e
            if dx:
                i = SIDES.index((-dx, -dy)) - 4
                r = at + (0 if dx > 0 else (CX - 1) * CY)
                out_v[q, r:r + 1] = post(q, halo_c[i, 4:5], cs[i])
        c = pltpu.make_async_copy(out_v.at[q], next_out.at[q], out_sem.at[q])
        c.start()
        stores.append(c)
    for c in stores:
        c.wait()


def body(n_gx, n_gy, populations, anchor, offsets, heading, velocity, live_count):
    pops = populations.reshape(19, ROWS, NZ)
    tiles = LANE_TILES
    vmem = pl.BlockSpec(memory_space=pltpu.VMEM)
    hbm = pl.BlockSpec(memory_space=pltpu.HBM)
    dma = pltpu.SemaphoreType.DMA
    held = (
        pltpu.VMEM((19, ROWS, NZ), F32),
        pltpu.VMEM((2, 12, CY, 128), F32),
        pltpu.VMEM((2, 12, CX, 128), F32),
        pltpu.VMEM((4, 16, 128), F32),
        pltpu.VMEM((8, LANE_TILES, 8, 128), F32),
        pltpu.VMEM((9, 1, 128), F32),
        pltpu.VMEM((BLOCKS, 8, BLOCK), F32),
        pltpu.VMEM((BLOCKS, 8, BLOCK), F32),
        pltpu.VMEM((4, ROWS, NZ), F32),
        pltpu.VMEM((3 * ROWS, 2 * NZ), BF16),
        pltpu.VMEM((BLOCKS, 2 * NZ, BLOCK), BF16),
        pltpu.VMEM((BLOCKS, ADJ_ROWS, BLOCK), F32),
    )
    pops, halo_x, halo_y, halo_c, lists, starts, own, base, mom, inner, zhl, plane = pl.pallas_call(
        functools.partial(exchange_kernel, n_gx, n_gy),
        out_shape=held,
        in_specs=[hbm] * 5 + [pl.BlockSpec(memory_space=pltpu.SMEM)],
        out_specs=[vmem] * 12,
        scratch_shapes=[
            pltpu.VMEM((tiles, 128), jnp.int32),
            pltpu.VMEM((3 * tiles, 128), F32),
            pltpu.VMEM((2 * tiles, 128), F32),
            pltpu.VMEM((3 * tiles, 128), F32),
            pltpu.VMEM((8 * tiles, 128), F32),
            pltpu.VMEM((2, 12, CY, 128), F32),
            pltpu.VMEM((2, 12, CX, 128), F32),
            pltpu.VMEM((4, 16, 128), F32),
            pltpu.VMEM((LANE_TILES, 8, 128), F32),
            pltpu.VMEM((1, 128), F32),
            pltpu.VMEM((3, SW, 128), F32),
            dma((8,)), dma((24,)), dma((24,)),
        ],
        compiler_params=pltpu.CompilerParams(collective_id=0, has_side_effects=True, vmem_limit_bytes=20 << 20),
        name="exchange",
    )(*[pltpu.with_memory_space_constraint(v, pltpu.HBM) for v in (
        pops, anchor.reshape(tiles, 128), offsets.reshape(3 * tiles, 128),
        jnp.swapaxes(heading.reshape(2, tiles, 128), 0, 1).reshape(2 * tiles, 128),
        velocity.reshape(3 * tiles, 128))], live_count)
    moved, force = pl.pallas_call(
        fluid_kernel,
        out_shape=(jax.ShapeDtypeStruct((19, ROWS, NZ), F32), jax.ShapeDtypeStruct((3 * tiles, 128), F32)),
        in_specs=[vmem] * 12,
        out_specs=[hbm, vmem],
        scratch_shapes=[
            pltpu.VMEM((BLOCKS, 8, BLOCK), F32),
            pltpu.VMEM((19, ROWS, NZ), F32),
            pltpu.SMEM((9, 1, 128), F32),
            pltpu.VMEM((7, ROWS, NZ), F32),
            pltpu.VMEM((3 * ADJ, 2 * NZ), BF16),
            pltpu.VMEM((3 * FAR_ROWS, 2 * NZ), BF16),
            pltpu.VMEM((3, ADJ_ROWS, NZ), F32),
            pltpu.VMEM((GHOST_TILES, 8, 128), F32),
            pltpu.VMEM((3, GHOST_TILES * 128, 128), F32),
            dma((19,)), dma,
        ],
        compiler_params=pltpu.CompilerParams(vmem_limit_bytes=32 << 20),
        name="fluid",
    )(pops, own, base, halo_x, halo_y, halo_c, lists, starts, mom, inner, zhl, plane)
    return (moved.reshape(populations.shape), force.reshape(1, 1, 3, SW))


def solution(mesh):
    return jax.shard_map(
        functools.partial(body, mesh.shape["gx"], mesh.shape["gy"]),
        mesh=mesh,
        in_specs=(
            P(None, "gx", "gy", None),
            P("gx", "gy", None),
            P("gx", "gy", None, None),
            P("gx", "gy", None, None),
            P("gx", "gy", None, None),
            P("gx", "gy"),
        ),
        out_specs=(P(None, "gx", "gy", None), P("gx", "gy", None, None)),
        check_vma=False,
    )
```

```python
import functools

import jax
import jax.numpy as jnp
import numpy as np
from jax import lax
from jax.experimental import pallas as pl
from jax.experimental.pallas import tpu as pltpu
from jax.sharding import PartitionSpec as P

DIRS = (
    (0, 0, 0), (1, 0, 0), (-1, 0, 0), (0, 1, 0), (0, -1, 0), (0, 0, 1), (0, 0, -1),
    (1, 1, 0), (-1, -1, 0), (1, -1, 0), (-1, 1, 0), (1, 0, 1), (-1, 0, -1),
    (1, 0, -1), (-1, 0, 1), (0, 1, 1), (0, -1, -1), (0, 1, -1), (0, -1, 1),
)
WEIGHTS = (1.0 / 3.0,) + (1.0 / 18.0,) * 6 + (1.0 / 36.0,) * 12
CUTOFF = 2.0 ** (1.0 / 3.0)
REACH = 1.125
FAR = 1.0e9
F32 = jnp.float32
BF16 = jnp.bfloat16
MESH = pl.DeviceIdType.MESH

CX, CY, NZ, SW = 8, 16, 128, 1024
ROWS = CX * CY
LANE_TILES = SW // 128

SIDES = ((-1, 0), (1, 0), (0, -1), (0, 1), (-1, -1), (-1, 1), (1, -1), (1, 1))
RANGES = ((0, 4, 7), (1, 0, 3), (2, 2, 5), (3, 6, 8), (3, 0, 1), (4, 4, 5), (5, 6, 7), (6, 2, 3), (7, 0, 1))


def facing(axis, sign):
    return [q for q in range(19) if DIRS[q][axis] == sign]


def corner_q(sx, sy):
    return DIRS.index((-sx, -sy, 0))


def split2(v):
    hi = v.astype(BF16)
    return hi, (v - hi.astype(F32)).astype(BF16)


def split3(v):
    hi = v.astype(BF16)
    rest = v - hi.astype(F32)
    mid = rest.astype(BF16)
    return hi, mid, (rest - mid.astype(F32)).astype(BF16)


def dot(a, b):
    return lax.dot_general(a, b, (((1,), (0,)), ((), ())), preferred_element_type=F32)


def dot_t(a, b):
    return lax.dot_general(a, b, (((1,), (1,)), ((), ())), preferred_element_type=F32)


def tent(d):
    return jnp.maximum(1.0 - jnp.abs(d), 0.0)


def moments(load):
    rho = None
    mom = [None, None, None]
    for q in range(19):
        f = load(q)
        rho = f if rho is None else rho + f
        for c in range(3):
            s = DIRS[q][c]
            if s:
                if mom[c] is None:
                    mom[c] = f if s > 0 else -f
                else:
                    mom[c] = mom[c] + f if s > 0 else mom[c] - f
    return rho, mom


def pair_terms(ox, oy, oz, px, py, pz):
    dx = ox - px
    dy = oy - py
    dz = oz - pz
    dz = dz - NZ * jnp.round(dz * (1.0 / NZ))
    raw = dx * dx + dy * dy + dz * dz
    inv = 1.0 / jnp.maximum(raw, 0.8)
    sixth = inv * inv * inv
    mag = (sixth + sixth - 1.0) * (sixth * inv)
    mag = jnp.where(raw < CUTOFF, mag, 0.0)
    return mag * dx, mag * dy, mag * dz


def classes(x, y, live):
    xl, xh = x < REACH, x > CX - 1 - REACH
    yl, yh = y < REACH, y > CY - 1 - REACH
    yc = jnp.where(yl, 0.0, jnp.where(yh, 2.0, 1.0))
    kind = jnp.where(xl, yc, jnp.where(xh, 6.0 - yc, jnp.where(yl, 7.0, jnp.where(yh, 3.0, 8.0))))
    return jnp.where(live > 0.0, kind, 9.0)


def sort_ranks(kind):
    masks = [(kind == k).astype(F32) for k in range(10)]
    ri = lax.broadcasted_iota(jnp.int32, (128, 256), 0)
    ci = lax.broadcasted_iota(jnp.int32, (128, 256), 1)
    upper = ((ri < ci) | (ci >= 128)).astype(F32).astype(BF16)
    pre = dot(jnp.concatenate(masks, axis=0).astype(BF16), upper)
    within, tile_sum = pre[:, :128], pre[:, 128:]
    place = lax.broadcasted_iota(jnp.int32, (80, 128), 0) & 7
    upto = tile_sum
    for by in (1, 2, 4):
        upto = upto + jnp.where(place >= by, pltpu.roll(upto, by, 0), 0.0)
    lane = lax.broadcasted_iota(jnp.int32, (1, 128), 1)
    rank = jnp.zeros((8, 128), F32)
    row = jnp.zeros((1, 128), F32)
    first = jnp.zeros((1, 128), F32)
    for k in range(10):
        cut = slice(8 * k, 8 * k + 8)
        row = jnp.where(lane == k, first, row)
        rank = rank + masks[k] * (within[cut] + (upto[cut] - tile_sum[cut]) + first)
        first = first + upto[8 * k + 7:8 * k + 8]
    return rank, row


def plane_weights(px, py, far):
    x8 = lax.broadcasted_iota(jnp.int32, (CX, 1), 0).astype(F32)
    y16 = lax.broadcasted_iota(jnp.int32, (CY, 1), 0).astype(F32)
    ki = lax.broadcasted_iota(jnp.int32, (16, 1), 0)
    ii, jj = lax.shift_right_logical(ki, 2), ki & 3
    xd = jnp.where(ii < 2, ii - 2, ii + CX - 2).astype(F32)
    yd = jnp.where(jj < 2, jj - 2, jj + CY - 2).astype(F32)
    tx, ty = tent(x8 - px), tent(y16 - py)
    parts = [tx[i:i + 1] * ty for i in range(CX)]
    parts += [tent(-1.0 - px) * ty, tent(CX - px) * ty, tent(-1.0 - py) * tx, tent(CY - py) * tx]
    parts += [tent(xd - px) * tent(yd - py)]
    if far:
        parts += [tent(-2.0 - px) * ty, tent(CX + 1.0 - px) * ty, tent(-2.0 - py) * tx, tent(CY + 1.0 - py) * tx]
    return jnp.concatenate(parts, axis=0)


def z_weights(pz):
    zi = lax.broadcasted_iota(jnp.int32, (NZ, 1), 0).astype(F32)
    return split2(tent(zi - pz))


def widen(v):
    hi, lo = split2(v)
    return jnp.concatenate([hi, lo], axis=1)


def sample(u, zh, zl):
    return dot(u, jnp.concatenate([zh, zh], axis=0)) + dot(u[:, :128], zl)


def columns(cols, at, place):
    turned = jnp.transpose(place)
    for c in range(3):
        cols[c, at:at + 128] = jnp.broadcast_to(turned[:, c:c + 1], (128, 128))


def pair_step(cols, mine, width):
    def step(n, acc):
        at = pl.multiple_of(n * 8, 8)
        p = [jnp.concatenate([cols[c, pl.ds(at, 8)]] * (width // 128), axis=1) for c in range(3)]
        return tuple(a + b for a, b in zip(acc, pair_terms(*mine, *p)))

    return step


def exchange_kernel(n_gx, n_gy, pops_hbm, anchor_hbm, offsets_hbm, heading_hbm, velocity_hbm, count_hbm,
                    pops, halo_x, halo_y, halo_c, lists, starts_out, own_out, base_out, mom, inner, zhl, plane,
                    anchor, offsets, heading, velocity, count, table,
                    msg_x, msg_y, msg_c, msg_l, msg_s, cols, load_sem, send_sem, recv_sem):
    gx = lax.axis_index("gx")
    gy = lax.axis_index("gy")

    def device(side):
        return (lax.rem(gx + side[0] + n_gx, n_gx), lax.rem(gy + side[1] + n_gy, n_gy))

    loads = [pltpu.make_async_copy(a, b, load_sem.at[k]) for k, (a, b) in enumerate((
        (anchor_hbm, anchor), (offsets_hbm, offsets), (heading_hbm, heading), (velocity_hbm, velocity),
        (count_hbm, count)))]
    loads += [pltpu.make_async_copy(pops_hbm.at[pl.ds(q, n)], pops.at[pl.ds(q, n)], load_sem.at[5 + k])
              for k, (q, n) in enumerate(((0, 5), (5, 5), (10, 5), (15, 4)))]
    for c in loads:
        c.start()
    barrier = pltpu.get_barrier_semaphore()
    for side in SIDES:
        pl.semaphore_signal(barrier, inc=1, device_id=device(side), device_id_type=MESH)
    for c in loads:
        c.wait()

    root = anchor[...]
    bxf = lax.shift_right_logical(root, 7).astype(F32)
    cxf = jnp.floor(bxf * (1.0 / (CY + 2)) + 0.01)
    x = cxf - 1.0 + offsets[0:8]
    y = bxf - cxf * (CY + 2) - 1.0 + offsets[8:16]
    z = (root & (NZ - 1)).astype(F32) + offsets[16:24]
    lane = lax.broadcasted_iota(jnp.int32, (8, 128), 1)
    sub = lax.broadcasted_iota(jnp.int32, (8, 128), 0)
    live = (sub * 128 + lane < count[0]).astype(F32)
    first, second = heading[pl.ds(0, 8, stride=2)], heading[pl.ds(1, 8, stride=2)]
    c1 = jnp.cos(second)
    w = [2.0 * velocity[0:8] - 0.5 * (jnp.cos(first) * c1),
         2.0 * velocity[8:16] - 0.5 * (jnp.sin(first) * c1),
         2.0 * velocity[16:24] - 0.5 * jnp.sin(second)]
    for k, v in enumerate((x, y, z, *w, live, jnp.zeros((8, 128), F32))):
        table[pl.ds(k, 8, stride=8)] = v
    rank, row = sort_ranks(classes(x, y, live))
    msg_s[...] = row
    starts_out[8] = row
    to_tile = jnp.floor(rank * (1.0 / 128.0))
    to_lane = rank - 128.0 * to_tile
    split = [v.astype(F32) for v in split3(table[...])]
    dst = lax.broadcasted_iota(jnp.int32, (128, 128), 0).astype(F32)
    ordered = jnp.zeros((24 * LANE_TILES, 128), F32)
    for t in range(0, LANE_TILES, 2):
        hot, rows = [], []
        for j in (t, t + 1):
            hot.append((dst == to_lane[j:j + 1]).astype(F32).astype(BF16))
            part = jnp.concatenate([v[8 * j:8 * j + 8] for v in split], axis=0)
            rows.append(jnp.concatenate(
                [jnp.where(to_tile[j:j + 1] == float(k), part, 0.0) for k in range(LANE_TILES)],
                axis=0).astype(BF16))
        ordered = ordered + dot_t(jnp.concatenate(rows, axis=1), jnp.concatenate(hot, axis=1))
    for t in range(LANE_TILES):
        at = 24 * t
        msg_l[t] = ordered[at:at + 8] + ordered[at + 8:at + 16] + ordered[at + 16:at + 24]

    rho, m = moments(lambda q: pops[q])
    inv = 1.0 / rho
    mom[0] = rho
    for c in range(3):
        mom[1 + c] = m[c] * inv
    for s, (adj, far) in enumerate(((0, 1), (CX - 1, CX - 2))):
        for c in range(4):
            msg_x[s, c] = mom[c, adj * CY:(adj + 1) * CY]
        for c in range(3):
            msg_x[s, 4 + c] = mom[1 + c, far * CY:(far + 1) * CY]
        for k, q in enumerate(facing(0, 2 * s - 1)):
            msg_x[s, 7 + k] = pops[q, adj * CY:(adj + 1) * CY]
    for s, (adj, far) in enumerate(((0, 1), (CY - 1, CY - 2))):
        for c in range(4):
            msg_y[s, c] = mom[c, pl.ds(adj, CX, stride=CY)]
        for c in range(3):
            msg_y[s, 4 + c] = mom[1 + c, pl.ds(far, CX, stride=CY)]
        for k, q in enumerate(facing(1, 2 * s - 1)):
            msg_y[s, 7 + k] = pops[q, pl.ds(adj, CX, stride=CY)]
    for i in range(4):
        sx, sy = SIDES[4 + i]
        ax, fx = (0, 1) if sx < 0 else (CX - 1, CX - 2)
        ay, fy = (0, 1) if sy < 0 else (CY - 1, CY - 2)
        msg_c[i] = jnp.zeros((16, 128), F32)
        for c in range(4):
            msg_c[i, c:c + 1] = mom[c, ax * CY + ay:ax * CY + ay + 1]
        for j, (nx, ny) in enumerate(((ax, fy), (fx, ay), (fx, fy))):
            for c in range(3):
                msg_c[i, 5 + 3 * j + c:6 + 3 * j + c] = mom[1 + c, nx * CY + ny:nx * CY + ny + 1]
        q = DIRS.index((sx, sy, 0))
        msg_c[i, 4:5] = pops[q, ax * CY + ay:ax * CY + ay + 1]

    def send(k, a, b, side, o):
        d = SIDES.index(side)
        return pltpu.make_async_remote_copy(
            src_ref=a, dst_ref=b, send_sem=send_sem.at[3 * d + k], recv_sem=recv_sem.at[3 * o + k],
            device_id=device(side), device_id_type=MESH)

    fluid, swimmers = [], []
    for d, side in enumerate(SIDES):
        o = SIDES.index((-side[0], -side[1]))
        if side[1] == 0:
            fluid.append(send(0, msg_x.at[d], halo_x.at[o], side, o))
        elif side[0] == 0:
            fluid.append(send(0, msg_y.at[d - 2], halo_y.at[o - 2], side, o))
        else:
            fluid.append(send(0, msg_c.at[d - 4], halo_c.at[o - 4], side, o))
        swimmers.append(send(1, msg_s, starts_out.at[o], side, o))
        swimmers.append(send(2, msg_l.at[:, pl.ds(0, 6)], lists.at[o, :, pl.ds(0, 6)], side, o))
    pl.semaphore_wait(barrier, 8)
    for c in fluid + swimmers:
        c.start()

    for c in range(3):
        inner[c * ROWS:(c + 1) * ROWS] = widen(mom[1 + c])
    for i in range(BLOCKS):
        n = BLOCK // 128
        vals = jnp.concatenate([table[8 * (n * i + j):8 * (n * i + j) + 8] for j in range(n)], axis=1)
        zh, zl = z_weights(vals[2:3])
        zhl[i, 0:NZ] = zh
        zhl[i, NZ:2 * NZ] = zl
        plane[i] = plane_weights(vals[0:1], vals[1:2], False)
        got = sample(inner[...], zh, zl)
        rows = [vals[0:3]]
        for c in range(3):
            s = jnp.sum(got[c * ROWS:(c + 1) * ROWS] * plane[i, 0:ROWS], axis=0, keepdims=True)
            rows.append((vals[3 + c:4 + c] - 2.0 * s) * vals[6:7])
        rows = jnp.concatenate(rows + [vals[6:8]], axis=0)
        for j in range(BLOCK // OWN):
            own_out[i * (BLOCK // OWN) + j] = rows[:, j * OWN:(j + 1) * OWN]

    for t in range(LANE_TILES):
        v = table[8 * t:8 * t + 8]
        columns(cols, t * 128, jnp.where((sub == 0) & (v[6:7] == 0.0), FAR, v))
    for i in range(0, SW // OWN, 2):
        width = 2 * OWN
        mine = [jnp.broadcast_to(jnp.concatenate([own_out[i, c:c + 1], own_out[i + 1, c:c + 1]], axis=1), (8, width))
                for c in range(3)]
        init = tuple(jnp.zeros((8, width), F32) for _ in range(3))
        got = lax.fori_loop(0, SW // 8, pair_step(cols, mine, width), init)
        for c in range(3):
            pairs = 0.24 * jnp.sum(got[c], axis=0, keepdims=True)
            for j in range(2):
                base_out[i + j, c:c + 1] = (pairs[:, j * OWN:(j + 1) * OWN] * own_out[i + j, 6:7]
                                            - own_out[i + j, 3 + c:4 + c])
    for i in range(SW // OWN):
        base_out[i, 3:8] = jnp.zeros((5, OWN), F32)

    for c in fluid + swimmers:
        c.wait()


ADJ = 64
FAR_ROWS = 48
ADJ_ROWS = ROWS + ADJ
BLOCK = 512
BLOCKS = SW // BLOCK
OWN = 256
GHOST_TILES = 8 * LANE_TILES + 4


def fluid_kernel(pops, own, base, halo_x, halo_y, halo_c, lists, starts_in, mom, inner, zhl, plane,
                 next_out, force_out,
                 acc, out_v, force_v, starts, node, near, outer, force, ghosts, cols, out_sem, start_sem, force_sem):
    start_copy = pltpu.make_async_copy(starts_in, starts, start_sem)
    start_copy.start()
    acc[...] = base[...]
    ghosts[...] = jnp.zeros(ghosts.shape, F32)
    force[...] = jnp.zeros(force.shape, F32)
    for c in range(3):
        corner = []
        for i in range(4):
            for j in range(4):
                sx, sy = (0 if i < 2 else 1), (0 if j < 2 else 1)
                fx, fy = i in (0, 3), j in (0, 3)
                k = 2 * sx + sy
                r = (11 if fy else 8) if fx else (5 if fy else 1)
                corner.append(halo_c[k, r + c:r + c + 1])
        near[c * ADJ:(c + 1) * ADJ] = widen(jnp.concatenate(
            [halo_x[0, 1 + c], halo_x[1, 1 + c], halo_y[0, 1 + c], halo_y[1, 1 + c]] + corner, axis=0))
        outer[c * FAR_ROWS:(c + 1) * FAR_ROWS] = widen(jnp.concatenate(
            [halo_x[0, 4 + c], halo_x[1, 4 + c], halo_y[0, 4 + c], halo_y[1, 4 + c]], axis=0))

    def spread(weights, react, zz):
        zh = zz[0:NZ]
        for c in range(3):
            wh, wl = split2(weights * react[c])
            both = dot_t(wh, zz)
            force[c] = force[c] + (both[:, :128] + both[:, 128:] + dot_t(wl, zh))

    per = BLOCK // OWN

    def own_block(i, carry):
        zz = zhl[i]
        got = sample(near[...], zz[0:NZ], zz[NZ:2 * NZ])
        vals = jnp.concatenate([own[per * i + j] for j in range(per)], axis=1)
        react = []
        for c in range(3):
            s = jnp.sum(got[c * ADJ:(c + 1) * ADJ] * plane[i, ROWS:ADJ_ROWS], axis=0, keepdims=True)
            s = 2.0 * s * vals[6:7]
            react.append(vals[3 + c:4 + c] - s)
            for j in range(per):
                acc[per * i + j, c:c + 1] = acc[per * i + j, c:c + 1] + s[:, j * OWN:(j + 1) * OWN]
        spread(plane[i], react, zz)
        return carry

    own_block(0, 0)
    start_copy.wait()
    n_own = starts[8, 0, 9].astype(jnp.int32)

    lane = lax.broadcasted_iota(jnp.int32, (8, 128), 1)
    sub = lax.broadcasted_iota(jnp.int32, (8, 128), 0)
    total = jnp.int32(0)
    puts, rest = [], []
    for d, lo, hi in RANGES:
        a = starts[d, 0, lo].astype(jnp.int32)
        b = starts[d, 0, hi].astype(jnp.int32)
        sx, sy = SIDES[d]
        moved = jnp.where(sub == 0, float(sx * CX), jnp.where(sub == 1, float(sy * CY), 0.0))
        by = (total - a) & 127
        upper = lane >= by

        def taken(t, d=d, a=a, b=b, by=by, moved=moved):
            at = t * 128 + lane
            v = jnp.where((at >= a) & (at < b), lists[d, jnp.minimum(t, LANE_TILES - 1)] + moved, 0.0)
            return pltpu.roll(v, by, 1)

        t0 = lax.shift_right_logical(a, 7)
        tile = lax.shift_right_logical(total - a + t0 * 128 + 1024, 7) - 8
        v0, v1 = taken(t0), taken(t0 + 1)
        puts.append((jnp.maximum(tile, 0), jnp.where(upper, v0, 0.0)))
        puts.append((tile + 1, jnp.where(upper, v1, v0)))
        puts.append((tile + 2, jnp.where(upper, 0.0, v1)))

        def more(t, carry, taken=taken, upper=upper, shift=tile - t0):
            v = taken(t)
            ghosts[t + shift] = ghosts[t + shift] + jnp.where(upper, v, 0.0)
            ghosts[t + shift + 1] = ghosts[t + shift + 1] + jnp.where(upper, 0.0, v)
            return carry

        rest.append((t0 + 2, lax.shift_right_logical(b + 127, 7), more))
        total = total + (b - a)
    for at, v in puts:
        ghosts[at] = ghosts[at] + v
    for lo, hi, more in rest:
        lax.fori_loop(lo, hi, more, 0)

    slot = lax.broadcasted_iota(jnp.int32, (1, BLOCK), 1)
    tiles = lax.shift_right_logical(total + 127, 7)
    ahead = BLOCK // 128

    def ghost_columns(t, carry):
        g = jnp.where((sub == 0) & (lane + t * 128 >= total), FAR, ghosts[t])
        turned = jnp.transpose(g)
        at = t * 128 if isinstance(t, int) else pl.multiple_of(t * 128, 128)
        for c in range(3):
            cols[c, pl.ds(at, 128)] = jnp.broadcast_to(turned[:, c:c + 1], (128, 128))
        return carry

    def ghost_block(i, carry):
        vals = jnp.concatenate([ghosts[ahead * i + j] for j in range(ahead)], axis=1)
        live = (slot + i * BLOCK < total).astype(F32)
        zh, zl = z_weights(vals[2:3])
        weights = plane_weights(vals[0:1], vals[1:2], True)
        gi = sample(inner[...], zh, zl)
        gn = sample(near[...], zh, zl)
        gf = sample(outer[...], zh, zl)
        react = []
        for c in range(3):
            s = (jnp.sum(gi[c * ROWS:(c + 1) * ROWS] * weights[0:ROWS], axis=0, keepdims=True)
                 + jnp.sum(gn[c * ADJ:(c + 1) * ADJ] * weights[ROWS:ADJ_ROWS], axis=0, keepdims=True)
                 + jnp.sum(gf[c * FAR_ROWS:(c + 1) * FAR_ROWS] * weights[ADJ_ROWS:], axis=0, keepdims=True))
            react.append((vals[3 + c:4 + c] - 2.0 * s) * live)
        spread(weights[0:ADJ_ROWS], react, jnp.concatenate([zh, zl], axis=0))
        return carry

    for t in range(ahead):
        ghost_columns(t, 0)
    ghost_block(0, 0)
    lax.fori_loop(ahead, tiles, ghost_columns, 0)
    lax.fori_loop(1, lax.shift_right_logical(total + BLOCK - 1, 9), ghost_block, 0)
    lax.fori_loop(1, lax.shift_right_logical(n_own + BLOCK - 1, 9), own_block, 0)

    def ghost_pairs(i, carry):
        mine = [jnp.broadcast_to(own[i, c:c + 1], (8, OWN)) for c in range(3)]
        one = pair_step(cols, mine, OWN)
        init = tuple(jnp.zeros((8, OWN), F32) for _ in range(3))

        def four(n, got):
            for k in range(4):
                got = one(4 * n + k, got)
            return got

        got = lax.fori_loop(0, lax.shift_right_logical(total + 31, 5), four, init)
        live = own[i, 6:7]
        for c in range(3):
            acc[i, c:c + 1] = acc[i, c:c + 1] + 0.24 * live * jnp.sum(got[c], axis=0, keepdims=True)
        return carry

    lax.fori_loop(0, lax.shift_right_logical(n_own + OWN - 1, 8), ghost_pairs, 0)
    for i in range(SW // OWN):
        for c in range(3):
            for j in range(2):
                r = c * LANE_TILES + 2 * i + j
                force_v[r:r + 1] = acc[i, c:c + 1, j * 128:(j + 1) * 128]
    force_copy = pltpu.make_async_copy(force_v, force_out, force_sem)
    force_copy.start()

    def prepare(rho, u0, half, g):
        u = [u0[c] + half * g[c] for c in range(3)]
        uu = u[0] * u[0] + u[1] * u[1] + u[2] * u[2]
        ug = u[0] * g[0] + u[1] * g[1] + u[2] * g[2]
        k0 = 1.25 * rho * (1.0 - 1.5 * uu) - 1.125 * ug
        return k0, 3.75 * rho, 5.625 * rho, u, [1.125 * v for v in g]

    def along(q, v):
        out = None
        for c in range(3):
            s = DIRS[q][c]
            if s:
                out = (v[c] if s > 0 else -v[c]) if out is None else (out + v[c] if s > 0 else out - v[c])
        return out

    def post(q, f, prep):
        k0, r1, r2, u, g = prep
        if q == 0:
            return -0.25 * f + WEIGHTS[0] * k0
        a, p = along(q, u), along(q, g)
        return -0.25 * f + WEIGHTS[q] * (k0 + a * (r1 + r2 * a + 3.0 * p) + p)

    def side_prep(rho, u0, lo, n):
        g = [force[c, lo:lo + n] for c in range(3)]
        return prepare(rho, u0, 0.5 / rho, g)

    k0, r1, r2, u, g = side_prep(mom[0], [mom[1 + c] for c in range(3)], 0, ROWS)
    node[0] = k0
    for c in range(3):
        node[1 + c] = u[c]
        node[4 + c] = g[c]
    xs = [side_prep(halo_x[s, 0], [halo_x[s, 1 + c] for c in range(3)], ROWS + s * CY, CY) for s in range(2)]
    ys = [side_prep(halo_y[s, 0], [halo_y[s, 1 + c] for c in range(3)], ROWS + 2 * CY + s * CX, CX)
          for s in range(2)]
    cs = []
    for i in range(4):
        sx, sy = SIDES[4 + i]
        r = ADJ_ROWS - 16 + (1 if sx < 0 else 2) * 4 + (1 if sy < 0 else 2)
        cs.append(side_prep(halo_c[i, 0:1], [halo_c[i, 1 + c:2 + c] for c in range(3)], r, 1))
    stores = []
    for q in range(19):
        dx, dy, dz = DIRS[q]
        rho_q = mom[0]
        prep = (node[0], 3.75 * rho_q, 5.625 * rho_q, [node[1 + c] for c in range(3)], [node[4 + c] for c in range(3)])

        def turned(v, dz=dz):
            return pltpu.roll(v, dz % NZ, 1) if dz else v

        v = turned(post(q, pops[q], prep))
        if dy:
            v = pltpu.roll(v, dy % ROWS, 0)
        if dx == 0:
            out_v[q] = v
        else:
            s = 0 if dx > 0 else 1
            e = turned(post(q, halo_x[s, 7 + facing(0, dx).index(q)], xs[s]))
            if dy:
                e = pltpu.roll(e, dy % CY, 0)
            if dx > 0:
                out_v[q, CY:ROWS] = v[0:ROWS - CY]
                out_v[q, 0:CY] = e
            else:
                out_v[q, 0:ROWS - CY] = v[CY:ROWS]
                out_v[q, ROWS - CY:ROWS] = e
        if dy:
            s = 0 if dy > 0 else 1
            at = 0 if dy > 0 else CY - 1
            e = turned(post(q, halo_y[s, 7 + facing(1, dy).index(q)], ys[s]))
            if dx:
                e = pltpu.roll(e, dx % CX, 0)
            out_v[q, pl.ds(at, CX, stride=CY)] = e
            if dx:
                i = SIDES.index((-dx, -dy)) - 4
                r = at + (0 if dx > 0 else (CX - 1) * CY)
                out_v[q, r:r + 1] = post(q, halo_c[i, 4:5], cs[i])
        c = pltpu.make_async_copy(out_v.at[q], next_out.at[q], out_sem.at[q])
        c.start()
        stores.append(c)
    force_copy.wait()
    for c in stores:
        c.wait()


def body(n_gx, n_gy, populations, anchor, offsets, heading, velocity, live_count):
    pops = populations.reshape(19, ROWS, NZ)
    tiles = LANE_TILES
    vmem = pl.BlockSpec(memory_space=pltpu.VMEM)
    hbm = pl.BlockSpec(memory_space=pltpu.HBM)
    dma = pltpu.SemaphoreType.DMA
    held = (
        pltpu.VMEM((19, ROWS, NZ), F32),
        pltpu.VMEM((2, 12, CY, 128), F32),
        pltpu.VMEM((2, 12, CX, 128), F32),
        pltpu.VMEM((4, 16, 128), F32),
        pltpu.VMEM((8, LANE_TILES, 8, 128), F32),
        pltpu.VMEM((9, 1, 128), F32),
        pltpu.VMEM((SW // OWN, 8, OWN), F32),
        pltpu.VMEM((SW // OWN, 8, OWN), F32),
        pltpu.VMEM((4, ROWS, NZ), F32),
        pltpu.VMEM((3 * ROWS, 2 * NZ), BF16),
        pltpu.VMEM((BLOCKS, 2 * NZ, BLOCK), BF16),
        pltpu.VMEM((BLOCKS, ADJ_ROWS, BLOCK), F32),
    )
    pops, halo_x, halo_y, halo_c, lists, starts, own, base, mom, inner, zhl, plane = pl.pallas_call(
        functools.partial(exchange_kernel, n_gx, n_gy),
        out_shape=held,
        in_specs=[hbm] * 6,
        out_specs=[vmem] * 12,
        scratch_shapes=[
            pltpu.VMEM((tiles, 128), jnp.int32),
            pltpu.VMEM((3 * tiles, 128), F32),
            pltpu.VMEM((2 * tiles, 128), F32),
            pltpu.VMEM((3 * tiles, 128), F32),
            pltpu.SMEM((1,), jnp.int32),
            pltpu.VMEM((8 * tiles, 128), F32),
            pltpu.VMEM((2, 12, CY, 128), F32),
            pltpu.VMEM((2, 12, CX, 128), F32),
            pltpu.VMEM((4, 16, 128), F32),
            pltpu.VMEM((LANE_TILES, 8, 128), F32),
            pltpu.VMEM((1, 128), F32),
            pltpu.VMEM((3, SW, 128), F32),
            dma((9,)), dma((24,)), dma((24,)),
        ],
        compiler_params=pltpu.CompilerParams(collective_id=0, has_side_effects=True, vmem_limit_bytes=20 << 20),
        name="exchange",
    )(*[pltpu.with_memory_space_constraint(v, pltpu.HBM) for v in (
        pops, anchor.reshape(tiles, 128), offsets.reshape(3 * tiles, 128),
        jnp.swapaxes(heading.reshape(2, tiles, 128), 0, 1).reshape(2 * tiles, 128),
        velocity.reshape(3 * tiles, 128))], live_count.reshape(1))
    moved, force = pl.pallas_call(
        fluid_kernel,
        out_shape=(jax.ShapeDtypeStruct((19, ROWS, NZ), F32), jax.ShapeDtypeStruct((3 * tiles, 128), F32)),
        in_specs=[vmem] * 12,
        out_specs=[hbm, hbm],
        scratch_shapes=[
            pltpu.VMEM((SW // OWN, 8, OWN), F32),
            pltpu.VMEM((19, ROWS, NZ), F32),
            pltpu.VMEM((3 * tiles, 128), F32),
            pltpu.SMEM((9, 1, 128), F32),
            pltpu.VMEM((7, ROWS, NZ), F32),
            pltpu.VMEM((3 * ADJ, 2 * NZ), BF16),
            pltpu.VMEM((3 * FAR_ROWS, 2 * NZ), BF16),
            pltpu.VMEM((3, ADJ_ROWS, NZ), F32),
            pltpu.VMEM((GHOST_TILES, 8, 128), F32),
            pltpu.VMEM((3, GHOST_TILES * 128, 128), F32),
            dma((19,)), dma, dma,
        ],
        compiler_params=pltpu.CompilerParams(vmem_limit_bytes=32 << 20),
        name="fluid",
    )(pops, own, base, halo_x, halo_y, halo_c, lists, starts, mom, inner, zhl, plane)
    return (moved.reshape(populations.shape), force.reshape(1, 1, 3, SW))


def solution(mesh):
    return jax.shard_map(
        functools.partial(body, mesh.shape["gx"], mesh.shape["gy"]),
        mesh=mesh,
        in_specs=(
            P(None, "gx", "gy", None),
            P("gx", "gy", None),
            P("gx", "gy", None, None),
            P("gx", "gy", None, None),
            P("gx", "gy", None, None),
            P("gx", "gy"),
        ),
        out_specs=(P(None, "gx", "gy", None), P("gx", "gy", None, None)),
        check_vma=False,
    )
```

```python
import functools

import jax
import jax.numpy as jnp
import numpy as np
from jax import lax
from jax.experimental import pallas as pl
from jax.experimental.pallas import tpu as pltpu
from jax.sharding import PartitionSpec as P

DIRS = (
    (0, 0, 0), (1, 0, 0), (-1, 0, 0), (0, 1, 0), (0, -1, 0), (0, 0, 1), (0, 0, -1),
    (1, 1, 0), (-1, -1, 0), (1, -1, 0), (-1, 1, 0), (1, 0, 1), (-1, 0, -1),
    (1, 0, -1), (-1, 0, 1), (0, 1, 1), (0, -1, -1), (0, 1, -1), (0, -1, 1),
)
WEIGHTS = (1.0 / 3.0,) + (1.0 / 18.0,) * 6 + (1.0 / 36.0,) * 12
CUTOFF = 2.0 ** (1.0 / 3.0)
REACH = 1.125
FAR = 1.0e9
F32 = jnp.float32
BF16 = jnp.bfloat16
MESH = pl.DeviceIdType.MESH

CX, CY, NZ, SW = 8, 16, 128, 1024
ROWS = CX * CY
LANE_TILES = SW // 128

SIDES = ((-1, 0), (1, 0), (0, -1), (0, 1), (-1, -1), (-1, 1), (1, -1), (1, 1))
RANGES = ((0, 4, 7), (1, 0, 3), (2, 2, 5), (3, 6, 8), (3, 0, 1), (4, 4, 5), (5, 6, 7), (6, 2, 3), (7, 0, 1))


def facing(axis, sign):
    return [q for q in range(19) if DIRS[q][axis] == sign]


def corner_q(sx, sy):
    return DIRS.index((-sx, -sy, 0))


def split2(v):
    hi = v.astype(BF16)
    return hi, (v - hi.astype(F32)).astype(BF16)


def split3(v):
    hi = v.astype(BF16)
    rest = v - hi.astype(F32)
    mid = rest.astype(BF16)
    return hi, mid, (rest - mid.astype(F32)).astype(BF16)


def dot(a, b):
    return lax.dot_general(a, b, (((1,), (0,)), ((), ())), preferred_element_type=F32)


def dot_t(a, b):
    return lax.dot_general(a, b, (((1,), (1,)), ((), ())), preferred_element_type=F32)


def tent(d):
    return jnp.maximum(1.0 - jnp.abs(d), 0.0)


def moments(load):
    rho = None
    mom = [None, None, None]
    for q in range(19):
        f = load(q)
        rho = f if rho is None else rho + f
        for c in range(3):
            s = DIRS[q][c]
            if s:
                if mom[c] is None:
                    mom[c] = f if s > 0 else -f
                else:
                    mom[c] = mom[c] + f if s > 0 else mom[c] - f
    return rho, mom


def pair_terms(ox, oy, oz, px, py, pz):
    dx = ox - px
    dy = oy - py
    dz = oz - pz
    dz = dz - NZ * jnp.round(dz * (1.0 / NZ))
    raw = dx * dx + dy * dy + dz * dz
    inv = 1.0 / jnp.maximum(raw, 0.8)
    sixth = inv * inv * inv
    mag = (sixth + sixth - 1.0) * (sixth * inv)
    mag = jnp.where(raw < CUTOFF, mag, 0.0)
    return mag * dx, mag * dy, mag * dz


def classes(x, y, live):
    xl, xh = x < REACH, x > CX - 1 - REACH
    yl, yh = y < REACH, y > CY - 1 - REACH
    yc = jnp.where(yl, 0.0, jnp.where(yh, 2.0, 1.0))
    kind = jnp.where(xl, yc, jnp.where(xh, 6.0 - yc, jnp.where(yl, 7.0, jnp.where(yh, 3.0, 8.0))))
    return jnp.where(live > 0.0, kind, 9.0)


def sort_ranks(kind):
    masks = [(kind == k).astype(F32) for k in range(10)]
    ri = lax.broadcasted_iota(jnp.int32, (128, 256), 0)
    ci = lax.broadcasted_iota(jnp.int32, (128, 256), 1)
    upper = ((ri < ci) | (ci >= 128)).astype(F32).astype(BF16)
    pre = dot(jnp.concatenate(masks, axis=0).astype(BF16), upper)
    within, tile_sum = pre[:, :128], pre[:, 128:]
    place = lax.broadcasted_iota(jnp.int32, (80, 128), 0) & 7
    upto = tile_sum
    for by in (1, 2, 4):
        upto = upto + jnp.where(place >= by, pltpu.roll(upto, by, 0), 0.0)
    lane = lax.broadcasted_iota(jnp.int32, (1, 128), 1)
    rank = jnp.zeros((8, 128), F32)
    row = jnp.zeros((1, 128), F32)
    first = jnp.zeros((1, 128), F32)
    for k in range(10):
        cut = slice(8 * k, 8 * k + 8)
        row = jnp.where(lane == k, first, row)
        rank = rank + masks[k] * (within[cut] + (upto[cut] - tile_sum[cut]) + first)
        first = first + upto[8 * k + 7:8 * k + 8]
    return rank, row


def plane_weights(px, py, far):
    x8 = lax.broadcasted_iota(jnp.int32, (CX, 1), 0).astype(F32)
    y16 = lax.broadcasted_iota(jnp.int32, (CY, 1), 0).astype(F32)
    ki = lax.broadcasted_iota(jnp.int32, (16, 1), 0)
    ii, jj = lax.shift_right_logical(ki, 2), ki & 3
    xd = jnp.where(ii < 2, ii - 2, ii + CX - 2).astype(F32)
    yd = jnp.where(jj < 2, jj - 2, jj + CY - 2).astype(F32)
    tx, ty = tent(x8 - px), tent(y16 - py)
    parts = [tx[i:i + 1] * ty for i in range(CX)]
    parts += [tent(-1.0 - px) * ty, tent(CX - px) * ty, tent(-1.0 - py) * tx, tent(CY - py) * tx]
    parts += [tent(xd - px) * tent(yd - py)]
    if far:
        parts += [tent(-2.0 - px) * ty, tent(CX + 1.0 - px) * ty, tent(-2.0 - py) * tx, tent(CY + 1.0 - py) * tx]
    return jnp.concatenate(parts, axis=0)


def z_weights(pz):
    zi = lax.broadcasted_iota(jnp.int32, (NZ, 1), 0).astype(F32)
    return split2(tent(zi - pz))


def widen(v):
    hi, lo = split2(v)
    return jnp.concatenate([hi, lo], axis=1)


def sample(u, zh, zl):
    return dot(u, jnp.concatenate([zh, zh], axis=0)) + dot(u[:, :128], zl)


def columns(cols, at, place):
    turned = jnp.transpose(place)
    for c in range(3):
        cols[c, at:at + 128] = jnp.broadcast_to(turned[:, c:c + 1], (128, 128))


def pair_step(cols, mine, width):
    def step(n, acc):
        at = pl.multiple_of(n * 8, 8)
        p = [jnp.concatenate([cols[c, pl.ds(at, 8)]] * (width // 128), axis=1) for c in range(3)]
        return tuple(a + b for a, b in zip(acc, pair_terms(*mine, *p)))

    return step


def exchange_kernel(n_gx, n_gy, pops_hbm, anchor_hbm, offsets_hbm, heading_hbm, velocity_hbm, count_hbm,
                    pops, halo_x, halo_y, halo_c, lists, starts_out, own_out, base_out, mom, inner, zhl, plane,
                    anchor, offsets, heading, velocity, count, table,
                    msg_x, msg_y, msg_c, msg_l, msg_s, cols, load_sem, send_sem, recv_sem, lower):
    gx = lax.axis_index("gx")
    gy = lax.axis_index("gy")

    def device(side):
        return (lax.rem(gx + side[0] + n_gx, n_gx), lax.rem(gy + side[1] + n_gy, n_gy))

    loads = [pltpu.make_async_copy(a, b, load_sem.at[k]) for k, (a, b) in enumerate((
        (anchor_hbm, anchor), (offsets_hbm, offsets), (heading_hbm, heading), (velocity_hbm, velocity),
        (count_hbm, count)))]
    loads += [pltpu.make_async_copy(pops_hbm.at[pl.ds(q, n)], pops.at[pl.ds(q, n)], load_sem.at[5 + k])
              for k, (q, n) in enumerate(((0, 5), (5, 5), (10, 5), (15, 4)))]
    for c in loads:
        c.start()
    barrier = pltpu.get_barrier_semaphore()
    for side in SIDES:
        if side[0] <= 0:
            pl.semaphore_signal(barrier, inc=1, device_id=device(side), device_id_type=MESH)
    for c in loads:
        c.wait()

    rho, m = moments(lambda q: pops[q])
    inv = 1.0 / rho
    mom[0] = rho
    for c in range(3):
        mom[1 + c] = m[c] * inv
    for s, (adj, far) in enumerate(((0, 1), (CX - 1, CX - 2))):
        for c in range(4):
            msg_x[s, c] = mom[c, adj * CY:(adj + 1) * CY]
        for c in range(3):
            msg_x[s, 4 + c] = mom[1 + c, far * CY:(far + 1) * CY]
        for k, q in enumerate(facing(0, 2 * s - 1)):
            msg_x[s, 7 + k] = pops[q, adj * CY:(adj + 1) * CY]

    def send(k, a, b, side, o):
        d = SIDES.index(side)
        return pltpu.make_async_remote_copy(
            src_ref=a, dst_ref=b, send_sem=send_sem.at[3 * d + k], recv_sem=recv_sem.at[3 * o + k],
            device_id=device(side), device_id_type=MESH)

    copies = {}
    for d, side in enumerate(SIDES):
        o = SIDES.index((-side[0], -side[1]))
        if side[1] == 0:
            first = send(0, msg_x.at[d], halo_x.at[o], side, o)
        elif side[0] == 0:
            first = send(0, msg_y.at[d - 2], halo_y.at[o - 2], side, o)
        else:
            first = send(0, msg_c.at[d - 4], halo_c.at[o - 4], side, o)
        copies[side] = (first, send(1, msg_s, starts_out.at[o], side, o),
                        send(2, msg_l.at[:, pl.ds(0, 6)], lists.at[o, :, pl.ds(0, 6)], side, o))

    def start(*sides):
        for k in range(3):
            for side in sides:
                copies[side][k].start()

    pl.semaphore_wait(barrier, 5)
    for side in SIDES:
        if side[0] > 0:
            pl.semaphore_signal(lower, inc=1, device_id=device(side), device_id_type=MESH)
    copies[(1, 0)][0].start()

    root = anchor[...]
    bxf = lax.shift_right_logical(root, 7).astype(F32)
    cxf = jnp.floor(bxf * (1.0 / (CY + 2)) + 0.01)
    x = cxf - 1.0 + offsets[0:8]
    y = bxf - cxf * (CY + 2) - 1.0 + offsets[8:16]
    z = (root & (NZ - 1)).astype(F32) + offsets[16:24]
    lane = lax.broadcasted_iota(jnp.int32, (8, 128), 1)
    sub = lax.broadcasted_iota(jnp.int32, (8, 128), 0)
    live = (sub * 128 + lane < count[0]).astype(F32)
    first, second = heading[pl.ds(0, 8, stride=2)], heading[pl.ds(1, 8, stride=2)]
    c1 = jnp.cos(second)
    w = [2.0 * velocity[0:8] - 0.5 * (jnp.cos(first) * c1),
         2.0 * velocity[8:16] - 0.5 * (jnp.sin(first) * c1),
         2.0 * velocity[16:24] - 0.5 * jnp.sin(second)]
    for k, v in enumerate((x, y, z, *w, live, jnp.zeros((8, 128), F32))):
        table[pl.ds(k, 8, stride=8)] = v
    rank, row = sort_ranks(classes(x, y, live))
    msg_s[...] = row
    starts_out[8] = row
    to_tile = jnp.floor(rank * (1.0 / 128.0))
    to_lane = rank - 128.0 * to_tile
    split = [v.astype(F32) for v in split3(table[...])]
    dst = lax.broadcasted_iota(jnp.int32, (128, 128), 0).astype(F32)
    ordered = jnp.zeros((24 * LANE_TILES, 128), F32)
    for t in range(0, LANE_TILES, 2):
        hot, rows = [], []
        for j in (t, t + 1):
            hot.append((dst == to_lane[j:j + 1]).astype(F32).astype(BF16))
            part = jnp.concatenate([v[8 * j:8 * j + 8] for v in split], axis=0)
            rows.append(jnp.concatenate(
                [jnp.where(to_tile[j:j + 1] == float(k), part, 0.0) for k in range(LANE_TILES)],
                axis=0).astype(BF16))
        ordered = ordered + dot_t(jnp.concatenate(rows, axis=1), jnp.concatenate(hot, axis=1))
    for t in range(LANE_TILES):
        at = 24 * t
        msg_l[t] = ordered[at:at + 8] + ordered[at + 8:at + 16] + ordered[at + 16:at + 24]

    for s, (adj, far) in enumerate(((0, 1), (CY - 1, CY - 2))):
        for c in range(4):
            msg_y[s, c] = mom[c, pl.ds(adj, CX, stride=CY)]
        for c in range(3):
            msg_y[s, 4 + c] = mom[1 + c, pl.ds(far, CX, stride=CY)]
        for k, q in enumerate(facing(1, 2 * s - 1)):
            msg_y[s, 7 + k] = pops[q, pl.ds(adj, CX, stride=CY)]
    for i in range(4):
        sx, sy = SIDES[4 + i]
        ax, fx = (0, 1) if sx < 0 else (CX - 1, CX - 2)
        ay, fy = (0, 1) if sy < 0 else (CY - 1, CY - 2)
        msg_c[i] = jnp.zeros((16, 128), F32)
        for c in range(4):
            msg_c[i, c:c + 1] = mom[c, ax * CY + ay:ax * CY + ay + 1]
        for j, (nx, ny) in enumerate(((ax, fy), (fx, ay), (fx, fy))):
            for c in range(3):
                msg_c[i, 5 + 3 * j + c:6 + 3 * j + c] = mom[1 + c, nx * CY + ny:nx * CY + ny + 1]
        q = DIRS.index((sx, sy, 0))
        msg_c[i, 4:5] = pops[q, ax * CY + ay:ax * CY + ay + 1]

    copies[(1, 0)][1].start()
    copies[(1, 0)][2].start()

    @pl.when(gx == n_gx - 1)
    def _():
        start((1, -1), (1, 1))

    for c in range(3):
        inner[c * ROWS:(c + 1) * ROWS] = widen(mom[1 + c])
    for i in range(BLOCKS):
        n = BLOCK // 128
        vals = jnp.concatenate([table[8 * (n * i + j):8 * (n * i + j) + 8] for j in range(n)], axis=1)
        zh, zl = z_weights(vals[2:3])
        zhl[i, 0:NZ] = zh
        zhl[i, NZ:2 * NZ] = zl
        plane[i] = plane_weights(vals[0:1], vals[1:2], False)
        got = sample(inner[...], zh, zl)
        rows = [vals[0:3]]
        for c in range(3):
            s = jnp.sum(got[c * ROWS:(c + 1) * ROWS] * plane[i, 0:ROWS], axis=0, keepdims=True)
            rows.append((vals[3 + c:4 + c] - 2.0 * s) * vals[6:7])
        rows = jnp.concatenate(rows + [vals[6:8]], axis=0)
        for j in range(BLOCK // OWN):
            own_out[i * (BLOCK // OWN) + j] = rows[:, j * OWN:(j + 1) * OWN]

    def own_pairs():
        for t in range(LANE_TILES):
            v = table[8 * t:8 * t + 8]
            columns(cols, t * 128, jnp.where((sub == 0) & (v[6:7] == 0.0), FAR, v))
        for i in range(0, SW // OWN, 2):
            width = 2 * OWN
            mine = [jnp.broadcast_to(jnp.concatenate([own_out[i, c:c + 1], own_out[i + 1, c:c + 1]], axis=1), (8, width))
                    for c in range(3)]
            init = tuple(jnp.zeros((8, width), F32) for _ in range(3))
            got = lax.fori_loop(0, SW // 8, pair_step(cols, mine, width), init)
            for c in range(3):
                pairs = 0.24 * jnp.sum(got[c], axis=0, keepdims=True)
                for j in range(2):
                    base_out[i + j, c:c + 1] = (pairs[:, j * OWN:(j + 1) * OWN] * own_out[i + j, 6:7]
                                                - own_out[i + j, 3 + c:4 + c])
        for i in range(SW // OWN):
            base_out[i, 3:8] = jnp.zeros((5, OWN), F32)

    start((0, -1), (0, 1))

    @pl.when(gx != n_gx - 1)
    def _():
        start((1, -1), (1, 1))

    @pl.when(gx == 0)
    def _():
        own_pairs()

    pl.semaphore_wait(lower, 3)
    start((-1, 0), (-1, -1), (-1, 1))

    @pl.when(gx != 0)
    def _():
        own_pairs()

    for side in SIDES:
        for c in copies[side]:
            c.wait()


ADJ = 64
FAR_ROWS = 48
ADJ_ROWS = ROWS + ADJ
BLOCK = 512
BLOCKS = SW // BLOCK
OWN = 256
GHOST_TILES = 8 * LANE_TILES + 4


def fluid_kernel(pops, own, base, halo_x, halo_y, halo_c, lists, starts_in, mom, inner, zhl, plane,
                 next_out, force_out,
                 acc, out_v, force_v, starts, node, near, outer, force, ghosts, cols, out_sem, start_sem, force_sem):
    start_copy = pltpu.make_async_copy(starts_in, starts, start_sem)
    start_copy.start()
    acc[...] = base[...]
    ghosts[...] = jnp.zeros(ghosts.shape, F32)
    force[...] = jnp.zeros(force.shape, F32)
    for c in range(3):
        corner = []
        for i in range(4):
            for j in range(4):
                sx, sy = (0 if i < 2 else 1), (0 if j < 2 else 1)
                fx, fy = i in (0, 3), j in (0, 3)
                k = 2 * sx + sy
                r = (11 if fy else 8) if fx else (5 if fy else 1)
                corner.append(halo_c[k, r + c:r + c + 1])
        near[c * ADJ:(c + 1) * ADJ] = widen(jnp.concatenate(
            [halo_x[0, 1 + c], halo_x[1, 1 + c], halo_y[0, 1 + c], halo_y[1, 1 + c]] + corner, axis=0))
        outer[c * FAR_ROWS:(c + 1) * FAR_ROWS] = widen(jnp.concatenate(
            [halo_x[0, 4 + c], halo_x[1, 4 + c], halo_y[0, 4 + c], halo_y[1, 4 + c]], axis=0))

    def spread(weights, react, zz):
        zh = zz[0:NZ]
        for c in range(3):
            wh, wl = split2(weights * react[c])
            both = dot_t(wh, zz)
            force[c] = force[c] + (both[:, :128] + both[:, 128:] + dot_t(wl, zh))

    per = BLOCK // OWN

    def own_block(i, carry):
        zz = zhl[i]
        got = sample(near[...], zz[0:NZ], zz[NZ:2 * NZ])
        vals = jnp.concatenate([own[per * i + j] for j in range(per)], axis=1)
        react = []
        for c in range(3):
            s = jnp.sum(got[c * ADJ:(c + 1) * ADJ] * plane[i, ROWS:ADJ_ROWS], axis=0, keepdims=True)
            s = 2.0 * s * vals[6:7]
            react.append(vals[3 + c:4 + c] - s)
            for j in range(per):
                acc[per * i + j, c:c + 1] = acc[per * i + j, c:c + 1] + s[:, j * OWN:(j + 1) * OWN]
        spread(plane[i], react, zz)
        return carry

    own_block(0, 0)
    start_copy.wait()
    n_own = starts[8, 0, 9].astype(jnp.int32)

    lane = lax.broadcasted_iota(jnp.int32, (8, 128), 1)
    sub = lax.broadcasted_iota(jnp.int32, (8, 128), 0)
    total = jnp.int32(0)
    puts, rest = [], []
    for d, lo, hi in RANGES:
        a = starts[d, 0, lo].astype(jnp.int32)
        b = starts[d, 0, hi].astype(jnp.int32)
        sx, sy = SIDES[d]
        moved = jnp.where(sub == 0, float(sx * CX), jnp.where(sub == 1, float(sy * CY), 0.0))
        by = (total - a) & 127
        upper = lane >= by

        def taken(t, d=d, a=a, b=b, by=by, moved=moved):
            at = t * 128 + lane
            v = jnp.where((at >= a) & (at < b), lists[d, jnp.minimum(t, LANE_TILES - 1)] + moved, 0.0)
            return pltpu.roll(v, by, 1)

        t0 = lax.shift_right_logical(a, 7)
        tile = lax.shift_right_logical(total - a + t0 * 128 + 1024, 7) - 8
        v0, v1 = taken(t0), taken(t0 + 1)
        puts.append((jnp.maximum(tile, 0), jnp.where(upper, v0, 0.0)))
        puts.append((tile + 1, jnp.where(upper, v1, v0)))
        puts.append((tile + 2, jnp.where(upper, 0.0, v1)))

        def more(t, carry, taken=taken, upper=upper, shift=tile - t0):
            v = taken(t)
            ghosts[t + shift] = ghosts[t + shift] + jnp.where(upper, v, 0.0)
            ghosts[t + shift + 1] = ghosts[t + shift + 1] + jnp.where(upper, 0.0, v)
            return carry

        rest.append((t0 + 2, lax.shift_right_logical(b + 127, 7), more))
        total = total + (b - a)
    for at, v in puts:
        ghosts[at] = ghosts[at] + v
    for lo, hi, more in rest:
        lax.fori_loop(lo, hi, more, 0)

    slot = lax.broadcasted_iota(jnp.int32, (1, BLOCK), 1)
    tiles = lax.shift_right_logical(total + 127, 7)
    ahead = BLOCK // 128

    def ghost_columns(t, carry):
        g = jnp.where((sub == 0) & (lane + t * 128 >= total), FAR, ghosts[t])
        turned = jnp.transpose(g)
        at = t * 128 if isinstance(t, int) else pl.multiple_of(t * 128, 128)
        for c in range(3):
            cols[c, pl.ds(at, 128)] = jnp.broadcast_to(turned[:, c:c + 1], (128, 128))
        return carry

    def ghost_block(i, carry):
        vals = jnp.concatenate([ghosts[ahead * i + j] for j in range(ahead)], axis=1)
        live = (slot + i * BLOCK < total).astype(F32)
        zh, zl = z_weights(vals[2:3])
        weights = plane_weights(vals[0:1], vals[1:2], True)
        gi = sample(inner[...], zh, zl)
        gn = sample(near[...], zh, zl)
        gf = sample(outer[...], zh, zl)
        react = []
        for c in range(3):
            s = (jnp.sum(gi[c * ROWS:(c + 1) * ROWS] * weights[0:ROWS], axis=0, keepdims=True)
                 + jnp.sum(gn[c * ADJ:(c + 1) * ADJ] * weights[ROWS:ADJ_ROWS], axis=0, keepdims=True)
                 + jnp.sum(gf[c * FAR_ROWS:(c + 1) * FAR_ROWS] * weights[ADJ_ROWS:], axis=0, keepdims=True))
            react.append((vals[3 + c:4 + c] - 2.0 * s) * live)
        spread(weights[0:ADJ_ROWS], react, jnp.concatenate([zh, zl], axis=0))
        return carry

    for t in range(ahead):
        ghost_columns(t, 0)
    ghost_block(0, 0)
    lax.fori_loop(ahead, tiles, ghost_columns, 0)
    lax.fori_loop(1, lax.shift_right_logical(total + BLOCK - 1, 9), ghost_block, 0)
    lax.fori_loop(1, lax.shift_right_logical(n_own + BLOCK - 1, 9), own_block, 0)

    def ghost_pairs(i, carry):
        mine = [jnp.broadcast_to(own[i, c:c + 1], (8, OWN)) for c in range(3)]
        one = pair_step(cols, mine, OWN)
        init = tuple(jnp.zeros((8, OWN), F32) for _ in range(3))

        def four(n, got):
            for k in range(4):
                got = one(4 * n + k, got)
            return got

        got = lax.fori_loop(0, lax.shift_right_logical(total + 31, 5), four, init)
        live = own[i, 6:7]
        for c in range(3):
            acc[i, c:c + 1] = acc[i, c:c + 1] + 0.24 * live * jnp.sum(got[c], axis=0, keepdims=True)
        return carry

    lax.fori_loop(0, lax.shift_right_logical(n_own + OWN - 1, 8), ghost_pairs, 0)
    for i in range(SW // OWN):
        for c in range(3):
            for j in range(2):
                r = c * LANE_TILES + 2 * i + j
                force_v[r:r + 1] = acc[i, c:c + 1, j * 128:(j + 1) * 128]
    force_copy = pltpu.make_async_copy(force_v, force_out, force_sem)
    force_copy.start()

    def prepare(rho, u0, half, g):
        u = [u0[c] + half * g[c] for c in range(3)]
        uu = u[0] * u[0] + u[1] * u[1] + u[2] * u[2]
        ug = u[0] * g[0] + u[1] * g[1] + u[2] * g[2]
        k0 = 1.25 * rho * (1.0 - 1.5 * uu) - 1.125 * ug
        return k0, 3.75 * rho, 5.625 * rho, u, [1.125 * v for v in g]

    def along(q, v):
        out = None
        for c in range(3):
            s = DIRS[q][c]
            if s:
                out = (v[c] if s > 0 else -v[c]) if out is None else (out + v[c] if s > 0 else out - v[c])
        return out

    def post(q, f, prep):
        k0, r1, r2, u, g = prep
        if q == 0:
            return -0.25 * f + WEIGHTS[0] * k0
        a, p = along(q, u), along(q, g)
        return -0.25 * f + WEIGHTS[q] * (k0 + a * (r1 + r2 * a + 3.0 * p) + p)

    def side_prep(rho, u0, lo, n):
        g = [force[c, lo:lo + n] for c in range(3)]
        return prepare(rho, u0, 0.5 / rho, g)

    k0, r1, r2, u, g = side_prep(mom[0], [mom[1 + c] for c in range(3)], 0, ROWS)
    node[0] = k0
    for c in range(3):
        node[1 + c] = u[c]
        node[4 + c] = g[c]
    xs = [side_prep(halo_x[s, 0], [halo_x[s, 1 + c] for c in range(3)], ROWS + s * CY, CY) for s in range(2)]
    ys = [side_prep(halo_y[s, 0], [halo_y[s, 1 + c] for c in range(3)], ROWS + 2 * CY + s * CX, CX)
          for s in range(2)]
    cs = []
    for i in range(4):
        sx, sy = SIDES[4 + i]
        r = ADJ_ROWS - 16 + (1 if sx < 0 else 2) * 4 + (1 if sy < 0 else 2)
        cs.append(side_prep(halo_c[i, 0:1], [halo_c[i, 1 + c:2 + c] for c in range(3)], r, 1))
    stores = []
    for q in range(19):
        dx, dy, dz = DIRS[q]
        rho_q = mom[0]
        prep = (node[0], 3.75 * rho_q, 5.625 * rho_q, [node[1 + c] for c in range(3)], [node[4 + c] for c in range(3)])

        def turned(v, dz=dz):
            return pltpu.roll(v, dz % NZ, 1) if dz else v

        v = turned(post(q, pops[q], prep))
        if dy:
            v = pltpu.roll(v, dy % ROWS, 0)
        if dx == 0:
            out_v[q] = v
        else:
            s = 0 if dx > 0 else 1
            e = turned(post(q, halo_x[s, 7 + facing(0, dx).index(q)], xs[s]))
            if dy:
                e = pltpu.roll(e, dy % CY, 0)
            if dx > 0:
                out_v[q, CY:ROWS] = v[0:ROWS - CY]
                out_v[q, 0:CY] = e
            else:
                out_v[q, 0:ROWS - CY] = v[CY:ROWS]
                out_v[q, ROWS - CY:ROWS] = e
        if dy:
            s = 0 if dy > 0 else 1
            at = 0 if dy > 0 else CY - 1
            e = turned(post(q, halo_y[s, 7 + facing(1, dy).index(q)], ys[s]))
            if dx:
                e = pltpu.roll(e, dx % CX, 0)
            out_v[q, pl.ds(at, CX, stride=CY)] = e
            if dx:
                i = SIDES.index((-dx, -dy)) - 4
                r = at + (0 if dx > 0 else (CX - 1) * CY)
                out_v[q, r:r + 1] = post(q, halo_c[i, 4:5], cs[i])
        c = pltpu.make_async_copy(out_v.at[q], next_out.at[q], out_sem.at[q])
        c.start()
        stores.append(c)
    force_copy.wait()
    for c in stores:
        c.wait()


def body(n_gx, n_gy, populations, anchor, offsets, heading, velocity, live_count):
    pops = populations.reshape(19, ROWS, NZ)
    tiles = LANE_TILES
    vmem = pl.BlockSpec(memory_space=pltpu.VMEM)
    hbm = pl.BlockSpec(memory_space=pltpu.HBM)
    dma = pltpu.SemaphoreType.DMA
    held = (
        pltpu.VMEM((19, ROWS, NZ), F32),
        pltpu.VMEM((2, 12, CY, 128), F32),
        pltpu.VMEM((2, 12, CX, 128), F32),
        pltpu.VMEM((4, 16, 128), F32),
        pltpu.VMEM((8, LANE_TILES, 8, 128), F32),
        pltpu.VMEM((9, 1, 128), F32),
        pltpu.VMEM((SW // OWN, 8, OWN), F32),
        pltpu.VMEM((SW // OWN, 8, OWN), F32),
        pltpu.VMEM((4, ROWS, NZ), F32),
        pltpu.VMEM((3 * ROWS, 2 * NZ), BF16),
        pltpu.VMEM((BLOCKS, 2 * NZ, BLOCK), BF16),
        pltpu.VMEM((BLOCKS, ADJ_ROWS, BLOCK), F32),
    )
    pops, halo_x, halo_y, halo_c, lists, starts, own, base, mom, inner, zhl, plane = pl.pallas_call(
        functools.partial(exchange_kernel, n_gx, n_gy),
        out_shape=held,
        in_specs=[hbm] * 6,
        out_specs=[vmem] * 12,
        scratch_shapes=[
            pltpu.VMEM((tiles, 128), jnp.int32),
            pltpu.VMEM((3 * tiles, 128), F32),
            pltpu.VMEM((2 * tiles, 128), F32),
            pltpu.VMEM((3 * tiles, 128), F32),
            pltpu.SMEM((1,), jnp.int32),
            pltpu.VMEM((8 * tiles, 128), F32),
            pltpu.VMEM((2, 12, CY, 128), F32),
            pltpu.VMEM((2, 12, CX, 128), F32),
            pltpu.VMEM((4, 16, 128), F32),
            pltpu.VMEM((LANE_TILES, 8, 128), F32),
            pltpu.VMEM((1, 128), F32),
            pltpu.VMEM((3, SW, 128), F32),
            dma((9,)), dma((24,)), dma((24,)), pltpu.SemaphoreType.REGULAR,
        ],
        compiler_params=pltpu.CompilerParams(collective_id=0, has_side_effects=True, vmem_limit_bytes=20 << 20),
        name="exchange",
    )(*[pltpu.with_memory_space_constraint(v, pltpu.HBM) for v in (
        pops, anchor.reshape(tiles, 128), offsets.reshape(3 * tiles, 128),
        jnp.swapaxes(heading.reshape(2, tiles, 128), 0, 1).reshape(2 * tiles, 128),
        velocity.reshape(3 * tiles, 128))], live_count.reshape(1))
    moved, force = pl.pallas_call(
        fluid_kernel,
        out_shape=(jax.ShapeDtypeStruct((19, ROWS, NZ), F32), jax.ShapeDtypeStruct((3 * tiles, 128), F32)),
        in_specs=[vmem] * 12,
        out_specs=[hbm, hbm],
        scratch_shapes=[
            pltpu.VMEM((SW // OWN, 8, OWN), F32),
            pltpu.VMEM((19, ROWS, NZ), F32),
            pltpu.VMEM((3 * tiles, 128), F32),
            pltpu.SMEM((9, 1, 128), F32),
            pltpu.VMEM((7, ROWS, NZ), F32),
            pltpu.VMEM((3 * ADJ, 2 * NZ), BF16),
            pltpu.VMEM((3 * FAR_ROWS, 2 * NZ), BF16),
            pltpu.VMEM((3, ADJ_ROWS, NZ), F32),
            pltpu.VMEM((GHOST_TILES, 8, 128), F32),
            pltpu.VMEM((3, GHOST_TILES * 128, 128), F32),
            dma((19,)), dma, dma,
        ],
        compiler_params=pltpu.CompilerParams(vmem_limit_bytes=32 << 20),
        name="fluid",
    )(pops, own, base, halo_x, halo_y, halo_c, lists, starts, mom, inner, zhl, plane)
    return (moved.reshape(populations.shape), force.reshape(1, 1, 3, SW))


def solution(mesh):
    return jax.shard_map(
        functools.partial(body, mesh.shape["gx"], mesh.shape["gy"]),
        mesh=mesh,
        in_specs=(
            P(None, "gx", "gy", None),
            P("gx", "gy", None),
            P("gx", "gy", None, None),
            P("gx", "gy", None, None),
            P("gx", "gy", None, None),
            P("gx", "gy"),
        ),
        out_specs=(P(None, "gx", "gy", None), P("gx", "gy", None, None)),
        check_vma=False,
    )
```

```python
import functools

import jax
import jax.numpy as jnp
import numpy as np
from jax import lax
from jax.experimental import pallas as pl
from jax.experimental.pallas import tpu as pltpu
from jax.sharding import PartitionSpec as P

DIRS = (
    (0, 0, 0), (1, 0, 0), (-1, 0, 0), (0, 1, 0), (0, -1, 0), (0, 0, 1), (0, 0, -1),
    (1, 1, 0), (-1, -1, 0), (1, -1, 0), (-1, 1, 0), (1, 0, 1), (-1, 0, -1),
    (1, 0, -1), (-1, 0, 1), (0, 1, 1), (0, -1, -1), (0, 1, -1), (0, -1, 1),
)
WEIGHTS = (1.0 / 3.0,) + (1.0 / 18.0,) * 6 + (1.0 / 36.0,) * 12
CUTOFF = 2.0 ** (1.0 / 3.0)
REACH = 1.125
FAR = 1.0e9
F32 = jnp.float32
BF16 = jnp.bfloat16
MESH = pl.DeviceIdType.MESH

CX, CY, NZ, SW = 8, 16, 128, 1024
ROWS = CX * CY
LANE_TILES = SW // 128

SIDES = ((-1, 0), (1, 0), (0, -1), (0, 1), (-1, -1), (-1, 1), (1, -1), (1, 1))
RANGES = ((0, 4, 7), (1, 0, 3), (2, 2, 5), (3, 6, 8), (3, 0, 1), (4, 4, 5), (5, 6, 7), (6, 2, 3), (7, 0, 1))


def facing(axis, sign):
    return [q for q in range(19) if DIRS[q][axis] == sign]


def corner_q(sx, sy):
    return DIRS.index((-sx, -sy, 0))


def split2(v):
    hi = v.astype(BF16)
    return hi, (v - hi.astype(F32)).astype(BF16)


def split3(v):
    hi = v.astype(BF16)
    rest = v - hi.astype(F32)
    mid = rest.astype(BF16)
    return hi, mid, (rest - mid.astype(F32)).astype(BF16)


def dot(a, b):
    return lax.dot_general(a, b, (((1,), (0,)), ((), ())), preferred_element_type=F32)


def dot_t(a, b):
    return lax.dot_general(a, b, (((1,), (1,)), ((), ())), preferred_element_type=F32)


def tent(d):
    return jnp.maximum(1.0 - jnp.abs(d), 0.0)


def moments(load):
    rho = None
    mom = [None, None, None]
    for q in range(19):
        f = load(q)
        rho = f if rho is None else rho + f
        for c in range(3):
            s = DIRS[q][c]
            if s:
                if mom[c] is None:
                    mom[c] = f if s > 0 else -f
                else:
                    mom[c] = mom[c] + f if s > 0 else mom[c] - f
    return rho, mom


def pair_terms(ox, oy, oz, px, py, pz):
    dx = ox - px
    dy = oy - py
    dz = oz - pz
    dz = dz - NZ * jnp.round(dz * (1.0 / NZ))
    raw = dx * dx + dy * dy + dz * dz
    inv = 1.0 / jnp.maximum(raw, 0.8)
    sixth = inv * inv * inv
    mag = (sixth + sixth - 1.0) * (sixth * inv)
    mag = jnp.where(raw < CUTOFF, mag, 0.0)
    return mag * dx, mag * dy, mag * dz


def classes(x, y, live):
    xl, xh = x < REACH, x > CX - 1 - REACH
    yl, yh = y < REACH, y > CY - 1 - REACH
    yc = jnp.where(yl, 0.0, jnp.where(yh, 2.0, 1.0))
    kind = jnp.where(xl, yc, jnp.where(xh, 6.0 - yc, jnp.where(yl, 7.0, jnp.where(yh, 3.0, 8.0))))
    return jnp.where(live > 0.0, kind, 9.0)


def sort_ranks(kind):
    masks = [(kind == k).astype(F32) for k in range(10)]
    ri = lax.broadcasted_iota(jnp.int32, (128, 256), 0)
    ci = lax.broadcasted_iota(jnp.int32, (128, 256), 1)
    upper = ((ri < ci) | (ci >= 128)).astype(F32).astype(BF16)
    pre = dot(jnp.concatenate(masks, axis=0).astype(BF16), upper)
    within, tile_sum = pre[:, :128], pre[:, 128:]
    place = lax.broadcasted_iota(jnp.int32, (80, 128), 0) & 7
    upto = tile_sum
    for by in (1, 2, 4):
        upto = upto + jnp.where(place >= by, pltpu.roll(upto, by, 0), 0.0)
    lane = lax.broadcasted_iota(jnp.int32, (1, 128), 1)
    rank = jnp.zeros((8, 128), F32)
    row = jnp.zeros((1, 128), F32)
    first = jnp.zeros((1, 128), F32)
    for k in range(10):
        cut = slice(8 * k, 8 * k + 8)
        row = jnp.where(lane == k, first, row)
        rank = rank + masks[k] * (within[cut] + (upto[cut] - tile_sum[cut]) + first)
        first = first + upto[8 * k + 7:8 * k + 8]
    return rank, row


def plane_weights(px, py, far):
    x8 = lax.broadcasted_iota(jnp.int32, (CX, 1), 0).astype(F32)
    y16 = lax.broadcasted_iota(jnp.int32, (CY, 1), 0).astype(F32)
    ki = lax.broadcasted_iota(jnp.int32, (16, 1), 0)
    ii, jj = lax.shift_right_logical(ki, 2), ki & 3
    xd = jnp.where(ii < 2, ii - 2, ii + CX - 2).astype(F32)
    yd = jnp.where(jj < 2, jj - 2, jj + CY - 2).astype(F32)
    tx, ty = tent(x8 - px), tent(y16 - py)
    parts = [tx[i:i + 1] * ty for i in range(CX)]
    parts += [tent(-1.0 - px) * ty, tent(CX - px) * ty, tent(-1.0 - py) * tx, tent(CY - py) * tx]
    parts += [tent(xd - px) * tent(yd - py)]
    if far:
        parts += [tent(-2.0 - px) * ty, tent(CX + 1.0 - px) * ty, tent(-2.0 - py) * tx, tent(CY + 1.0 - py) * tx]
    return jnp.concatenate(parts, axis=0)


def z_weights(pz):
    zi = lax.broadcasted_iota(jnp.int32, (NZ, 1), 0).astype(F32)
    return split2(tent(zi - pz))


def widen(v):
    hi, lo = split2(v)
    return jnp.concatenate([hi, lo], axis=1)


def sample(u, zh, zl):
    return dot(u, jnp.concatenate([zh, zh], axis=0)) + dot(u[:, :128], zl)


def columns(cols, at, place):
    turned = jnp.transpose(place)
    for c in range(3):
        cols[c, at:at + 128] = jnp.broadcast_to(turned[:, c:c + 1], (128, 128))


def pair_step(cols, mine, width):
    def step(n, acc):
        at = pl.multiple_of(n * 8, 8)
        p = [jnp.concatenate([cols[c, pl.ds(at, 8)]] * (width // 128), axis=1) for c in range(3)]
        return tuple(a + b for a, b in zip(acc, pair_terms(*mine, *p)))

    return step


def exchange_kernel(n_gx, n_gy, pops_hbm, anchor_hbm, offsets_hbm, heading_hbm, velocity_hbm, count_hbm,
                    pops, halo_x, halo_y, halo_c, lists, starts_out, own_out, base_out, mom, inner, zhl, plane,
                    anchor, offsets, heading, velocity, count, table,
                    msg_x, msg_y, msg_c, msg_l, msg_s, cols, load_sem, send_sem, recv_sem, lower):
    gx = lax.axis_index("gx")
    gy = lax.axis_index("gy")

    def device(side):
        return (lax.rem(gx + side[0] + n_gx, n_gx), lax.rem(gy + side[1] + n_gy, n_gy))

    loads = [pltpu.make_async_copy(a, b, load_sem.at[k]) for k, (a, b) in enumerate((
        (anchor_hbm, anchor), (offsets_hbm, offsets), (heading_hbm, heading), (velocity_hbm, velocity),
        (count_hbm, count)))]
    loads += [pltpu.make_async_copy(pops_hbm.at[pl.ds(q, n)], pops.at[pl.ds(q, n)], load_sem.at[5 + k])
              for k, (q, n) in enumerate(((0, 5), (5, 5), (10, 5), (15, 4)))]
    for c in loads:
        c.start()
    barrier = pltpu.get_barrier_semaphore()
    for side in SIDES:
        if side[0] <= 0:
            pl.semaphore_signal(barrier, inc=1, device_id=device(side), device_id_type=MESH)
    for c in loads[:5]:
        c.wait()

    root = anchor[...]
    bxf = lax.shift_right_logical(root, 7).astype(F32)
    cxf = jnp.floor(bxf * (1.0 / (CY + 2)) + 0.01)
    x = cxf - 1.0 + offsets[0:8]
    y = bxf - cxf * (CY + 2) - 1.0 + offsets[8:16]
    z = (root & (NZ - 1)).astype(F32) + offsets[16:24]
    lane = lax.broadcasted_iota(jnp.int32, (8, 128), 1)
    sub = lax.broadcasted_iota(jnp.int32, (8, 128), 0)
    live = (sub * 128 + lane < count[0]).astype(F32)
    first, second = heading[pl.ds(0, 8, stride=2)], heading[pl.ds(1, 8, stride=2)]
    c1 = jnp.cos(second)
    w = [2.0 * velocity[0:8] - 0.5 * (jnp.cos(first) * c1),
         2.0 * velocity[8:16] - 0.5 * (jnp.sin(first) * c1),
         2.0 * velocity[16:24] - 0.5 * jnp.sin(second)]
    for k, v in enumerate((x, y, z, *w, live, jnp.zeros((8, 128), F32))):
        table[pl.ds(k, 8, stride=8)] = v
    rank, row = sort_ranks(classes(x, y, live))
    msg_s[...] = row
    starts_out[8] = row
    to_tile = jnp.floor(rank * (1.0 / 128.0))
    to_lane = rank - 128.0 * to_tile
    split = [v.astype(F32) for v in split3(table[...])]
    dst = lax.broadcasted_iota(jnp.int32, (128, 128), 0).astype(F32)
    ordered = jnp.zeros((24 * LANE_TILES, 128), F32)
    for t in range(0, LANE_TILES, 2):
        hot, rows = [], []
        for j in (t, t + 1):
            hot.append((dst == to_lane[j:j + 1]).astype(F32).astype(BF16))
            part = jnp.concatenate([v[8 * j:8 * j + 8] for v in split], axis=0)
            rows.append(jnp.concatenate(
                [jnp.where(to_tile[j:j + 1] == float(k), part, 0.0) for k in range(LANE_TILES)],
                axis=0).astype(BF16))
        ordered = ordered + dot_t(jnp.concatenate(rows, axis=1), jnp.concatenate(hot, axis=1))
    for t in range(LANE_TILES):
        at = 24 * t
        msg_l[t] = ordered[at:at + 8] + ordered[at + 8:at + 16] + ordered[at + 16:at + 24]

    def send(k, a, b, side, o):
        d = SIDES.index(side)
        return pltpu.make_async_remote_copy(
            src_ref=a, dst_ref=b, send_sem=send_sem.at[3 * d + k], recv_sem=recv_sem.at[3 * o + k],
            device_id=device(side), device_id_type=MESH)

    copies = {}
    for d, side in enumerate(SIDES):
        o = SIDES.index((-side[0], -side[1]))
        if side[1] == 0:
            first = send(0, msg_x.at[d], halo_x.at[o], side, o)
        elif side[0] == 0:
            first = send(0, msg_y.at[d - 2], halo_y.at[o - 2], side, o)
        else:
            first = send(0, msg_c.at[d - 4], halo_c.at[o - 4], side, o)
        copies[side] = (first, send(1, msg_s, starts_out.at[o], side, o),
                        send(2, msg_l.at[:, pl.ds(0, 6)], lists.at[o, :, pl.ds(0, 6)], side, o))

    def start(sides, kinds=(0, 1, 2)):
        for k in kinds:
            for side in sides:
                copies[side][k].start()

    corners_up, along_y, down = ((1, -1), (1, 1)), ((0, -1), (0, 1)), ((-1, 0), (-1, -1), (-1, 1))
    last = gx == n_gx - 1
    late = gx >= n_gx - max(n_gx // 4, 1)
    pl.semaphore_wait(barrier, 5)
    for side in SIDES:
        if side[0] > 0:
            pl.semaphore_signal(lower, inc=1, device_id=device(side), device_id_type=MESH)

    @pl.when(last)
    def _():
        start(corners_up, (1, 2))

    start(((1, 0),), (1, 2))

    for c in loads[5:]:
        c.wait()
    rho, m = moments(lambda q: pops[q])
    inv = 1.0 / rho
    mom[0] = rho
    for c in range(3):
        mom[1 + c] = m[c] * inv
    for s, (adj, far) in enumerate(((0, 1), (CX - 1, CX - 2))):
        for c in range(4):
            msg_x[s, c] = mom[c, adj * CY:(adj + 1) * CY]
        for c in range(3):
            msg_x[s, 4 + c] = mom[1 + c, far * CY:(far + 1) * CY]
        for k, q in enumerate(facing(0, 2 * s - 1)):
            msg_x[s, 7 + k] = pops[q, adj * CY:(adj + 1) * CY]

    for i in range(4):
        sx, sy = SIDES[4 + i]
        ax, fx = (0, 1) if sx < 0 else (CX - 1, CX - 2)
        ay, fy = (0, 1) if sy < 0 else (CY - 1, CY - 2)
        msg_c[i] = jnp.zeros((16, 128), F32)
        for c in range(4):
            msg_c[i, c:c + 1] = mom[c, ax * CY + ay:ax * CY + ay + 1]
        for j, (nx, ny) in enumerate(((ax, fy), (fx, ay), (fx, fy))):
            for c in range(3):
                msg_c[i, 5 + 3 * j + c:6 + 3 * j + c] = mom[1 + c, nx * CY + ny:nx * CY + ny + 1]
        q = DIRS.index((sx, sy, 0))
        msg_c[i, 4:5] = pops[q, ax * CY + ay:ax * CY + ay + 1]


    @pl.when(last)
    def _():
        start(corners_up, (0,))

    start(((1, 0),), (0,))
    for s, (adj, far) in enumerate(((0, 1), (CY - 1, CY - 2))):
        for c in range(4):
            msg_y[s, c] = mom[c, pl.ds(adj, CX, stride=CY)]
        for c in range(3):
            msg_y[s, 4 + c] = mom[1 + c, pl.ds(far, CX, stride=CY)]
        for k, q in enumerate(facing(1, 2 * s - 1)):
            msg_y[s, 7 + k] = pops[q, pl.ds(adj, CX, stride=CY)]
    def own_pairs():
        for t in range(LANE_TILES):
            v = table[8 * t:8 * t + 8]
            columns(cols, t * 128, jnp.where((sub == 0) & (v[6:7] == 0.0), FAR, v))
        for i in range(0, SW // OWN, 2):
            width = 2 * OWN
            mine = [jnp.broadcast_to(jnp.concatenate([own_out[i, c:c + 1], own_out[i + 1, c:c + 1]], axis=1), (8, width))
                    for c in range(3)]
            init = tuple(jnp.zeros((8, width), F32) for _ in range(3))
            got = lax.fori_loop(0, SW // 8, pair_step(cols, mine, width), init)
            for c in range(3):
                pairs = 0.24 * jnp.sum(got[c], axis=0, keepdims=True)
                for j in range(2):
                    base_out[i + j, c:c + 1] = (pairs[:, j * OWN:(j + 1) * OWN] * own_out[i + j, 6:7]
                                                - own_out[i + j, 3 + c:4 + c])
        for i in range(SW // OWN):
            base_out[i, 3:8] = jnp.zeros((5, OWN), F32)

    def send_down():
        pl.semaphore_wait(lower, 3)
        start(down)

    @pl.when(jnp.logical_not(late))
    def _():
        start(along_y + corners_up)

    @pl.when(jnp.logical_not(late) & (gx != 0))
    def _():
        send_down()

    for c in range(3):
        inner[c * ROWS:(c + 1) * ROWS] = widen(mom[1 + c])
    for i in range(BLOCKS):
        n = BLOCK // 128
        vals = jnp.concatenate([table[8 * (n * i + j):8 * (n * i + j) + 8] for j in range(n)], axis=1)
        zh, zl = z_weights(vals[2:3])
        zhl[i, 0:NZ] = zh
        zhl[i, NZ:2 * NZ] = zl
        plane[i] = plane_weights(vals[0:1], vals[1:2], False)
        got = sample(inner[...], zh, zl)
        rows = [vals[0:3]]
        for c in range(3):
            s = jnp.sum(got[c * ROWS:(c + 1) * ROWS] * plane[i, 0:ROWS], axis=0, keepdims=True)
            rows.append((vals[3 + c:4 + c] - 2.0 * s) * vals[6:7])
        rows = jnp.concatenate(rows + [vals[6:8]], axis=0)
        for j in range(BLOCK // OWN):
            own_out[i * (BLOCK // OWN) + j] = rows[:, j * OWN:(j + 1) * OWN]

    @pl.when(late)
    def _():
        start(along_y)

    @pl.when(late & jnp.logical_not(last))
    def _():
        start(corners_up)

    @pl.when(late)
    def _():
        send_down()

    own_pairs()

    @pl.when(gx == 0)
    def _():
        send_down()

    for side in SIDES:
        for c in copies[side]:
            c.wait()


ADJ = 64
FAR_ROWS = 48
ADJ_ROWS = ROWS + ADJ
BLOCK = 512
BLOCKS = SW // BLOCK
OWN = 256
GHOST_TILES = 8 * LANE_TILES + 4


def fluid_kernel(pops, own, base, halo_x, halo_y, halo_c, lists, starts_in, mom, inner, zhl, plane,
                 next_out, force_out,
                 acc, out_v, force_v, starts, node, near, outer, force, ghosts, cols, out_sem, start_sem, force_sem):
    start_copy = pltpu.make_async_copy(starts_in, starts, start_sem)
    start_copy.start()
    acc[...] = base[...]
    ghosts[...] = jnp.zeros(ghosts.shape, F32)
    force[...] = jnp.zeros(force.shape, F32)
    for c in range(3):
        corner = []
        for i in range(4):
            for j in range(4):
                sx, sy = (0 if i < 2 else 1), (0 if j < 2 else 1)
                fx, fy = i in (0, 3), j in (0, 3)
                k = 2 * sx + sy
                r = (11 if fy else 8) if fx else (5 if fy else 1)
                corner.append(halo_c[k, r + c:r + c + 1])
        near[c * ADJ:(c + 1) * ADJ] = widen(jnp.concatenate(
            [halo_x[0, 1 + c], halo_x[1, 1 + c], halo_y[0, 1 + c], halo_y[1, 1 + c]] + corner, axis=0))
        outer[c * FAR_ROWS:(c + 1) * FAR_ROWS] = widen(jnp.concatenate(
            [halo_x[0, 4 + c], halo_x[1, 4 + c], halo_y[0, 4 + c], halo_y[1, 4 + c]], axis=0))

    def spread(weights, react, zz):
        zh = zz[0:NZ]
        for c in range(3):
            wh, wl = split2(weights * react[c])
            both = dot_t(wh, zz)
            force[c] = force[c] + (both[:, :128] + both[:, 128:] + dot_t(wl, zh))

    per = BLOCK // OWN

    def own_block(i, carry):
        zz = zhl[i]
        got = sample(near[...], zz[0:NZ], zz[NZ:2 * NZ])
        vals = jnp.concatenate([own[per * i + j] for j in range(per)], axis=1)
        react = []
        for c in range(3):
            s = jnp.sum(got[c * ADJ:(c + 1) * ADJ] * plane[i, ROWS:ADJ_ROWS], axis=0, keepdims=True)
            s = 2.0 * s * vals[6:7]
            react.append(vals[3 + c:4 + c] - s)
            for j in range(per):
                acc[per * i + j, c:c + 1] = acc[per * i + j, c:c + 1] + s[:, j * OWN:(j + 1) * OWN]
        spread(plane[i], react, zz)
        return carry

    own_block(0, 0)
    start_copy.wait()
    n_own = starts[8, 0, 9].astype(jnp.int32)

    lane = lax.broadcasted_iota(jnp.int32, (8, 128), 1)
    sub = lax.broadcasted_iota(jnp.int32, (8, 128), 0)
    total = jnp.int32(0)
    puts, rest = [], []
    for d, lo, hi in RANGES:
        a = starts[d, 0, lo].astype(jnp.int32)
        b = starts[d, 0, hi].astype(jnp.int32)
        sx, sy = SIDES[d]
        moved = jnp.where(sub == 0, float(sx * CX), jnp.where(sub == 1, float(sy * CY), 0.0))
        by = (total - a) & 127
        upper = lane >= by

        def taken(t, d=d, a=a, b=b, by=by, moved=moved):
            at = t * 128 + lane
            v = jnp.where((at >= a) & (at < b), lists[d, jnp.minimum(t, LANE_TILES - 1)] + moved, 0.0)
            return pltpu.roll(v, by, 1)

        t0 = lax.shift_right_logical(a, 7)
        tile = lax.shift_right_logical(total - a + t0 * 128 + 1024, 7) - 8
        v0, v1 = taken(t0), taken(t0 + 1)
        puts.append((jnp.maximum(tile, 0), jnp.where(upper, v0, 0.0)))
        puts.append((tile + 1, jnp.where(upper, v1, v0)))
        puts.append((tile + 2, jnp.where(upper, 0.0, v1)))

        def more(t, carry, taken=taken, upper=upper, shift=tile - t0):
            v = taken(t)
            ghosts[t + shift] = ghosts[t + shift] + jnp.where(upper, v, 0.0)
            ghosts[t + shift + 1] = ghosts[t + shift + 1] + jnp.where(upper, 0.0, v)
            return carry

        rest.append((t0 + 2, lax.shift_right_logical(b + 127, 7), more))
        total = total + (b - a)
    for at, v in puts:
        ghosts[at] = ghosts[at] + v
    for lo, hi, more in rest:
        lax.fori_loop(lo, hi, more, 0)

    slot = lax.broadcasted_iota(jnp.int32, (1, BLOCK), 1)
    tiles = lax.shift_right_logical(total + 127, 7)
    ahead = BLOCK // 128

    def ghost_columns(t, carry):
        g = jnp.where((sub == 0) & (lane + t * 128 >= total), FAR, ghosts[t])
        turned = jnp.transpose(g)
        at = t * 128 if isinstance(t, int) else pl.multiple_of(t * 128, 128)
        for c in range(3):
            cols[c, pl.ds(at, 128)] = jnp.broadcast_to(turned[:, c:c + 1], (128, 128))
        return carry

    def ghost_block(i, carry):
        vals = jnp.concatenate([ghosts[ahead * i + j] for j in range(ahead)], axis=1)
        live = (slot + i * BLOCK < total).astype(F32)
        zh, zl = z_weights(vals[2:3])
        weights = plane_weights(vals[0:1], vals[1:2], True)
        gi = sample(inner[...], zh, zl)
        gn = sample(near[...], zh, zl)
        gf = sample(outer[...], zh, zl)
        react = []
        for c in range(3):
            s = (jnp.sum(gi[c * ROWS:(c + 1) * ROWS] * weights[0:ROWS], axis=0, keepdims=True)
                 + jnp.sum(gn[c * ADJ:(c + 1) * ADJ] * weights[ROWS:ADJ_ROWS], axis=0, keepdims=True)
                 + jnp.sum(gf[c * FAR_ROWS:(c + 1) * FAR_ROWS] * weights[ADJ_ROWS:], axis=0, keepdims=True))
            react.append((vals[3 + c:4 + c] - 2.0 * s) * live)
        spread(weights[0:ADJ_ROWS], react, jnp.concatenate([zh, zl], axis=0))
        return carry

    for t in range(ahead):
        ghost_columns(t, 0)
    ghost_block(0, 0)
    lax.fori_loop(ahead, tiles, ghost_columns, 0)
    lax.fori_loop(1, lax.shift_right_logical(total + BLOCK - 1, 9), ghost_block, 0)
    lax.fori_loop(1, lax.shift_right_logical(n_own + BLOCK - 1, 9), own_block, 0)

    def ghost_pairs(i, carry):
        mine = [jnp.broadcast_to(own[i, c:c + 1], (8, OWN)) for c in range(3)]
        one = pair_step(cols, mine, OWN)
        init = tuple(jnp.zeros((8, OWN), F32) for _ in range(3))

        def four(n, got):
            for k in range(4):
                got = one(4 * n + k, got)
            return got

        got = lax.fori_loop(0, lax.shift_right_logical(total + 31, 5), four, init)
        live = own[i, 6:7]
        for c in range(3):
            acc[i, c:c + 1] = acc[i, c:c + 1] + 0.24 * live * jnp.sum(got[c], axis=0, keepdims=True)
        return carry

    lax.fori_loop(0, lax.shift_right_logical(n_own + OWN - 1, 8), ghost_pairs, 0)
    for i in range(SW // OWN):
        for c in range(3):
            for j in range(2):
                r = c * LANE_TILES + 2 * i + j
                force_v[r:r + 1] = acc[i, c:c + 1, j * 128:(j + 1) * 128]
    force_copy = pltpu.make_async_copy(force_v, force_out, force_sem)
    force_copy.start()

    def prepare(rho, u0, half, g):
        u = [u0[c] + half * g[c] for c in range(3)]
        uu = u[0] * u[0] + u[1] * u[1] + u[2] * u[2]
        ug = u[0] * g[0] + u[1] * g[1] + u[2] * g[2]
        k0 = 1.25 * rho * (1.0 - 1.5 * uu) - 1.125 * ug
        return k0, 3.75 * rho, 5.625 * rho, u, [1.125 * v for v in g]

    def along(q, v):
        out = None
        for c in range(3):
            s = DIRS[q][c]
            if s:
                out = (v[c] if s > 0 else -v[c]) if out is None else (out + v[c] if s > 0 else out - v[c])
        return out

    def post(q, f, prep):
        k0, r1, r2, u, g = prep
        if q == 0:
            return -0.25 * f + WEIGHTS[0] * k0
        a, p = along(q, u), along(q, g)
        return -0.25 * f + WEIGHTS[q] * (k0 + a * (r1 + r2 * a + 3.0 * p) + p)

    def side_prep(rho, u0, lo, n):
        g = [force[c, lo:lo + n] for c in range(3)]
        return prepare(rho, u0, 0.5 / rho, g)

    k0, r1, r2, u, g = side_prep(mom[0], [mom[1 + c] for c in range(3)], 0, ROWS)
    node[0] = k0
    for c in range(3):
        node[1 + c] = u[c]
        node[4 + c] = g[c]
    xs = [side_prep(halo_x[s, 0], [halo_x[s, 1 + c] for c in range(3)], ROWS + s * CY, CY) for s in range(2)]
    ys = [side_prep(halo_y[s, 0], [halo_y[s, 1 + c] for c in range(3)], ROWS + 2 * CY + s * CX, CX)
          for s in range(2)]
    cs = []
    for i in range(4):
        sx, sy = SIDES[4 + i]
        r = ADJ_ROWS - 16 + (1 if sx < 0 else 2) * 4 + (1 if sy < 0 else 2)
        cs.append(side_prep(halo_c[i, 0:1], [halo_c[i, 1 + c:2 + c] for c in range(3)], r, 1))
    stores = []
    for q in range(19):
        dx, dy, dz = DIRS[q]
        rho_q = mom[0]
        prep = (node[0], 3.75 * rho_q, 5.625 * rho_q, [node[1 + c] for c in range(3)], [node[4 + c] for c in range(3)])

        def turned(v, dz=dz):
            return pltpu.roll(v, dz % NZ, 1) if dz else v

        v = turned(post(q, pops[q], prep))
        if dy:
            v = pltpu.roll(v, dy % ROWS, 0)
        if dx == 0:
            out_v[q] = v
        else:
            s = 0 if dx > 0 else 1
            e = turned(post(q, halo_x[s, 7 + facing(0, dx).index(q)], xs[s]))
            if dy:
                e = pltpu.roll(e, dy % CY, 0)
            if dx > 0:
                out_v[q, CY:ROWS] = v[0:ROWS - CY]
                out_v[q, 0:CY] = e
            else:
                out_v[q, 0:ROWS - CY] = v[CY:ROWS]
                out_v[q, ROWS - CY:ROWS] = e
        if dy:
            s = 0 if dy > 0 else 1
            at = 0 if dy > 0 else CY - 1
            e = turned(post(q, halo_y[s, 7 + facing(1, dy).index(q)], ys[s]))
            if dx:
                e = pltpu.roll(e, dx % CX, 0)
            out_v[q, pl.ds(at, CX, stride=CY)] = e
            if dx:
                i = SIDES.index((-dx, -dy)) - 4
                r = at + (0 if dx > 0 else (CX - 1) * CY)
                out_v[q, r:r + 1] = post(q, halo_c[i, 4:5], cs[i])
        c = pltpu.make_async_copy(out_v.at[q], next_out.at[q], out_sem.at[q])
        c.start()
        stores.append(c)
    force_copy.wait()
    for c in stores:
        c.wait()


def body(n_gx, n_gy, populations, anchor, offsets, heading, velocity, live_count):
    pops = populations.reshape(19, ROWS, NZ)
    tiles = LANE_TILES
    vmem = pl.BlockSpec(memory_space=pltpu.VMEM)
    hbm = pl.BlockSpec(memory_space=pltpu.HBM)
    dma = pltpu.SemaphoreType.DMA
    held = (
        pltpu.VMEM((19, ROWS, NZ), F32),
        pltpu.VMEM((2, 12, CY, 128), F32),
        pltpu.VMEM((2, 12, CX, 128), F32),
        pltpu.VMEM((4, 16, 128), F32),
        pltpu.VMEM((8, LANE_TILES, 8, 128), F32),
        pltpu.VMEM((9, 1, 128), F32),
        pltpu.VMEM((SW // OWN, 8, OWN), F32),
        pltpu.VMEM((SW // OWN, 8, OWN), F32),
        pltpu.VMEM((4, ROWS, NZ), F32),
        pltpu.VMEM((3 * ROWS, 2 * NZ), BF16),
        pltpu.VMEM((BLOCKS, 2 * NZ, BLOCK), BF16),
        pltpu.VMEM((BLOCKS, ADJ_ROWS, BLOCK), F32),
    )
    pops, halo_x, halo_y, halo_c, lists, starts, own, base, mom, inner, zhl, plane = pl.pallas_call(
        functools.partial(exchange_kernel, n_gx, n_gy),
        out_shape=held,
        in_specs=[hbm] * 6,
        out_specs=[vmem] * 12,
        scratch_shapes=[
            pltpu.VMEM((tiles, 128), jnp.int32),
            pltpu.VMEM((3 * tiles, 128), F32),
            pltpu.VMEM((2 * tiles, 128), F32),
            pltpu.VMEM((3 * tiles, 128), F32),
            pltpu.SMEM((1,), jnp.int32),
            pltpu.VMEM((8 * tiles, 128), F32),
            pltpu.VMEM((2, 12, CY, 128), F32),
            pltpu.VMEM((2, 12, CX, 128), F32),
            pltpu.VMEM((4, 16, 128), F32),
            pltpu.VMEM((LANE_TILES, 8, 128), F32),
            pltpu.VMEM((1, 128), F32),
            pltpu.VMEM((3, SW, 128), F32),
            dma((9,)), dma((24,)), dma((24,)), pltpu.SemaphoreType.REGULAR,
        ],
        compiler_params=pltpu.CompilerParams(collective_id=0, has_side_effects=True, vmem_limit_bytes=20 << 20),
        name="exchange",
    )(*[pltpu.with_memory_space_constraint(v, pltpu.HBM) for v in (
        pops, anchor.reshape(tiles, 128), offsets.reshape(3 * tiles, 128),
        jnp.swapaxes(heading.reshape(2, tiles, 128), 0, 1).reshape(2 * tiles, 128),
        velocity.reshape(3 * tiles, 128))], live_count.reshape(1))
    moved, force = pl.pallas_call(
        fluid_kernel,
        out_shape=(jax.ShapeDtypeStruct((19, ROWS, NZ), F32), jax.ShapeDtypeStruct((3 * tiles, 128), F32)),
        in_specs=[vmem] * 12,
        out_specs=[hbm, hbm],
        scratch_shapes=[
            pltpu.VMEM((SW // OWN, 8, OWN), F32),
            pltpu.VMEM((19, ROWS, NZ), F32),
            pltpu.VMEM((3 * tiles, 128), F32),
            pltpu.SMEM((9, 1, 128), F32),
            pltpu.VMEM((7, ROWS, NZ), F32),
            pltpu.VMEM((3 * ADJ, 2 * NZ), BF16),
            pltpu.VMEM((3 * FAR_ROWS, 2 * NZ), BF16),
            pltpu.VMEM((3, ADJ_ROWS, NZ), F32),
            pltpu.VMEM((GHOST_TILES, 8, 128), F32),
            pltpu.VMEM((3, GHOST_TILES * 128, 128), F32),
            dma((19,)), dma, dma,
        ],
        compiler_params=pltpu.CompilerParams(vmem_limit_bytes=32 << 20),
        name="fluid",
    )(pops, own, base, halo_x, halo_y, halo_c, lists, starts, mom, inner, zhl, plane)
    return (moved.reshape(populations.shape), force.reshape(1, 1, 3, SW))


def solution(mesh):
    return jax.shard_map(
        functools.partial(body, mesh.shape["gx"], mesh.shape["gy"]),
        mesh=mesh,
        in_specs=(
            P(None, "gx", "gy", None),
            P("gx", "gy", None),
            P("gx", "gy", None, None),
            P("gx", "gy", None, None),
            P("gx", "gy", None, None),
            P("gx", "gy"),
        ),
        out_specs=(P(None, "gx", "gy", None), P("gx", "gy", None, None)),
        check_vma=False,
    )
```

```python
import functools

import jax
import jax.numpy as jnp
import numpy as np
from jax import lax
from jax.experimental import pallas as pl
from jax.experimental.pallas import tpu as pltpu
from jax.sharding import PartitionSpec as P

DIRS = (
    (0, 0, 0), (1, 0, 0), (-1, 0, 0), (0, 1, 0), (0, -1, 0), (0, 0, 1), (0, 0, -1),
    (1, 1, 0), (-1, -1, 0), (1, -1, 0), (-1, 1, 0), (1, 0, 1), (-1, 0, -1),
    (1, 0, -1), (-1, 0, 1), (0, 1, 1), (0, -1, -1), (0, 1, -1), (0, -1, 1),
)
WEIGHTS = (1.0 / 3.0,) + (1.0 / 18.0,) * 6 + (1.0 / 36.0,) * 12
CUTOFF = 2.0 ** (1.0 / 3.0)
REACH = 1.125
FAR = 1.0e9
F32 = jnp.float32
BF16 = jnp.bfloat16
MESH = pl.DeviceIdType.MESH

CX, CY, NZ, SW = 8, 16, 128, 1024
ROWS = CX * CY
LANE_TILES = SW // 128

SIDES = ((-1, 0), (1, 0), (0, -1), (0, 1), (-1, -1), (-1, 1), (1, -1), (1, 1))
RANGES = ((0, 4, 7), (1, 0, 3), (2, 2, 5), (3, 6, 8), (3, 0, 1), (4, 4, 5), (5, 6, 7), (6, 2, 3), (7, 0, 1))


def facing(axis, sign):
    return [q for q in range(19) if DIRS[q][axis] == sign]


def corner_q(sx, sy):
    return DIRS.index((-sx, -sy, 0))


def split2(v):
    hi = v.astype(BF16)
    return hi, (v - hi.astype(F32)).astype(BF16)


def split3(v):
    hi = v.astype(BF16)
    rest = v - hi.astype(F32)
    mid = rest.astype(BF16)
    return hi, mid, (rest - mid.astype(F32)).astype(BF16)


def dot(a, b):
    return lax.dot_general(a, b, (((1,), (0,)), ((), ())), preferred_element_type=F32)


def dot_t(a, b):
    return lax.dot_general(a, b, (((1,), (1,)), ((), ())), preferred_element_type=F32)


def tent(d):
    return jnp.maximum(1.0 - jnp.abs(d), 0.0)


def moments(load):
    rho = None
    mom = [None, None, None]
    for q in range(19):
        f = load(q)
        rho = f if rho is None else rho + f
        for c in range(3):
            s = DIRS[q][c]
            if s:
                if mom[c] is None:
                    mom[c] = f if s > 0 else -f
                else:
                    mom[c] = mom[c] + f if s > 0 else mom[c] - f
    return rho, mom


def pair_terms(ox, oy, oz, px, py, pz):
    dx = ox - px
    dy = oy - py
    dz = oz - pz
    dz = dz - NZ * jnp.round(dz * (1.0 / NZ))
    raw = dx * dx + dy * dy + dz * dz
    inv = 1.0 / jnp.maximum(raw, 0.8)
    sixth = inv * inv * inv
    mag = (sixth + sixth - 1.0) * (sixth * inv)
    mag = jnp.where(raw < CUTOFF, mag, 0.0)
    return mag * dx, mag * dy, mag * dz


def classes(x, y, live):
    xl, xh = x < REACH, x > CX - 1 - REACH
    yl, yh = y < REACH, y > CY - 1 - REACH
    yc = jnp.where(yl, 0.0, jnp.where(yh, 2.0, 1.0))
    kind = jnp.where(xl, yc, jnp.where(xh, 6.0 - yc, jnp.where(yl, 7.0, jnp.where(yh, 3.0, 8.0))))
    return jnp.where(live > 0.0, kind, 9.0)


def sort_ranks(kind):
    masks = [(kind == k).astype(F32) for k in range(10)]
    ri = lax.broadcasted_iota(jnp.int32, (128, 256), 0)
    ci = lax.broadcasted_iota(jnp.int32, (128, 256), 1)
    upper = ((ri < ci) | (ci >= 128)).astype(F32).astype(BF16)
    pre = dot(jnp.concatenate(masks, axis=0).astype(BF16), upper)
    within, tile_sum = pre[:, :128], pre[:, 128:]
    place = lax.broadcasted_iota(jnp.int32, (80, 128), 0) & 7
    upto = tile_sum
    for by in (1, 2, 4):
        upto = upto + jnp.where(place >= by, pltpu.roll(upto, by, 0), 0.0)
    lane = lax.broadcasted_iota(jnp.int32, (1, 128), 1)
    rank = jnp.zeros((8, 128), F32)
    row = jnp.zeros((1, 128), F32)
    first = jnp.zeros((1, 128), F32)
    for k in range(10):
        cut = slice(8 * k, 8 * k + 8)
        row = jnp.where(lane == k, first, row)
        rank = rank + masks[k] * (within[cut] + (upto[cut] - tile_sum[cut]) + first)
        first = first + upto[8 * k + 7:8 * k + 8]
    return rank, row


def plane_weights(px, py, far):
    x8 = lax.broadcasted_iota(jnp.int32, (CX, 1), 0).astype(F32)
    y16 = lax.broadcasted_iota(jnp.int32, (CY, 1), 0).astype(F32)
    ki = lax.broadcasted_iota(jnp.int32, (16, 1), 0)
    ii, jj = lax.shift_right_logical(ki, 2), ki & 3
    xd = jnp.where(ii < 2, ii - 2, ii + CX - 2).astype(F32)
    yd = jnp.where(jj < 2, jj - 2, jj + CY - 2).astype(F32)
    tx, ty = tent(x8 - px), tent(y16 - py)
    parts = [tx[i:i + 1] * ty for i in range(CX)]
    parts += [tent(-1.0 - px) * ty, tent(CX - px) * ty, tent(-1.0 - py) * tx, tent(CY - py) * tx]
    parts += [tent(xd - px) * tent(yd - py)]
    if far:
        parts += [tent(-2.0 - px) * ty, tent(CX + 1.0 - px) * ty, tent(-2.0 - py) * tx, tent(CY + 1.0 - py) * tx]
    return jnp.concatenate(parts, axis=0)


def z_weights(pz):
    zi = lax.broadcasted_iota(jnp.int32, (NZ, 1), 0).astype(F32)
    return split2(tent(zi - pz))


def widen(v):
    hi, lo = split2(v)
    return jnp.concatenate([hi, lo], axis=1)


def sample(u, zh, zl):
    return dot(u, jnp.concatenate([zh, zh], axis=0)) + dot(u[:, :128], zl)


def columns(cols, at, place):
    turned = jnp.transpose(place)
    for c in range(3):
        cols[c, at:at + 128] = jnp.broadcast_to(turned[:, c:c + 1], (128, 128))


def pair_step(cols, mine, width):
    def step(n, acc):
        at = pl.multiple_of(n * 8, 8)
        p = [jnp.concatenate([cols[c, pl.ds(at, 8)]] * (width // 128), axis=1) for c in range(3)]
        return tuple(a + b for a, b in zip(acc, pair_terms(*mine, *p)))

    return step


def exchange_kernel(n_gx, n_gy, pops_hbm, anchor_hbm, offsets_hbm, heading_hbm, velocity_hbm, count_hbm,
                    pops, halo_x, halo_y, halo_c, lists, starts_out, own_out, base_out, mom, inner, zhl, plane, cols,
                    anchor, offsets, heading, velocity, count, table,
                    msg_x, msg_y, msg_c, msg_l, msg_s, load_sem, send_sem, recv_sem, face_send, face_recv, lower, beside):
    gx = lax.axis_index("gx")
    gy = lax.axis_index("gy")

    def device(side):
        return (lax.rem(gx + side[0] + n_gx, n_gx), lax.rem(gy + side[1] + n_gy, n_gy))

    loads = [pltpu.make_async_copy(a, b, load_sem.at[k]) for k, (a, b) in enumerate((
        (anchor_hbm, anchor), (offsets_hbm, offsets), (heading_hbm, heading), (velocity_hbm, velocity),
        (count_hbm, count)))]
    loads += [pltpu.make_async_copy(pops_hbm.at[pl.ds(q, n)], pops.at[pl.ds(q, n)], load_sem.at[5 + k])
              for k, (q, n) in enumerate(((0, 5), (5, 5), (10, 5), (15, 4)))]
    for c in loads:
        c.start()
    even = lax.rem(gy, 2) == 0
    odd = jnp.logical_not(even)
    barrier = pltpu.get_barrier_semaphore()

    def tell(semaphore, sides):
        for side in sides:
            pl.semaphore_signal(semaphore, inc=1, device_id=device(side), device_id_type=MESH)

    corners_up, along_y, down = ((1, -1), (1, 1)), ((0, -1), (0, 1)), ((-1, 0), (-1, -1), (-1, 1))
    tell(barrier, down)

    @pl.when(even)
    def _():
        tell(barrier, along_y)
        pl.semaphore_wait(barrier, 3)

    @pl.when(odd)
    def _():
        pl.semaphore_wait(barrier, 5)
        tell(beside, along_y)

    tell(lower, ((1, 0),) + corners_up)

    face = []
    for d in range(2):
        for k, q in enumerate(facing(0, 2 * d - 1)):
            face.append(pltpu.make_async_remote_copy(
                src_ref=pops_hbm.at[q, pl.ds(d * (ROWS - CY), CY)], dst_ref=halo_x.at[1 - d, 7 + k],
                send_sem=face_send.at[5 * d + k], recv_sem=face_recv.at[5 * (1 - d) + k],
                device_id=device(SIDES[d]), device_id_type=MESH))
    for c in face[5:]:
        c.start()

    group = max(n_gx // 4, 1)
    head = (lax.rem(gx, group) == 0) & (gx != 0)
    idle = (gx == 0) | ((lax.rem(gx, group) == group - 1) & (gx != n_gx - 1))

    @pl.when(head)
    def _():
        pl.semaphore_wait(lower, 3)
        for c in face[:5]:
            c.start()

    for c in loads[:5]:
        c.wait()

    root = anchor[...]
    bxf = lax.shift_right_logical(root, 7).astype(F32)
    cxf = jnp.floor(bxf * (1.0 / (CY + 2)) + 0.01)
    x = cxf - 1.0 + offsets[0:8]
    y = bxf - cxf * (CY + 2) - 1.0 + offsets[8:16]
    z = (root & (NZ - 1)).astype(F32) + offsets[16:24]
    lane = lax.broadcasted_iota(jnp.int32, (8, 128), 1)
    sub = lax.broadcasted_iota(jnp.int32, (8, 128), 0)
    live = (sub * 128 + lane < count[0]).astype(F32)
    first, second = heading[pl.ds(0, 8, stride=2)], heading[pl.ds(1, 8, stride=2)]
    c1 = jnp.cos(second)
    w = [2.0 * velocity[0:8] - 0.5 * (jnp.cos(first) * c1),
         2.0 * velocity[8:16] - 0.5 * (jnp.sin(first) * c1),
         2.0 * velocity[16:24] - 0.5 * jnp.sin(second)]
    for k, v in enumerate((x, y, z, *w, live, jnp.zeros((8, 128), F32))):
        table[pl.ds(k, 8, stride=8)] = v
    rank, row = sort_ranks(classes(x, y, live))
    msg_s[...] = row
    starts_out[8] = jnp.where(lane[0:1] == 10, idle.astype(F32), row)
    to_tile = jnp.floor(rank * (1.0 / 128.0))
    to_lane = rank - 128.0 * to_tile
    split = [v.astype(F32) for v in split3(table[...])]
    dst = lax.broadcasted_iota(jnp.int32, (128, 128), 0).astype(F32)
    ordered = jnp.zeros((24 * LANE_TILES, 128), F32)
    for t in range(0, LANE_TILES, 2):
        hot, rows = [], []
        for j in (t, t + 1):
            hot.append((dst == to_lane[j:j + 1]).astype(F32).astype(BF16))
            part = jnp.concatenate([v[8 * j:8 * j + 8] for v in split], axis=0)
            rows.append(jnp.concatenate(
                [jnp.where(to_tile[j:j + 1] == float(k), part, 0.0) for k in range(LANE_TILES)],
                axis=0).astype(BF16))
        ordered = ordered + dot_t(jnp.concatenate(rows, axis=1), jnp.concatenate(hot, axis=1))
    for t in range(LANE_TILES):
        at = 24 * t
        msg_l[t] = ordered[at:at + 8] + ordered[at + 8:at + 16] + ordered[at + 16:at + 24]

    def send(k, a, b, side, o):
        d = SIDES.index(side)
        return pltpu.make_async_remote_copy(
            src_ref=a, dst_ref=b, send_sem=send_sem.at[3 * d + k], recv_sem=recv_sem.at[3 * o + k],
            device_id=device(side), device_id_type=MESH)

    copies = {}
    for d, side in enumerate(SIDES):
        o = SIDES.index((-side[0], -side[1]))
        if side[1] == 0:
            first = send(0, msg_x.at[d], halo_x.at[o, pl.ds(0, 7)], side, o)
        elif side[0] == 0:
            first = send(0, msg_y.at[d - 2], halo_y.at[o - 2], side, o)
        else:
            first = send(0, msg_c.at[d - 4], halo_c.at[o - 4], side, o)
        copies[side] = (first, send(1, msg_s, starts_out.at[o], side, o),
                        send(2, msg_l.at[:, pl.ds(0, 6)], lists.at[o, :, pl.ds(0, 6)], side, o))

    def start(sides, kinds=(0, 1, 2)):
        for k in kinds:
            for side in sides:
                copies[side][k].start()

    last = gx == n_gx - 1
    late = gx >= n_gx - max(n_gx // 4, 1)

    @pl.when(last)
    def _():
        start(corners_up, (1, 2))

    @pl.when(head)
    def _():
        start(down, (1, 2))

    start(((1, 0),), (1, 2))

    for c in loads[5:]:
        c.wait()
    rho, m = moments(lambda q: pops[q])
    inv = 1.0 / rho
    mom[0] = rho
    for c in range(3):
        mom[1 + c] = m[c] * inv
    for s, (adj, far) in enumerate(((0, 1), (CX - 1, CX - 2))):
        for c in range(4):
            msg_x[s, c] = mom[c, adj * CY:(adj + 1) * CY]
        for c in range(3):
            msg_x[s, 4 + c] = mom[1 + c, far * CY:(far + 1) * CY]

    for i in range(4):
        sx, sy = SIDES[4 + i]
        ax, fx = (0, 1) if sx < 0 else (CX - 1, CX - 2)
        ay, fy = (0, 1) if sy < 0 else (CY - 1, CY - 2)
        msg_c[i] = jnp.zeros((16, 128), F32)
        for c in range(4):
            msg_c[i, c:c + 1] = mom[c, ax * CY + ay:ax * CY + ay + 1]
        for j, (nx, ny) in enumerate(((ax, fy), (fx, ay), (fx, fy))):
            for c in range(3):
                msg_c[i, 5 + 3 * j + c:6 + 3 * j + c] = mom[1 + c, nx * CY + ny:nx * CY + ny + 1]
        q = DIRS.index((sx, sy, 0))
        msg_c[i, 4:5] = pops[q, ax * CY + ay:ax * CY + ay + 1]


    @pl.when(last)
    def _():
        start(corners_up, (0,))

    @pl.when(head)
    def _():
        start(down, (0,))

    start(((1, 0),), (0,))
    for s, (adj, far) in enumerate(((0, 1), (CY - 1, CY - 2))):
        for c in range(4):
            msg_y[s, c] = mom[c, pl.ds(adj, CX, stride=CY)]
        for c in range(3):
            msg_y[s, 4 + c] = mom[1 + c, pl.ds(far, CX, stride=CY)]
        for k, q in enumerate(facing(1, 2 * s - 1)):
            msg_y[s, 7 + k] = pops[q, pl.ds(adj, CX, stride=CY)]
    def own_pairs():
        for i in range(0, SW // OWN, 2):
            width = 2 * OWN
            mine = [jnp.broadcast_to(jnp.concatenate([own_out[i, c:c + 1], own_out[i + 1, c:c + 1]], axis=1), (8, width))
                    for c in range(3)]
            init = tuple(jnp.zeros((8, width), F32) for _ in range(3))
            got = lax.fori_loop(0, SW // 8, pair_step(cols, mine, width), init)
            for c in range(3):
                pairs = 0.24 * jnp.sum(got[c], axis=0, keepdims=True)
                for j in range(2):
                    base_out[i + j, c:c + 1] = (base_out[i + j, c:c + 1]
                                                + pairs[:, j * OWN:(j + 1) * OWN] * own_out[i + j, 6:7])

    def send_down():
        pl.semaphore_wait(lower, 3)
        for c in face[:5]:
            c.start()
        start(down)

    def send_along():
        @pl.when(even)
        def _():
            pl.semaphore_wait(beside, 2)

        start(along_y)

    @pl.when(jnp.logical_not(late))
    def _():
        send_along()
        start(corners_up)

    @pl.when(jnp.logical_not(late | head) & (gx != 0))
    def _():
        send_down()

    for c in range(3):
        inner[c * ROWS:(c + 1) * ROWS] = widen(mom[1 + c])
    for i in range(BLOCKS):
        n = BLOCK // 128
        vals = jnp.concatenate([table[8 * (n * i + j):8 * (n * i + j) + 8] for j in range(n)], axis=1)
        zh, zl = z_weights(vals[2:3])
        zhl[i, 0:NZ] = zh
        zhl[i, NZ:2 * NZ] = zl
        plane[i] = plane_weights(vals[0:1], vals[1:2], False)
        got = sample(inner[...], zh, zl)
        rows = [vals[0:3]]
        for c in range(3):
            s = jnp.sum(got[c * ROWS:(c + 1) * ROWS] * plane[i, 0:ROWS], axis=0, keepdims=True)
            rows.append((vals[3 + c:4 + c] - 2.0 * s) * vals[6:7])
        rows = jnp.concatenate(rows + [vals[6:8]], axis=0)
        for j in range(BLOCK // OWN):
            own_out[i * (BLOCK // OWN) + j] = rows[:, j * OWN:(j + 1) * OWN]

    @pl.when(late)
    def _():
        send_along()

    @pl.when(late & jnp.logical_not(last))
    def _():
        start(corners_up)

    @pl.when(late & jnp.logical_not(head))
    def _():
        send_down()

    for t in range(LANE_TILES):
        v = table[8 * t:8 * t + 8]
        columns(cols, t * 128, jnp.where((sub == 0) & (v[6:7] == 0.0), FAR, v))
    for i in range(SW // OWN):
        base_out[i] = jnp.concatenate([-own_out[i, 3:6], jnp.zeros((5, OWN), F32)], axis=0)

    @pl.when(idle)
    def _():
        own_pairs()

    @pl.when(gx == 0)
    def _():
        send_down()

    for c in face:
        c.wait()
    for side in SIDES:
        for c in copies[side]:
            c.wait()


ADJ = 64
FAR_ROWS = 48
ADJ_ROWS = ROWS + ADJ
BLOCK = 512
BLOCKS = SW // BLOCK
OWN = 256
GHOSTS = 384
GHOST_TILES = 8 * LANE_TILES + 4


def fluid_kernel(pops, own, base, halo_x, halo_y, halo_c, lists, starts_in, mom, inner, zhl, plane, own_cols,
                 next_out, force_out,
                 acc, out_v, force_v, starts, node, near, outer, force, ghosts, cols, out_sem, start_sem, force_sem):
    start_copy = pltpu.make_async_copy(starts_in, starts, start_sem)
    start_copy.start()
    acc[...] = base[...]
    ghosts[...] = jnp.zeros(ghosts.shape, F32)
    force[...] = jnp.zeros(force.shape, F32)
    for c in range(3):
        corner = []
        for i in range(4):
            for j in range(4):
                sx, sy = (0 if i < 2 else 1), (0 if j < 2 else 1)
                fx, fy = i in (0, 3), j in (0, 3)
                k = 2 * sx + sy
                r = (11 if fy else 8) if fx else (5 if fy else 1)
                corner.append(halo_c[k, r + c:r + c + 1])
        near[c * ADJ:(c + 1) * ADJ] = widen(jnp.concatenate(
            [halo_x[0, 1 + c], halo_x[1, 1 + c], halo_y[0, 1 + c], halo_y[1, 1 + c]] + corner, axis=0))
        outer[c * FAR_ROWS:(c + 1) * FAR_ROWS] = widen(jnp.concatenate(
            [halo_x[0, 4 + c], halo_x[1, 4 + c], halo_y[0, 4 + c], halo_y[1, 4 + c]], axis=0))

    def spread(weights, react, zz):
        zh = zz[0:NZ]
        for c in range(3):
            wh, wl = split2(weights * react[c])
            both = dot_t(wh, zz)
            force[c] = force[c] + (both[:, :128] + both[:, 128:] + dot_t(wl, zh))

    per = BLOCK // OWN

    def own_block(i, carry):
        zz = zhl[i]
        got = sample(near[...], zz[0:NZ], zz[NZ:2 * NZ])
        vals = jnp.concatenate([own[per * i + j] for j in range(per)], axis=1)
        react = []
        for c in range(3):
            s = jnp.sum(got[c * ADJ:(c + 1) * ADJ] * plane[i, ROWS:ADJ_ROWS], axis=0, keepdims=True)
            s = 2.0 * s * vals[6:7]
            react.append(vals[3 + c:4 + c] - s)
            for j in range(per):
                acc[per * i + j, c:c + 1] = acc[per * i + j, c:c + 1] + s[:, j * OWN:(j + 1) * OWN]
        spread(plane[i], react, zz)
        return carry

    own_block(0, 0)
    start_copy.wait()
    n_own = starts[8, 0, 9].astype(jnp.int32)

    lane = lax.broadcasted_iota(jnp.int32, (8, 128), 1)
    sub = lax.broadcasted_iota(jnp.int32, (8, 128), 0)
    total = jnp.int32(0)
    puts, rest = [], []
    for d, lo, hi in RANGES:
        a = starts[d, 0, lo].astype(jnp.int32)
        b = starts[d, 0, hi].astype(jnp.int32)
        sx, sy = SIDES[d]
        moved = jnp.where(sub == 0, float(sx * CX), jnp.where(sub == 1, float(sy * CY), 0.0))
        by = (total - a) & 127
        upper = lane >= by

        def taken(t, d=d, a=a, b=b, by=by, moved=moved):
            at = t * 128 + lane
            v = jnp.where((at >= a) & (at < b), lists[d, jnp.minimum(t, LANE_TILES - 1)] + moved, 0.0)
            return pltpu.roll(v, by, 1)

        t0 = lax.shift_right_logical(a, 7)
        tile = lax.shift_right_logical(total - a + t0 * 128 + 1024, 7) - 8
        v0, v1 = taken(t0), taken(t0 + 1)
        puts.append((jnp.maximum(tile, 0), jnp.where(upper, v0, 0.0)))
        puts.append((tile + 1, jnp.where(upper, v1, v0)))
        puts.append((tile + 2, jnp.where(upper, 0.0, v1)))

        def more(t, carry, taken=taken, upper=upper, shift=tile - t0):
            v = taken(t)
            ghosts[t + shift] = ghosts[t + shift] + jnp.where(upper, v, 0.0)
            ghosts[t + shift + 1] = ghosts[t + shift + 1] + jnp.where(upper, 0.0, v)
            return carry

        rest.append((t0 + 2, lax.shift_right_logical(b + 127, 7), more))
        total = total + (b - a)
    for at, v in puts:
        ghosts[at] = ghosts[at] + v
    for lo, hi, more in rest:
        lax.fori_loop(lo, hi, more, 0)

    slot = lax.broadcasted_iota(jnp.int32, (1, GHOSTS), 1)
    tiles = lax.shift_right_logical(total + 127, 7)
    ahead = GHOSTS // 128

    def ghost_columns(t, carry):
        g = jnp.where((sub == 0) & (lane + t * 128 >= total), FAR, ghosts[t])
        turned = jnp.transpose(g)
        at = t * 128 if isinstance(t, int) else pl.multiple_of(t * 128, 128)
        for c in range(3):
            cols[c, pl.ds(at, 128)] = jnp.broadcast_to(turned[:, c:c + 1], (128, 128))
        return carry

    def ghost_block(i, carry):
        vals = jnp.concatenate([ghosts[ahead * i + j] for j in range(ahead)], axis=1)
        live = (slot + i * GHOSTS < total).astype(F32)
        zh, zl = z_weights(vals[2:3])
        weights = plane_weights(vals[0:1], vals[1:2], True)
        gi = sample(inner[...], zh, zl)
        gn = sample(near[...], zh, zl)
        gf = sample(outer[...], zh, zl)
        react = []
        for c in range(3):
            s = (jnp.sum(gi[c * ROWS:(c + 1) * ROWS] * weights[0:ROWS], axis=0, keepdims=True)
                 + jnp.sum(gn[c * ADJ:(c + 1) * ADJ] * weights[ROWS:ADJ_ROWS], axis=0, keepdims=True)
                 + jnp.sum(gf[c * FAR_ROWS:(c + 1) * FAR_ROWS] * weights[ADJ_ROWS:], axis=0, keepdims=True))
            react.append((vals[3 + c:4 + c] - 2.0 * s) * live)
        spread(weights[0:ADJ_ROWS], react, jnp.concatenate([zh, zl], axis=0))
        return carry

    for t in range(ahead):
        ghost_columns(t, 0)
    ghost_block(0, 0)
    lax.fori_loop(ahead, tiles, ghost_columns, 0)
    lax.fori_loop(1, lax.div(total + GHOSTS - 1, GHOSTS), ghost_block, 0)
    lax.fori_loop(1, lax.shift_right_logical(n_own + BLOCK - 1, 9), own_block, 0)

    own_left = jnp.where(starts[8, 0, 10] > 0.5, 0, n_own)

    def ghost_pairs(i, carry):
        mine = [jnp.broadcast_to(own[i, c:c + 1], (8, OWN)) for c in range(3)]
        got = tuple(jnp.zeros((8, OWN), F32) for _ in range(3))
        for source, n in ((own_cols, own_left), (cols, total)):
            one = pair_step(source, mine, OWN)

            def four(n, got, one=one):
                for k in range(4):
                    got = one(4 * n + k, got)
                return got

            got = lax.fori_loop(0, lax.shift_right_logical(n + 31, 5), four, got)
        live = own[i, 6:7]
        for c in range(3):
            acc[i, c:c + 1] = acc[i, c:c + 1] + 0.24 * live * jnp.sum(got[c], axis=0, keepdims=True)
        return carry

    lax.fori_loop(0, lax.shift_right_logical(n_own + OWN - 1, 8), ghost_pairs, 0)
    for i in range(SW // OWN):
        for c in range(3):
            for j in range(2):
                r = c * LANE_TILES + 2 * i + j
                force_v[r:r + 1] = acc[i, c:c + 1, j * 128:(j + 1) * 128]
    force_copy = pltpu.make_async_copy(force_v, force_out, force_sem)
    force_copy.start()

    def prepare(rho, u0, half, g):
        u = [u0[c] + half * g[c] for c in range(3)]
        uu = u[0] * u[0] + u[1] * u[1] + u[2] * u[2]
        ug = u[0] * g[0] + u[1] * g[1] + u[2] * g[2]
        k0 = 1.25 * rho * (1.0 - 1.5 * uu) - 1.125 * ug
        return k0, 3.75 * rho, 5.625 * rho, u, [1.125 * v for v in g]

    def along(q, v):
        out = None
        for c in range(3):
            s = DIRS[q][c]
            if s:
                out = (v[c] if s > 0 else -v[c]) if out is None else (out + v[c] if s > 0 else out - v[c])
        return out

    def post(q, f, prep):
        k0, r1, r2, u, g = prep
        if q == 0:
            return -0.25 * f + WEIGHTS[0] * k0
        a, p = along(q, u), along(q, g)
        return -0.25 * f + WEIGHTS[q] * (k0 + a * (r1 + r2 * a + 3.0 * p) + p)

    def side_prep(rho, u0, lo, n):
        g = [force[c, lo:lo + n] for c in range(3)]
        return prepare(rho, u0, 0.5 / rho, g)

    k0, r1, r2, u, g = side_prep(mom[0], [mom[1 + c] for c in range(3)], 0, ROWS)
    node[0] = k0
    for c in range(3):
        node[1 + c] = u[c]
        node[4 + c] = g[c]
    xs = [side_prep(halo_x[s, 0], [halo_x[s, 1 + c] for c in range(3)], ROWS + s * CY, CY) for s in range(2)]
    ys = [side_prep(halo_y[s, 0], [halo_y[s, 1 + c] for c in range(3)], ROWS + 2 * CY + s * CX, CX)
          for s in range(2)]
    cs = []
    for i in range(4):
        sx, sy = SIDES[4 + i]
        r = ADJ_ROWS - 16 + (1 if sx < 0 else 2) * 4 + (1 if sy < 0 else 2)
        cs.append(side_prep(halo_c[i, 0:1], [halo_c[i, 1 + c:2 + c] for c in range(3)], r, 1))
    stores = []
    for q in range(19):
        dx, dy, dz = DIRS[q]
        rho_q = mom[0]
        prep = (node[0], 3.75 * rho_q, 5.625 * rho_q, [node[1 + c] for c in range(3)], [node[4 + c] for c in range(3)])

        def turned(v, dz=dz):
            return pltpu.roll(v, dz % NZ, 1) if dz else v

        v = turned(post(q, pops[q], prep))
        if dy:
            v = pltpu.roll(v, dy % ROWS, 0)
        if dx == 0:
            out_v[q] = v
        else:
            s = 0 if dx > 0 else 1
            e = turned(post(q, halo_x[s, 7 + facing(0, dx).index(q)], xs[s]))
            if dy:
                e = pltpu.roll(e, dy % CY, 0)
            if dx > 0:
                out_v[q, CY:ROWS] = v[0:ROWS - CY]
                out_v[q, 0:CY] = e
            else:
                out_v[q, 0:ROWS - CY] = v[CY:ROWS]
                out_v[q, ROWS - CY:ROWS] = e
        if dy:
            s = 0 if dy > 0 else 1
            at = 0 if dy > 0 else CY - 1
            e = turned(post(q, halo_y[s, 7 + facing(1, dy).index(q)], ys[s]))
            if dx:
                e = pltpu.roll(e, dx % CX, 0)
            out_v[q, pl.ds(at, CX, stride=CY)] = e
            if dx:
                i = SIDES.index((-dx, -dy)) - 4
                r = at + (0 if dx > 0 else (CX - 1) * CY)
                out_v[q, r:r + 1] = post(q, halo_c[i, 4:5], cs[i])
        c = pltpu.make_async_copy(out_v.at[q], next_out.at[q], out_sem.at[q])
        c.start()
        stores.append(c)
    force_copy.wait()
    for c in stores:
        c.wait()


def body(n_gx, n_gy, populations, anchor, offsets, heading, velocity, live_count):
    pops = populations.reshape(19, ROWS, NZ)
    tiles = LANE_TILES
    vmem = pl.BlockSpec(memory_space=pltpu.VMEM)
    hbm = pl.BlockSpec(memory_space=pltpu.HBM)
    dma = pltpu.SemaphoreType.DMA
    held = (
        pltpu.VMEM((19, ROWS, NZ), F32),
        pltpu.VMEM((2, 12, CY, 128), F32),
        pltpu.VMEM((2, 12, CX, 128), F32),
        pltpu.VMEM((4, 16, 128), F32),
        pltpu.VMEM((8, LANE_TILES, 8, 128), F32),
        pltpu.VMEM((9, 1, 128), F32),
        pltpu.VMEM((SW // OWN, 8, OWN), F32),
        pltpu.VMEM((SW // OWN, 8, OWN), F32),
        pltpu.VMEM((4, ROWS, NZ), F32),
        pltpu.VMEM((3 * ROWS, 2 * NZ), BF16),
        pltpu.VMEM((BLOCKS, 2 * NZ, BLOCK), BF16),
        pltpu.VMEM((BLOCKS, ADJ_ROWS, BLOCK), F32),
        pltpu.VMEM((3, SW, 128), F32),
    )
    pops, halo_x, halo_y, halo_c, lists, starts, own, base, mom, inner, zhl, plane, own_cols = pl.pallas_call(
        functools.partial(exchange_kernel, n_gx, n_gy),
        out_shape=held,
        in_specs=[hbm] * 6,
        out_specs=[vmem] * 13,
        scratch_shapes=[
            pltpu.VMEM((tiles, 128), jnp.int32),
            pltpu.VMEM((3 * tiles, 128), F32),
            pltpu.VMEM((2 * tiles, 128), F32),
            pltpu.VMEM((3 * tiles, 128), F32),
            pltpu.SMEM((1,), jnp.int32),
            pltpu.VMEM((8 * tiles, 128), F32),
            pltpu.VMEM((2, 7, CY, 128), F32),
            pltpu.VMEM((2, 12, CX, 128), F32),
            pltpu.VMEM((4, 16, 128), F32),
            pltpu.VMEM((LANE_TILES, 8, 128), F32),
            pltpu.VMEM((1, 128), F32),
            dma((9,)), dma((24,)), dma((24,)), dma((10,)), dma((10,)),
            pltpu.SemaphoreType.REGULAR, pltpu.SemaphoreType.REGULAR,
        ],
        compiler_params=pltpu.CompilerParams(collective_id=0, has_side_effects=True, vmem_limit_bytes=20 << 20),
        name="exchange",
    )(*[pltpu.with_memory_space_constraint(v, pltpu.HBM) for v in (
        pops, anchor.reshape(tiles, 128), offsets.reshape(3 * tiles, 128),
        jnp.swapaxes(heading.reshape(2, tiles, 128), 0, 1).reshape(2 * tiles, 128),
        velocity.reshape(3 * tiles, 128))], live_count.reshape(1))
    moved, force = pl.pallas_call(
        fluid_kernel,
        out_shape=(jax.ShapeDtypeStruct((19, ROWS, NZ), F32), jax.ShapeDtypeStruct((3 * tiles, 128), F32)),
        in_specs=[vmem] * 13,
        out_specs=[hbm, hbm],
        scratch_shapes=[
            pltpu.VMEM((SW // OWN, 8, OWN), F32),
            pltpu.VMEM((19, ROWS, NZ), F32),
            pltpu.VMEM((3 * tiles, 128), F32),
            pltpu.SMEM((9, 1, 128), F32),
            pltpu.VMEM((7, ROWS, NZ), F32),
            pltpu.VMEM((3 * ADJ, 2 * NZ), BF16),
            pltpu.VMEM((3 * FAR_ROWS, 2 * NZ), BF16),
            pltpu.VMEM((3, ADJ_ROWS, NZ), F32),
            pltpu.VMEM((GHOST_TILES, 8, 128), F32),
            pltpu.VMEM((3, GHOST_TILES * 128, 128), F32),
            dma((19,)), dma, dma,
        ],
        compiler_params=pltpu.CompilerParams(vmem_limit_bytes=32 << 20),
        name="fluid",
    )(pops, own, base, halo_x, halo_y, halo_c, lists, starts, mom, inner, zhl, plane, own_cols)
    return (moved.reshape(populations.shape), force.reshape(1, 1, 3, SW))


def solution(mesh):
    return jax.shard_map(
        functools.partial(body, mesh.shape["gx"], mesh.shape["gy"]),
        mesh=mesh,
        in_specs=(
            P(None, "gx", "gy", None),
            P("gx", "gy", None),
            P("gx", "gy", None, None),
            P("gx", "gy", None, None),
            P("gx", "gy", None, None),
            P("gx", "gy"),
        ),
        out_specs=(P(None, "gx", "gy", None), P("gx", "gy", None, None)),
        check_vma=False,
    )
```

```python
import functools

import jax
import jax.numpy as jnp
import numpy as np
from jax import lax
from jax.experimental import pallas as pl
from jax.experimental.pallas import tpu as pltpu
from jax.sharding import PartitionSpec as P

DIRS = (
    (0, 0, 0), (1, 0, 0), (-1, 0, 0), (0, 1, 0), (0, -1, 0), (0, 0, 1), (0, 0, -1),
    (1, 1, 0), (-1, -1, 0), (1, -1, 0), (-1, 1, 0), (1, 0, 1), (-1, 0, -1),
    (1, 0, -1), (-1, 0, 1), (0, 1, 1), (0, -1, -1), (0, 1, -1), (0, -1, 1),
)
WEIGHTS = (1.0 / 3.0,) + (1.0 / 18.0,) * 6 + (1.0 / 36.0,) * 12
CUTOFF = 2.0 ** (1.0 / 3.0)
REACH = 1.125
FAR = 1.0e9
F32 = jnp.float32
BF16 = jnp.bfloat16
MESH = pl.DeviceIdType.MESH

CX, CY, NZ, SW = 8, 16, 128, 1024
ROWS = CX * CY
LANE_TILES = SW // 128

SIDES = ((-1, 0), (1, 0), (0, -1), (0, 1), (-1, -1), (-1, 1), (1, -1), (1, 1))
RANGES = ((0, 4, 7), (1, 0, 3), (2, 2, 5), (3, 6, 8), (3, 0, 1), (4, 4, 5), (5, 6, 7), (6, 2, 3), (7, 0, 1))


def facing(axis, sign):
    return [q for q in range(19) if DIRS[q][axis] == sign]


def corner_q(sx, sy):
    return DIRS.index((-sx, -sy, 0))


def split2(v):
    hi = v.astype(BF16)
    return hi, (v - hi.astype(F32)).astype(BF16)


def split3(v):
    hi = v.astype(BF16)
    rest = v - hi.astype(F32)
    mid = rest.astype(BF16)
    return hi, mid, (rest - mid.astype(F32)).astype(BF16)


def dot(a, b):
    return lax.dot_general(a, b, (((1,), (0,)), ((), ())), preferred_element_type=F32)


def dot_t(a, b):
    return lax.dot_general(a, b, (((1,), (1,)), ((), ())), preferred_element_type=F32)


def tent(d):
    return jnp.maximum(1.0 - jnp.abs(d), 0.0)


def moments(load):
    rho = None
    mom = [None, None, None]
    for q in range(19):
        f = load(q)
        rho = f if rho is None else rho + f
        for c in range(3):
            s = DIRS[q][c]
            if s:
                if mom[c] is None:
                    mom[c] = f if s > 0 else -f
                else:
                    mom[c] = mom[c] + f if s > 0 else mom[c] - f
    return rho, mom


def pair_terms(ox, oy, oz, px, py, pz):
    dx = ox - px
    dy = oy - py
    dz = oz - pz
    dz = dz - NZ * jnp.round(dz * (1.0 / NZ))
    raw = dx * dx + dy * dy + dz * dz
    inv = 1.0 / jnp.maximum(raw, 0.8)
    sixth = inv * inv * inv
    mag = (sixth + sixth - 1.0) * (sixth * inv)
    mag = jnp.where(raw < CUTOFF, mag, 0.0)
    return mag * dx, mag * dy, mag * dz


def classes(x, y, live):
    xl, xh = x < REACH, x > CX - 1 - REACH
    yl, yh = y < REACH, y > CY - 1 - REACH
    yc = jnp.where(yl, 0.0, jnp.where(yh, 2.0, 1.0))
    kind = jnp.where(xl, yc, jnp.where(xh, 6.0 - yc, jnp.where(yl, 7.0, jnp.where(yh, 3.0, 8.0))))
    return jnp.where(live > 0.0, kind, 9.0)


def sort_ranks(kind):
    masks = [(kind == k).astype(F32) for k in range(10)]
    ri = lax.broadcasted_iota(jnp.int32, (128, 256), 0)
    ci = lax.broadcasted_iota(jnp.int32, (128, 256), 1)
    upper = ((ri < ci) | (ci >= 128)).astype(F32).astype(BF16)
    pre = dot(jnp.concatenate(masks, axis=0).astype(BF16), upper)
    within, tile_sum = pre[:, :128], pre[:, 128:]
    place = lax.broadcasted_iota(jnp.int32, (80, 128), 0) & 7
    upto = tile_sum
    for by in (1, 2, 4):
        upto = upto + jnp.where(place >= by, pltpu.roll(upto, by, 0), 0.0)
    lane = lax.broadcasted_iota(jnp.int32, (1, 128), 1)
    rank = jnp.zeros((8, 128), F32)
    row = jnp.zeros((1, 128), F32)
    first = jnp.zeros((1, 128), F32)
    for k in range(10):
        cut = slice(8 * k, 8 * k + 8)
        row = jnp.where(lane == k, first, row)
        rank = rank + masks[k] * (within[cut] + (upto[cut] - tile_sum[cut]) + first)
        first = first + upto[8 * k + 7:8 * k + 8]
    return rank, row


def plane_weights(px, py, far):
    x8 = lax.broadcasted_iota(jnp.int32, (CX, 1), 0).astype(F32)
    y16 = lax.broadcasted_iota(jnp.int32, (CY, 1), 0).astype(F32)
    ki = lax.broadcasted_iota(jnp.int32, (16, 1), 0)
    ii, jj = lax.shift_right_logical(ki, 2), ki & 3
    xd = jnp.where(ii < 2, ii - 2, ii + CX - 2).astype(F32)
    yd = jnp.where(jj < 2, jj - 2, jj + CY - 2).astype(F32)
    tx, ty = tent(x8 - px), tent(y16 - py)
    parts = [tx[i:i + 1] * ty for i in range(CX)]
    parts += [tent(-1.0 - px) * ty, tent(CX - px) * ty, tent(-1.0 - py) * tx, tent(CY - py) * tx]
    parts += [tent(xd - px) * tent(yd - py)]
    if far:
        parts += [tent(-2.0 - px) * ty, tent(CX + 1.0 - px) * ty, tent(-2.0 - py) * tx, tent(CY + 1.0 - py) * tx]
    return jnp.concatenate(parts, axis=0)


def z_weights(pz):
    zi = lax.broadcasted_iota(jnp.int32, (NZ, 1), 0).astype(F32)
    return split2(tent(zi - pz))


def widen(v):
    hi, lo = split2(v)
    return jnp.concatenate([hi, lo], axis=1)


def sample(u, zh, zl):
    return dot(u, jnp.concatenate([zh, zh], axis=0)) + dot(u[:, :128], zl)


def columns(cols, at, place):
    turned = jnp.transpose(place)
    for c in range(3):
        cols[c, at:at + 128] = jnp.broadcast_to(turned[:, c:c + 1], (128, 128))


def pair_step(cols, mine, width):
    def step(n, acc):
        at = pl.multiple_of(n * 8, 8)
        p = [jnp.concatenate([cols[c, pl.ds(at, 8)]] * (width // 128), axis=1) for c in range(3)]
        return tuple(a + b for a, b in zip(acc, pair_terms(*mine, *p)))

    return step


def exchange_kernel(n_gx, n_gy, pops_hbm, anchor_hbm, offsets_hbm, heading_hbm, velocity_hbm, count_hbm,
                    pops, halo_x, halo_y, halo_c, lists, starts_out, own_out, base_out, mom, inner, zhl, plane, cols,
                    anchor, offsets, heading, velocity, count, table,
                    msg_x, msg_y, msg_c, msg_l, msg_s, load_sem, send_sem, recv_sem, face_send, face_recv, lower, beside):
    gx = lax.axis_index("gx")
    gy = lax.axis_index("gy")

    def device(side):
        return (lax.rem(gx + side[0] + n_gx, n_gx), lax.rem(gy + side[1] + n_gy, n_gy))

    loads = [pltpu.make_async_copy(a, b, load_sem.at[k]) for k, (a, b) in enumerate((
        (anchor_hbm, anchor), (offsets_hbm, offsets), (heading_hbm, heading), (velocity_hbm, velocity),
        (count_hbm, count)))]
    loads += [pltpu.make_async_copy(pops_hbm.at[pl.ds(q, n)], pops.at[pl.ds(q, n)], load_sem.at[5 + k])
              for k, (q, n) in enumerate(((0, 5), (5, 5), (10, 5), (15, 4)))]
    for c in loads:
        c.start()
    even = lax.rem(gy, 2) == 0
    odd = jnp.logical_not(even)
    barrier = pltpu.get_barrier_semaphore()

    def tell(semaphore, sides):
        for side in sides:
            pl.semaphore_signal(semaphore, inc=1, device_id=device(side), device_id_type=MESH)

    corners_up, along_y, down = ((1, -1), (1, 1)), ((0, -1), (0, 1)), ((-1, -1), (-1, 1), (-1, 0))
    tell(barrier, down)

    @pl.when(even)
    def _():
        tell(barrier, along_y)
        pl.semaphore_wait(barrier, 3)

    @pl.when(odd)
    def _():
        pl.semaphore_wait(barrier, 5)
        tell(beside, along_y)

    tell(lower, ((1, 0),) + corners_up)

    face = []
    for d in range(2):
        for k, q in enumerate(facing(0, 2 * d - 1)):
            face.append(pltpu.make_async_remote_copy(
                src_ref=pops_hbm.at[q, pl.ds(d * (ROWS - CY), CY)], dst_ref=halo_x.at[1 - d, 7 + k],
                send_sem=face_send.at[5 * d + k], recv_sem=face_recv.at[5 * (1 - d) + k],
                device_id=device(SIDES[d]), device_id_type=MESH))
    for c in face[5:]:
        c.start()

    group = max(n_gx // 4, 1)
    head = (lax.rem(gx, group) == 0) & (gx != 0)
    idle = (gx == 0) | ((lax.rem(gx, group) == group - 1) & (gx != n_gx - 1))

    @pl.when(head)
    def _():
        pl.semaphore_wait(lower, 3)
        for c in face[:5]:
            c.start()

    for c in loads[:5]:
        c.wait()

    root = anchor[...]
    bxf = lax.shift_right_logical(root, 7).astype(F32)
    cxf = jnp.floor(bxf * (1.0 / (CY + 2)) + 0.01)
    x = cxf - 1.0 + offsets[0:8]
    y = bxf - cxf * (CY + 2) - 1.0 + offsets[8:16]
    z = (root & (NZ - 1)).astype(F32) + offsets[16:24]
    lane = lax.broadcasted_iota(jnp.int32, (8, 128), 1)
    sub = lax.broadcasted_iota(jnp.int32, (8, 128), 0)
    live = (sub * 128 + lane < count[0]).astype(F32)
    first, second = heading[pl.ds(0, 8, stride=2)], heading[pl.ds(1, 8, stride=2)]
    c1 = jnp.cos(second)
    w = [2.0 * velocity[0:8] - 0.5 * (jnp.cos(first) * c1),
         2.0 * velocity[8:16] - 0.5 * (jnp.sin(first) * c1),
         2.0 * velocity[16:24] - 0.5 * jnp.sin(second)]
    for k, v in enumerate((x, y, z, *w, live, jnp.zeros((8, 128), F32))):
        table[pl.ds(k, 8, stride=8)] = v
    rank, row = sort_ranks(classes(x, y, live))
    msg_s[...] = row
    starts_out[8] = jnp.where(lane[0:1] == 10, idle.astype(F32), row)
    to_tile = jnp.floor(rank * (1.0 / 128.0))
    to_lane = rank - 128.0 * to_tile
    split = [v.astype(F32) for v in split3(table[...])]
    dst = lax.broadcasted_iota(jnp.int32, (128, 128), 0).astype(F32)
    ordered = jnp.zeros((24 * LANE_TILES, 128), F32)
    for t in range(0, LANE_TILES, 2):
        hot, rows = [], []
        for j in (t, t + 1):
            hot.append((dst == to_lane[j:j + 1]).astype(F32).astype(BF16))
            part = jnp.concatenate([v[8 * j:8 * j + 8] for v in split], axis=0)
            rows.append(jnp.concatenate(
                [jnp.where(to_tile[j:j + 1] == float(k), part, 0.0) for k in range(LANE_TILES)],
                axis=0).astype(BF16))
        ordered = ordered + dot_t(jnp.concatenate(rows, axis=1), jnp.concatenate(hot, axis=1))
    for t in range(LANE_TILES):
        at = 24 * t
        msg_l[t] = ordered[at:at + 8] + ordered[at + 8:at + 16] + ordered[at + 16:at + 24]

    def send(k, a, b, side, o):
        d = SIDES.index(side)
        return pltpu.make_async_remote_copy(
            src_ref=a, dst_ref=b, send_sem=send_sem.at[3 * d + k], recv_sem=recv_sem.at[3 * o + k],
            device_id=device(side), device_id_type=MESH)

    copies = {}
    for d, side in enumerate(SIDES):
        o = SIDES.index((-side[0], -side[1]))
        if side[1] == 0:
            first = send(0, msg_x.at[d], halo_x.at[o, pl.ds(0, 7)], side, o)
        elif side[0] == 0:
            first = send(0, msg_y.at[d - 2], halo_y.at[o - 2], side, o)
        else:
            first = send(0, msg_c.at[d - 4], halo_c.at[o - 4], side, o)
        copies[side] = (first, send(1, msg_s, starts_out.at[o], side, o),
                        send(2, msg_l.at[:, pl.ds(0, 6)], lists.at[o, :, pl.ds(0, 6)], side, o))

    def start(sides, kinds=(0, 1, 2)):
        for k in kinds:
            for side in sides:
                copies[side][k].start()

    last = gx == n_gx - 1
    late = gx >= n_gx - max(n_gx // 4, 1)

    @pl.when(last)
    def _():
        start(corners_up, (1, 2))

    @pl.when(head)
    def _():
        start(down, (1, 2))

    start(((1, 0),), (1, 2))

    for c in loads[5:]:
        c.wait()
    rho, m = moments(lambda q: pops[q])
    inv = 1.0 / rho
    mom[0] = rho
    for c in range(3):
        mom[1 + c] = m[c] * inv
    for s, (adj, far) in enumerate(((0, 1), (CX - 1, CX - 2))):
        for c in range(4):
            msg_x[s, c] = mom[c, adj * CY:(adj + 1) * CY]
        for c in range(3):
            msg_x[s, 4 + c] = mom[1 + c, far * CY:(far + 1) * CY]

    for i in range(4):
        sx, sy = SIDES[4 + i]
        ax, fx = (0, 1) if sx < 0 else (CX - 1, CX - 2)
        ay, fy = (0, 1) if sy < 0 else (CY - 1, CY - 2)
        msg_c[i] = jnp.zeros((16, 128), F32)
        for c in range(4):
            msg_c[i, c:c + 1] = mom[c, ax * CY + ay:ax * CY + ay + 1]
        for j, (nx, ny) in enumerate(((ax, fy), (fx, ay), (fx, fy))):
            for c in range(3):
                msg_c[i, 5 + 3 * j + c:6 + 3 * j + c] = mom[1 + c, nx * CY + ny:nx * CY + ny + 1]
        q = DIRS.index((sx, sy, 0))
        msg_c[i, 4:5] = pops[q, ax * CY + ay:ax * CY + ay + 1]


    @pl.when(last)
    def _():
        start(corners_up, (0,))

    @pl.when(head)
    def _():
        start(down, (0,))

    start(((1, 0),), (0,))
    for s, (adj, far) in enumerate(((0, 1), (CY - 1, CY - 2))):
        for c in range(4):
            msg_y[s, c] = mom[c, pl.ds(adj, CX, stride=CY)]
        for c in range(3):
            msg_y[s, 4 + c] = mom[1 + c, pl.ds(far, CX, stride=CY)]
        for k, q in enumerate(facing(1, 2 * s - 1)):
            msg_y[s, 7 + k] = pops[q, pl.ds(adj, CX, stride=CY)]
    def own_pairs():
        for i in range(0, SW // OWN, 2):
            width = 2 * OWN
            mine = [jnp.broadcast_to(jnp.concatenate([own_out[i, c:c + 1], own_out[i + 1, c:c + 1]], axis=1), (8, width))
                    for c in range(3)]
            init = tuple(jnp.zeros((8, width), F32) for _ in range(3))
            got = lax.fori_loop(0, SW // 8, pair_step(cols, mine, width), init)
            for c in range(3):
                pairs = 0.24 * jnp.sum(got[c], axis=0, keepdims=True)
                for j in range(2):
                    base_out[i + j, c:c + 1] = (base_out[i + j, c:c + 1]
                                                + pairs[:, j * OWN:(j + 1) * OWN] * own_out[i + j, 6:7])

    def send_down():
        pl.semaphore_wait(lower, 3)
        for c in face[:5]:
            c.start()
        start(down)

    def send_along():
        @pl.when(even)
        def _():
            pl.semaphore_wait(beside, 2)

        start(along_y)

    @pl.when(jnp.logical_not(late))
    def _():
        send_along()
        start(corners_up)

    @pl.when(jnp.logical_not(late | head) & (gx != 0))
    def _():
        send_down()

    for c in range(3):
        inner[c * ROWS:(c + 1) * ROWS] = widen(mom[1 + c])
    for i in range(BLOCKS):
        n = BLOCK // 128
        vals = jnp.concatenate([table[8 * (n * i + j):8 * (n * i + j) + 8] for j in range(n)], axis=1)
        zh, zl = z_weights(vals[2:3])
        zhl[i, 0:NZ] = zh
        zhl[i, NZ:2 * NZ] = zl
        plane[i] = plane_weights(vals[0:1], vals[1:2], False)
        got = sample(inner[...], zh, zl)
        rows = [vals[0:3]]
        for c in range(3):
            s = jnp.sum(got[c * ROWS:(c + 1) * ROWS] * plane[i, 0:ROWS], axis=0, keepdims=True)
            rows.append((vals[3 + c:4 + c] - 2.0 * s) * vals[6:7])
        rows = jnp.concatenate(rows + [vals[6:8]], axis=0)
        for j in range(BLOCK // OWN):
            own_out[i * (BLOCK // OWN) + j] = rows[:, j * OWN:(j + 1) * OWN]

    @pl.when(late)
    def _():
        send_along()

    @pl.when(late & jnp.logical_not(last))
    def _():
        start(corners_up)

    @pl.when(late & jnp.logical_not(head))
    def _():
        send_down()

    for t in range(LANE_TILES):
        v = table[8 * t:8 * t + 8]
        columns(cols, t * 128, jnp.where((sub == 0) & (v[6:7] == 0.0), FAR, v))
    for i in range(SW // OWN):
        base_out[i] = jnp.concatenate([-own_out[i, 3:6], jnp.zeros((5, OWN), F32)], axis=0)

    @pl.when(idle)
    def _():
        own_pairs()

    @pl.when(gx == 0)
    def _():
        send_down()

    for c in face:
        c.wait()
    for side in SIDES:
        for c in copies[side]:
            c.wait()


ADJ = 64
FAR_ROWS = 48
ADJ_ROWS = ROWS + ADJ
BLOCK = 512
BLOCKS = SW // BLOCK
OWN = 256
GHOSTS = 384
GHOST_TILES = 8 * LANE_TILES + 4


def fluid_kernel(pops, own, base, halo_x, halo_y, halo_c, lists, starts_in, mom, inner, zhl, plane, own_cols,
                 next_out, force_out,
                 acc, out_v, force_v, starts, node, near, outer, force, ghosts, cols, out_sem, start_sem, force_sem):
    start_copy = pltpu.make_async_copy(starts_in, starts, start_sem)
    start_copy.start()
    acc[...] = base[...]
    ghosts[...] = jnp.zeros(ghosts.shape, F32)
    force[...] = jnp.zeros(force.shape, F32)
    for c in range(3):
        corner = []
        for i in range(4):
            for j in range(4):
                sx, sy = (0 if i < 2 else 1), (0 if j < 2 else 1)
                fx, fy = i in (0, 3), j in (0, 3)
                k = 2 * sx + sy
                r = (11 if fy else 8) if fx else (5 if fy else 1)
                corner.append(halo_c[k, r + c:r + c + 1])
        near[c * ADJ:(c + 1) * ADJ] = widen(jnp.concatenate(
            [halo_x[0, 1 + c], halo_x[1, 1 + c], halo_y[0, 1 + c], halo_y[1, 1 + c]] + corner, axis=0))
        outer[c * FAR_ROWS:(c + 1) * FAR_ROWS] = widen(jnp.concatenate(
            [halo_x[0, 4 + c], halo_x[1, 4 + c], halo_y[0, 4 + c], halo_y[1, 4 + c]], axis=0))

    def spread(weights, react, zz):
        zh = zz[0:NZ]
        for c in range(3):
            wh, wl = split2(weights * react[c])
            both = dot_t(wh, zz)
            force[c] = force[c] + (both[:, :128] + both[:, 128:] + dot_t(wl, zh))

    per = BLOCK // OWN

    def own_block(i, carry):
        zz = zhl[i]
        got = sample(near[...], zz[0:NZ], zz[NZ:2 * NZ])
        vals = jnp.concatenate([own[per * i + j] for j in range(per)], axis=1)
        react = []
        for c in range(3):
            s = jnp.sum(got[c * ADJ:(c + 1) * ADJ] * plane[i, ROWS:ADJ_ROWS], axis=0, keepdims=True)
            s = 2.0 * s * vals[6:7]
            react.append(vals[3 + c:4 + c] - s)
            for j in range(per):
                acc[per * i + j, c:c + 1] = acc[per * i + j, c:c + 1] + s[:, j * OWN:(j + 1) * OWN]
        spread(plane[i], react, zz)
        return carry

    own_block(0, 0)
    start_copy.wait()
    n_own = starts[8, 0, 9].astype(jnp.int32)

    lane = lax.broadcasted_iota(jnp.int32, (8, 128), 1)
    sub = lax.broadcasted_iota(jnp.int32, (8, 128), 0)
    total = jnp.int32(0)
    puts, rest = [], []
    for d, lo, hi in RANGES:
        a = starts[d, 0, lo].astype(jnp.int32)
        b = starts[d, 0, hi].astype(jnp.int32)
        sx, sy = SIDES[d]
        moved = jnp.where(sub == 0, float(sx * CX), jnp.where(sub == 1, float(sy * CY), 0.0))
        by = (total - a) & 127
        upper = lane >= by

        def taken(t, d=d, a=a, b=b, by=by, moved=moved):
            at = t * 128 + lane
            v = jnp.where((at >= a) & (at < b), lists[d, jnp.minimum(t, LANE_TILES - 1)] + moved, 0.0)
            return pltpu.roll(v, by, 1)

        t0 = lax.shift_right_logical(a, 7)
        tile = lax.shift_right_logical(total - a + t0 * 128 + 1024, 7) - 8
        v0, v1 = taken(t0), taken(t0 + 1)
        puts.append((jnp.maximum(tile, 0), jnp.where(upper, v0, 0.0)))
        puts.append((tile + 1, jnp.where(upper, v1, v0)))
        puts.append((tile + 2, jnp.where(upper, 0.0, v1)))

        def more(t, carry, taken=taken, upper=upper, shift=tile - t0):
            v = taken(t)
            ghosts[t + shift] = ghosts[t + shift] + jnp.where(upper, v, 0.0)
            ghosts[t + shift + 1] = ghosts[t + shift + 1] + jnp.where(upper, 0.0, v)
            return carry

        rest.append((t0 + 2, lax.shift_right_logical(b + 127, 7), more))
        total = total + (b - a)
    for at, v in puts:
        ghosts[at] = ghosts[at] + v
    for lo, hi, more in rest:
        lax.fori_loop(lo, hi, more, 0)

    slot = lax.broadcasted_iota(jnp.int32, (1, GHOSTS), 1)
    tiles = lax.shift_right_logical(total + 127, 7)
    ahead = GHOSTS // 128

    def ghost_columns(t, carry):
        g = jnp.where((sub == 0) & (lane + t * 128 >= total), FAR, ghosts[t])
        turned = jnp.transpose(g)
        at = t * 128 if isinstance(t, int) else pl.multiple_of(t * 128, 128)
        for c in range(3):
            cols[c, pl.ds(at, 128)] = jnp.broadcast_to(turned[:, c:c + 1], (128, 128))
        return carry

    def ghost_block(i, carry):
        vals = jnp.concatenate([ghosts[ahead * i + j] for j in range(ahead)], axis=1)
        live = (slot + i * GHOSTS < total).astype(F32)
        zh, zl = z_weights(vals[2:3])
        weights = plane_weights(vals[0:1], vals[1:2], True)
        gi = sample(inner[...], zh, zl)
        gn = sample(near[...], zh, zl)
        gf = sample(outer[...], zh, zl)
        react = []
        for c in range(3):
            s = (jnp.sum(gi[c * ROWS:(c + 1) * ROWS] * weights[0:ROWS], axis=0, keepdims=True)
                 + jnp.sum(gn[c * ADJ:(c + 1) * ADJ] * weights[ROWS:ADJ_ROWS], axis=0, keepdims=True)
                 + jnp.sum(gf[c * FAR_ROWS:(c + 1) * FAR_ROWS] * weights[ADJ_ROWS:], axis=0, keepdims=True))
            react.append((vals[3 + c:4 + c] - 2.0 * s) * live)
        spread(weights[0:ADJ_ROWS], react, jnp.concatenate([zh, zl], axis=0))
        return carry

    for t in range(ahead):
        ghost_columns(t, 0)
    ghost_block(0, 0)
    lax.fori_loop(ahead, tiles, ghost_columns, 0)
    lax.fori_loop(1, lax.div(total + GHOSTS - 1, GHOSTS), ghost_block, 0)
    lax.fori_loop(1, lax.shift_right_logical(n_own + BLOCK - 1, 9), own_block, 0)

    own_left = jnp.where(starts[8, 0, 10] > 0.5, 0, n_own)

    def ghost_pairs(i, carry):
        mine = [jnp.broadcast_to(own[i, c:c + 1], (8, OWN)) for c in range(3)]
        got = tuple(jnp.zeros((8, OWN), F32) for _ in range(3))
        for source, n in ((own_cols, own_left), (cols, total)):
            one = pair_step(source, mine, OWN)

            def four(n, got, one=one):
                for k in range(4):
                    got = one(4 * n + k, got)
                return got

            got = lax.fori_loop(0, lax.shift_right_logical(n + 31, 5), four, got)
        live = own[i, 6:7]
        for c in range(3):
            acc[i, c:c + 1] = acc[i, c:c + 1] + 0.24 * live * jnp.sum(got[c], axis=0, keepdims=True)
        return carry

    lax.fori_loop(0, lax.shift_right_logical(n_own + OWN - 1, 8), ghost_pairs, 0)
    for i in range(SW // OWN):
        for c in range(3):
            for j in range(2):
                r = c * LANE_TILES + 2 * i + j
                force_v[r:r + 1] = acc[i, c:c + 1, j * 128:(j + 1) * 128]
    force_copy = pltpu.make_async_copy(force_v, force_out, force_sem)
    force_copy.start()

    def prepare(rho, u0, half, g):
        u = [u0[c] + half * g[c] for c in range(3)]
        uu = u[0] * u[0] + u[1] * u[1] + u[2] * u[2]
        ug = u[0] * g[0] + u[1] * g[1] + u[2] * g[2]
        k0 = 1.25 * rho * (1.0 - 1.5 * uu) - 1.125 * ug
        return k0, 3.75 * rho, 5.625 * rho, u, [1.125 * v for v in g]

    def along(q, v):
        out = None
        for c in range(3):
            s = DIRS[q][c]
            if s:
                out = (v[c] if s > 0 else -v[c]) if out is None else (out + v[c] if s > 0 else out - v[c])
        return out

    def post(q, f, prep):
        k0, r1, r2, u, g = prep
        if q == 0:
            return -0.25 * f + WEIGHTS[0] * k0
        a, p = along(q, u), along(q, g)
        return -0.25 * f + WEIGHTS[q] * (k0 + a * (r1 + r2 * a + 3.0 * p) + p)

    def side_prep(rho, u0, lo, n):
        g = [force[c, lo:lo + n] for c in range(3)]
        return prepare(rho, u0, 0.5 / rho, g)

    k0, r1, r2, u, g = side_prep(mom[0], [mom[1 + c] for c in range(3)], 0, ROWS)
    node[0] = k0
    for c in range(3):
        node[1 + c] = u[c]
        node[4 + c] = g[c]
    xs = [side_prep(halo_x[s, 0], [halo_x[s, 1 + c] for c in range(3)], ROWS + s * CY, CY) for s in range(2)]
    ys = [side_prep(halo_y[s, 0], [halo_y[s, 1 + c] for c in range(3)], ROWS + 2 * CY + s * CX, CX)
          for s in range(2)]
    cs = []
    for i in range(4):
        sx, sy = SIDES[4 + i]
        r = ADJ_ROWS - 16 + (1 if sx < 0 else 2) * 4 + (1 if sy < 0 else 2)
        cs.append(side_prep(halo_c[i, 0:1], [halo_c[i, 1 + c:2 + c] for c in range(3)], r, 1))
    stores = []
    for q in range(19):
        dx, dy, dz = DIRS[q]
        rho_q = mom[0]
        prep = (node[0], 3.75 * rho_q, 5.625 * rho_q, [node[1 + c] for c in range(3)], [node[4 + c] for c in range(3)])

        def turned(v, dz=dz):
            return pltpu.roll(v, dz % NZ, 1) if dz else v

        v = turned(post(q, pops[q], prep))
        if dy:
            v = pltpu.roll(v, dy % ROWS, 0)
        if dx == 0:
            out_v[q] = v
        else:
            s = 0 if dx > 0 else 1
            e = turned(post(q, halo_x[s, 7 + facing(0, dx).index(q)], xs[s]))
            if dy:
                e = pltpu.roll(e, dy % CY, 0)
            if dx > 0:
                out_v[q, CY:ROWS] = v[0:ROWS - CY]
                out_v[q, 0:CY] = e
            else:
                out_v[q, 0:ROWS - CY] = v[CY:ROWS]
                out_v[q, ROWS - CY:ROWS] = e
        if dy:
            s = 0 if dy > 0 else 1
            at = 0 if dy > 0 else CY - 1
            e = turned(post(q, halo_y[s, 7 + facing(1, dy).index(q)], ys[s]))
            if dx:
                e = pltpu.roll(e, dx % CX, 0)
            out_v[q, pl.ds(at, CX, stride=CY)] = e
            if dx:
                i = SIDES.index((-dx, -dy)) - 4
                r = at + (0 if dx > 0 else (CX - 1) * CY)
                out_v[q, r:r + 1] = post(q, halo_c[i, 4:5], cs[i])
        c = pltpu.make_async_copy(out_v.at[q], next_out.at[q], out_sem.at[q])
        c.start()
        stores.append(c)
    force_copy.wait()
    for c in stores:
        c.wait()


def body(n_gx, n_gy, populations, anchor, offsets, heading, velocity, live_count):
    pops = populations.reshape(19, ROWS, NZ)
    tiles = LANE_TILES
    vmem = pl.BlockSpec(memory_space=pltpu.VMEM)
    hbm = pl.BlockSpec(memory_space=pltpu.HBM)
    dma = pltpu.SemaphoreType.DMA
    held = (
        pltpu.VMEM((19, ROWS, NZ), F32),
        pltpu.VMEM((2, 12, CY, 128), F32),
        pltpu.VMEM((2, 12, CX, 128), F32),
        pltpu.VMEM((4, 16, 128), F32),
        pltpu.VMEM((8, LANE_TILES, 8, 128), F32),
        pltpu.VMEM((9, 1, 128), F32),
        pltpu.VMEM((SW // OWN, 8, OWN), F32),
        pltpu.VMEM((SW // OWN, 8, OWN), F32),
        pltpu.VMEM((4, ROWS, NZ), F32),
        pltpu.VMEM((3 * ROWS, 2 * NZ), BF16),
        pltpu.VMEM((BLOCKS, 2 * NZ, BLOCK), BF16),
        pltpu.VMEM((BLOCKS, ADJ_ROWS, BLOCK), F32),
        pltpu.VMEM((3, SW, 128), F32),
    )
    pops, halo_x, halo_y, halo_c, lists, starts, own, base, mom, inner, zhl, plane, own_cols = pl.pallas_call(
        functools.partial(exchange_kernel, n_gx, n_gy),
        out_shape=held,
        in_specs=[hbm] * 6,
        out_specs=[vmem] * 13,
        scratch_shapes=[
            pltpu.VMEM((tiles, 128), jnp.int32),
            pltpu.VMEM((3 * tiles, 128), F32),
            pltpu.VMEM((2 * tiles, 128), F32),
            pltpu.VMEM((3 * tiles, 128), F32),
            pltpu.SMEM((1,), jnp.int32),
            pltpu.VMEM((8 * tiles, 128), F32),
            pltpu.VMEM((2, 7, CY, 128), F32),
            pltpu.VMEM((2, 12, CX, 128), F32),
            pltpu.VMEM((4, 16, 128), F32),
            pltpu.VMEM((LANE_TILES, 8, 128), F32),
            pltpu.VMEM((1, 128), F32),
            dma((9,)), dma((24,)), dma((24,)), dma((10,)), dma((10,)),
            pltpu.SemaphoreType.REGULAR, pltpu.SemaphoreType.REGULAR,
        ],
        compiler_params=pltpu.CompilerParams(collective_id=0, has_side_effects=True, vmem_limit_bytes=20 << 20),
        name="exchange",
    )(*[pltpu.with_memory_space_constraint(v, pltpu.HBM) for v in (
        pops, anchor.reshape(tiles, 128), offsets.reshape(3 * tiles, 128),
        jnp.swapaxes(heading.reshape(2, tiles, 128), 0, 1).reshape(2 * tiles, 128),
        velocity.reshape(3 * tiles, 128))], live_count.reshape(1))
    moved, force = pl.pallas_call(
        fluid_kernel,
        out_shape=(jax.ShapeDtypeStruct((19, ROWS, NZ), F32), jax.ShapeDtypeStruct((3 * tiles, 128), F32)),
        in_specs=[vmem] * 13,
        out_specs=[hbm, hbm],
        scratch_shapes=[
            pltpu.VMEM((SW // OWN, 8, OWN), F32),
            pltpu.VMEM((19, ROWS, NZ), F32),
            pltpu.VMEM((3 * tiles, 128), F32),
            pltpu.SMEM((9, 1, 128), F32),
            pltpu.VMEM((7, ROWS, NZ), F32),
            pltpu.VMEM((3 * ADJ, 2 * NZ), BF16),
            pltpu.VMEM((3 * FAR_ROWS, 2 * NZ), BF16),
            pltpu.VMEM((3, ADJ_ROWS, NZ), F32),
            pltpu.VMEM((GHOST_TILES, 8, 128), F32),
            pltpu.VMEM((3, GHOST_TILES * 128, 128), F32),
            dma((19,)), dma, dma,
        ],
        compiler_params=pltpu.CompilerParams(vmem_limit_bytes=32 << 20),
        name="fluid",
    )(pops, own, base, halo_x, halo_y, halo_c, lists, starts, mom, inner, zhl, plane, own_cols)
    return (moved.reshape(populations.shape), force.reshape(1, 1, 3, SW))


def solution(mesh):
    return jax.shard_map(
        functools.partial(body, mesh.shape["gx"], mesh.shape["gy"]),
        mesh=mesh,
        in_specs=(
            P(None, "gx", "gy", None),
            P("gx", "gy", None),
            P("gx", "gy", None, None),
            P("gx", "gy", None, None),
            P("gx", "gy", None, None),
            P("gx", "gy"),
        ),
        out_specs=(P(None, "gx", "gy", None), P("gx", "gy", None, None)),
        check_vma=False,
    )
```

```python
import functools

import jax
import jax.numpy as jnp
import numpy as np
from jax import lax
from jax.experimental import pallas as pl
from jax.experimental.pallas import tpu as pltpu
from jax.sharding import PartitionSpec as P

DIRS = (
    (0, 0, 0), (1, 0, 0), (-1, 0, 0), (0, 1, 0), (0, -1, 0), (0, 0, 1), (0, 0, -1),
    (1, 1, 0), (-1, -1, 0), (1, -1, 0), (-1, 1, 0), (1, 0, 1), (-1, 0, -1),
    (1, 0, -1), (-1, 0, 1), (0, 1, 1), (0, -1, -1), (0, 1, -1), (0, -1, 1),
)
WEIGHTS = (1.0 / 3.0,) + (1.0 / 18.0,) * 6 + (1.0 / 36.0,) * 12
CUTOFF = 2.0 ** (1.0 / 3.0)
REACH = 1.125
FAR = 1.0e9
F32 = jnp.float32
BF16 = jnp.bfloat16
MESH = pl.DeviceIdType.MESH

CX, CY, NZ, SW = 8, 16, 128, 1024
ROWS = CX * CY
LANE_TILES = SW // 128

SIDES = ((-1, 0), (1, 0), (0, -1), (0, 1), (-1, -1), (-1, 1), (1, -1), (1, 1))
RANGES = ((0, 4, 7), (1, 0, 3), (2, 2, 5), (3, 6, 8), (3, 0, 1), (4, 4, 5), (5, 6, 7), (6, 2, 3), (7, 0, 1))


def facing(axis, sign):
    return [q for q in range(19) if DIRS[q][axis] == sign]


def corner_q(sx, sy):
    return DIRS.index((-sx, -sy, 0))


def split2(v):
    hi = v.astype(BF16)
    return hi, (v - hi.astype(F32)).astype(BF16)


def split3(v):
    hi = v.astype(BF16)
    rest = v - hi.astype(F32)
    mid = rest.astype(BF16)
    return hi, mid, (rest - mid.astype(F32)).astype(BF16)


def dot(a, b):
    return lax.dot_general(a, b, (((1,), (0,)), ((), ())), preferred_element_type=F32)


def dot_t(a, b):
    return lax.dot_general(a, b, (((1,), (1,)), ((), ())), preferred_element_type=F32)


def tent(d):
    return jnp.maximum(1.0 - jnp.abs(d), 0.0)


def moments(load):
    rho = None
    mom = [None, None, None]
    for q in range(19):
        f = load(q)
        rho = f if rho is None else rho + f
        for c in range(3):
            s = DIRS[q][c]
            if s:
                if mom[c] is None:
                    mom[c] = f if s > 0 else -f
                else:
                    mom[c] = mom[c] + f if s > 0 else mom[c] - f
    return rho, mom


def pair_terms(ox, oy, oz, px, py, pz):
    dx = ox - px
    dy = oy - py
    dz = oz - pz
    dz = dz - NZ * jnp.round(dz * (1.0 / NZ))
    raw = dx * dx + dy * dy + dz * dz
    inv = 1.0 / jnp.maximum(raw, 0.8)
    sixth = inv * inv * inv
    mag = (sixth + sixth - 1.0) * (sixth * inv)
    mag = jnp.where(raw < CUTOFF, mag, 0.0)
    return mag * dx, mag * dy, mag * dz


def classes(x, y, live):
    xl, xh = x < REACH, x > CX - 1 - REACH
    yl, yh = y < REACH, y > CY - 1 - REACH
    yc = jnp.where(yl, 0.0, jnp.where(yh, 2.0, 1.0))
    kind = jnp.where(xl, yc, jnp.where(xh, 6.0 - yc, jnp.where(yl, 7.0, jnp.where(yh, 3.0, 8.0))))
    return jnp.where(live > 0.0, kind, 9.0)


def sort_ranks(kind):
    masks = [(kind == k).astype(F32) for k in range(10)]
    ri = lax.broadcasted_iota(jnp.int32, (128, 256), 0)
    ci = lax.broadcasted_iota(jnp.int32, (128, 256), 1)
    upper = ((ri < ci) | (ci >= 128)).astype(F32).astype(BF16)
    pre = dot(jnp.concatenate(masks, axis=0).astype(BF16), upper)
    within, tile_sum = pre[:, :128], pre[:, 128:]
    place = lax.broadcasted_iota(jnp.int32, (80, 128), 0) & 7
    upto = tile_sum
    for by in (1, 2, 4):
        upto = upto + jnp.where(place >= by, pltpu.roll(upto, by, 0), 0.0)
    lane = lax.broadcasted_iota(jnp.int32, (1, 128), 1)
    rank = jnp.zeros((8, 128), F32)
    row = jnp.zeros((1, 128), F32)
    first = jnp.zeros((1, 128), F32)
    for k in range(10):
        cut = slice(8 * k, 8 * k + 8)
        row = jnp.where(lane == k, first, row)
        rank = rank + masks[k] * (within[cut] + (upto[cut] - tile_sum[cut]) + first)
        first = first + upto[8 * k + 7:8 * k + 8]
    return rank, row


def plane_weights(px, py, far):
    x8 = lax.broadcasted_iota(jnp.int32, (CX, 1), 0).astype(F32)
    y16 = lax.broadcasted_iota(jnp.int32, (CY, 1), 0).astype(F32)
    ki = lax.broadcasted_iota(jnp.int32, (16, 1), 0)
    ii, jj = lax.shift_right_logical(ki, 2), ki & 3
    xd = jnp.where(ii < 2, ii - 2, ii + CX - 2).astype(F32)
    yd = jnp.where(jj < 2, jj - 2, jj + CY - 2).astype(F32)
    tx, ty = tent(x8 - px), tent(y16 - py)
    parts = [tx[i:i + 1] * ty for i in range(CX)]
    parts += [tent(-1.0 - px) * ty, tent(CX - px) * ty, tent(-1.0 - py) * tx, tent(CY - py) * tx]
    parts += [tent(xd - px) * tent(yd - py)]
    if far:
        parts += [tent(-2.0 - px) * ty, tent(CX + 1.0 - px) * ty, tent(-2.0 - py) * tx, tent(CY + 1.0 - py) * tx]
    return jnp.concatenate(parts, axis=0)


def z_weights(pz):
    zi = lax.broadcasted_iota(jnp.int32, (NZ, 1), 0).astype(F32)
    return split2(tent(zi - pz))


def widen(v):
    hi, lo = split2(v)
    return jnp.concatenate([hi, lo], axis=1)


def sample(u, zh, zl):
    return dot(u, jnp.concatenate([zh, zh], axis=0)) + dot(u[:, :128], zl)


def columns(cols, at, place):
    turned = jnp.transpose(place)
    for c in range(3):
        cols[c, at:at + 128] = jnp.broadcast_to(turned[:, c:c + 1], (128, 128))


def pair_step(cols, mine, width):
    def step(n, acc):
        at = pl.multiple_of(n * 8, 8)
        p = [jnp.concatenate([cols[c, pl.ds(at, 8)]] * (width // 128), axis=1) for c in range(3)]
        return tuple(a + b for a, b in zip(acc, pair_terms(*mine, *p)))

    return step


def exchange_kernel(n_gx, n_gy, pops_hbm, anchor_hbm, offsets_hbm, heading_hbm, velocity_hbm, count_hbm,
                    pops, halo_x, halo_y, halo_c, lists, starts_out, own_out, base_out, mom, inner, zhl, plane, cols,
                    anchor, offsets, heading, velocity, count, table,
                    msg_x, msg_y, msg_c, msg_l, msg_s, load_sem, send_sem, recv_sem, face_send, face_recv, lower, beside):
    gx = lax.axis_index("gx")
    gy = lax.axis_index("gy")

    def device(side):
        return (lax.rem(gx + side[0] + n_gx, n_gx), lax.rem(gy + side[1] + n_gy, n_gy))

    loads = [pltpu.make_async_copy(a, b, load_sem.at[k]) for k, (a, b) in enumerate((
        (anchor_hbm, anchor), (offsets_hbm, offsets), (heading_hbm, heading), (velocity_hbm, velocity),
        (count_hbm, count)))]
    loads += [pltpu.make_async_copy(pops_hbm.at[pl.ds(q, n)], pops.at[pl.ds(q, n)], load_sem.at[5 + k])
              for k, (q, n) in enumerate(((0, 5), (5, 5), (10, 5), (15, 4)))]
    for c in loads:
        c.start()
    even = lax.rem(gy, 2) == 0
    odd = jnp.logical_not(even)
    barrier = pltpu.get_barrier_semaphore()

    def tell(semaphore, sides):
        for side in sides:
            pl.semaphore_signal(semaphore, inc=1, device_id=device(side), device_id_type=MESH)

    corners_up, along_y, down = ((1, -1), (1, 1)), ((0, -1), (0, 1)), ((-1, -1), (-1, 1), (-1, 0))
    tell(barrier, down)

    @pl.when(even)
    def _():
        tell(barrier, along_y)
        pl.semaphore_wait(barrier, 3)

    @pl.when(odd)
    def _():
        pl.semaphore_wait(barrier, 5)
        tell(beside, along_y)

    tell(lower, ((1, 0),) + corners_up)

    face = []
    for d in range(2):
        for k, q in enumerate(facing(0, 2 * d - 1)):
            face.append(pltpu.make_async_remote_copy(
                src_ref=pops_hbm.at[q, pl.ds(d * (ROWS - CY), CY)], dst_ref=halo_x.at[1 - d, 7 + k],
                send_sem=face_send.at[5 * d + k], recv_sem=face_recv.at[5 * (1 - d) + k],
                device_id=device(SIDES[d]), device_id_type=MESH))
    for c in face[5:]:
        c.start()

    group = max(n_gx // 4, 1)
    head = (lax.rem(gx, group) == 0) & (gx != 0)
    idle = gx >= 0

    @pl.when(head)
    def _():
        pl.semaphore_wait(lower, 3)
        for c in face[:5]:
            c.start()

    for c in loads[:5]:
        c.wait()

    root = anchor[...]
    bxf = lax.shift_right_logical(root, 7).astype(F32)
    cxf = jnp.floor(bxf * (1.0 / (CY + 2)) + 0.01)
    x = cxf - 1.0 + offsets[0:8]
    y = bxf - cxf * (CY + 2) - 1.0 + offsets[8:16]
    z = (root & (NZ - 1)).astype(F32) + offsets[16:24]
    lane = lax.broadcasted_iota(jnp.int32, (8, 128), 1)
    sub = lax.broadcasted_iota(jnp.int32, (8, 128), 0)
    live = (sub * 128 + lane < count[0]).astype(F32)
    first, second = heading[pl.ds(0, 8, stride=2)], heading[pl.ds(1, 8, stride=2)]
    c1 = jnp.cos(second)
    w = [2.0 * velocity[0:8] - 0.5 * (jnp.cos(first) * c1),
         2.0 * velocity[8:16] - 0.5 * (jnp.sin(first) * c1),
         2.0 * velocity[16:24] - 0.5 * jnp.sin(second)]
    for k, v in enumerate((x, y, z, *w, live, jnp.zeros((8, 128), F32))):
        table[pl.ds(k, 8, stride=8)] = v
    rank, row = sort_ranks(classes(x, y, live))
    msg_s[...] = row
    starts_out[8] = jnp.where(lane[0:1] == 10, idle.astype(F32), row)
    to_tile = jnp.floor(rank * (1.0 / 128.0))
    to_lane = rank - 128.0 * to_tile
    split = [v.astype(F32) for v in split3(table[...])]
    dst = lax.broadcasted_iota(jnp.int32, (128, 128), 0).astype(F32)
    ordered = jnp.zeros((24 * LANE_TILES, 128), F32)
    for t in range(0, LANE_TILES, 2):
        hot, rows = [], []
        for j in (t, t + 1):
            hot.append((dst == to_lane[j:j + 1]).astype(F32).astype(BF16))
            part = jnp.concatenate([v[8 * j:8 * j + 8] for v in split], axis=0)
            rows.append(jnp.concatenate(
                [jnp.where(to_tile[j:j + 1] == float(k), part, 0.0) for k in range(LANE_TILES)],
                axis=0).astype(BF16))
        ordered = ordered + dot_t(jnp.concatenate(rows, axis=1), jnp.concatenate(hot, axis=1))
    for t in range(LANE_TILES):
        at = 24 * t
        msg_l[t] = ordered[at:at + 8] + ordered[at + 8:at + 16] + ordered[at + 16:at + 24]

    def send(k, a, b, side, o):
        d = SIDES.index(side)
        return pltpu.make_async_remote_copy(
            src_ref=a, dst_ref=b, send_sem=send_sem.at[3 * d + k], recv_sem=recv_sem.at[3 * o + k],
            device_id=device(side), device_id_type=MESH)

    copies = {}
    for d, side in enumerate(SIDES):
        o = SIDES.index((-side[0], -side[1]))
        if side[1] == 0:
            first = send(0, msg_x.at[d], halo_x.at[o, pl.ds(0, 7)], side, o)
        elif side[0] == 0:
            first = send(0, msg_y.at[d - 2], halo_y.at[o - 2], side, o)
        else:
            first = send(0, msg_c.at[d - 4], halo_c.at[o - 4], side, o)
        copies[side] = (first, send(1, msg_s, starts_out.at[o], side, o),
                        send(2, msg_l.at[:, pl.ds(0, 6)], lists.at[o, :, pl.ds(0, 6)], side, o))

    def start(sides, kinds=(0, 1, 2)):
        for k in kinds:
            for side in sides:
                copies[side][k].start()

    last = gx == n_gx - 1
    late = gx >= n_gx - max(n_gx // 4, 1)

    @pl.when(last)
    def _():
        start(corners_up, (1, 2))

    @pl.when(head)
    def _():
        start(down, (1, 2))

    start(((1, 0),), (1, 2))

    for c in loads[5:]:
        c.wait()
    rho, m = moments(lambda q: pops[q])
    inv = 1.0 / rho
    mom[0] = rho
    for c in range(3):
        mom[1 + c] = m[c] * inv
    for s, (adj, far) in enumerate(((0, 1), (CX - 1, CX - 2))):
        for c in range(4):
            msg_x[s, c] = mom[c, adj * CY:(adj + 1) * CY]
        for c in range(3):
            msg_x[s, 4 + c] = mom[1 + c, far * CY:(far + 1) * CY]

    for i in range(4):
        sx, sy = SIDES[4 + i]
        ax, fx = (0, 1) if sx < 0 else (CX - 1, CX - 2)
        ay, fy = (0, 1) if sy < 0 else (CY - 1, CY - 2)
        msg_c[i] = jnp.zeros((16, 128), F32)
        for c in range(4):
            msg_c[i, c:c + 1] = mom[c, ax * CY + ay:ax * CY + ay + 1]
        for j, (nx, ny) in enumerate(((ax, fy), (fx, ay), (fx, fy))):
            for c in range(3):
                msg_c[i, 5 + 3 * j + c:6 + 3 * j + c] = mom[1 + c, nx * CY + ny:nx * CY + ny + 1]
        q = DIRS.index((sx, sy, 0))
        msg_c[i, 4:5] = pops[q, ax * CY + ay:ax * CY + ay + 1]


    @pl.when(last)
    def _():
        start(corners_up, (0,))

    @pl.when(head)
    def _():
        start(down, (0,))

    start(((1, 0),), (0,))
    for s, (adj, far) in enumerate(((0, 1), (CY - 1, CY - 2))):
        for c in range(4):
            msg_y[s, c] = mom[c, pl.ds(adj, CX, stride=CY)]
        for c in range(3):
            msg_y[s, 4 + c] = mom[1 + c, pl.ds(far, CX, stride=CY)]
        for k, q in enumerate(facing(1, 2 * s - 1)):
            msg_y[s, 7 + k] = pops[q, pl.ds(adj, CX, stride=CY)]
    def own_pairs():
        for i in range(0, SW // OWN, 2):
            width = 2 * OWN
            mine = [jnp.broadcast_to(jnp.concatenate([own_out[i, c:c + 1], own_out[i + 1, c:c + 1]], axis=1), (8, width))
                    for c in range(3)]
            init = tuple(jnp.zeros((8, width), F32) for _ in range(3))
            got = lax.fori_loop(0, SW // 8, pair_step(cols, mine, width), init)
            for c in range(3):
                pairs = 0.24 * jnp.sum(got[c], axis=0, keepdims=True)
                for j in range(2):
                    base_out[i + j, c:c + 1] = (base_out[i + j, c:c + 1]
                                                + pairs[:, j * OWN:(j + 1) * OWN] * own_out[i + j, 6:7])

    def send_down():
        pl.semaphore_wait(lower, 3)
        for c in face[:5]:
            c.start()
        start(down)

    def send_along():
        @pl.when(even)
        def _():
            pl.semaphore_wait(beside, 2)

        start(along_y)

    @pl.when(jnp.logical_not(late))
    def _():
        send_along()
        start(corners_up)

    @pl.when(jnp.logical_not(late | head) & (gx != 0))
    def _():
        send_down()

    for c in range(3):
        inner[c * ROWS:(c + 1) * ROWS] = widen(mom[1 + c])
    for i in range(BLOCKS):
        n = BLOCK // 128
        vals = jnp.concatenate([table[8 * (n * i + j):8 * (n * i + j) + 8] for j in range(n)], axis=1)
        zh, zl = z_weights(vals[2:3])
        zhl[i, 0:NZ] = zh
        zhl[i, NZ:2 * NZ] = zl
        plane[i] = plane_weights(vals[0:1], vals[1:2], False)
        got = sample(inner[...], zh, zl)
        rows = [vals[0:3]]
        for c in range(3):
            s = jnp.sum(got[c * ROWS:(c + 1) * ROWS] * plane[i, 0:ROWS], axis=0, keepdims=True)
            rows.append((vals[3 + c:4 + c] - 2.0 * s) * vals[6:7])
        rows = jnp.concatenate(rows + [vals[6:8]], axis=0)
        for j in range(BLOCK // OWN):
            own_out[i * (BLOCK // OWN) + j] = rows[:, j * OWN:(j + 1) * OWN]

    @pl.when(late)
    def _():
        send_along()

    @pl.when(late & jnp.logical_not(last))
    def _():
        start(corners_up)

    @pl.when(late & jnp.logical_not(head))
    def _():
        send_down()

    for t in range(LANE_TILES):
        v = table[8 * t:8 * t + 8]
        columns(cols, t * 128, jnp.where((sub == 0) & (v[6:7] == 0.0), FAR, v))
    for i in range(SW // OWN):
        base_out[i] = jnp.concatenate([-own_out[i, 3:6], jnp.zeros((5, OWN), F32)], axis=0)

    @pl.when(idle)
    def _():
        own_pairs()

    @pl.when(gx == 0)
    def _():
        send_down()

    for c in face:
        c.wait()
    for side in SIDES:
        for c in copies[side]:
            c.wait()


ADJ = 64
FAR_ROWS = 48
ADJ_ROWS = ROWS + ADJ
BLOCK = 512
BLOCKS = SW // BLOCK
OWN = 256
GHOSTS = 384
GHOST_TILES = 8 * LANE_TILES + 4


def fluid_kernel(pops, own, base, halo_x, halo_y, halo_c, lists, starts_in, mom, inner, zhl, plane, own_cols,
                 next_out, force_out,
                 acc, out_v, force_v, starts, node, near, outer, force, ghosts, cols, out_sem, start_sem, force_sem):
    start_copy = pltpu.make_async_copy(starts_in, starts, start_sem)
    start_copy.start()
    acc[...] = base[...]
    ghosts[...] = jnp.zeros(ghosts.shape, F32)
    force[...] = jnp.zeros(force.shape, F32)
    for c in range(3):
        corner = []
        for i in range(4):
            for j in range(4):
                sx, sy = (0 if i < 2 else 1), (0 if j < 2 else 1)
                fx, fy = i in (0, 3), j in (0, 3)
                k = 2 * sx + sy
                r = (11 if fy else 8) if fx else (5 if fy else 1)
                corner.append(halo_c[k, r + c:r + c + 1])
        near[c * ADJ:(c + 1) * ADJ] = widen(jnp.concatenate(
            [halo_x[0, 1 + c], halo_x[1, 1 + c], halo_y[0, 1 + c], halo_y[1, 1 + c]] + corner, axis=0))
        outer[c * FAR_ROWS:(c + 1) * FAR_ROWS] = widen(jnp.concatenate(
            [halo_x[0, 4 + c], halo_x[1, 4 + c], halo_y[0, 4 + c], halo_y[1, 4 + c]], axis=0))

    def spread(weights, react, zz):
        zh = zz[0:NZ]
        for c in range(3):
            wh, wl = split2(weights * react[c])
            both = dot_t(wh, zz)
            force[c] = force[c] + (both[:, :128] + both[:, 128:] + dot_t(wl, zh))

    per = BLOCK // OWN

    def own_block(i, carry):
        zz = zhl[i]
        got = sample(near[...], zz[0:NZ], zz[NZ:2 * NZ])
        vals = jnp.concatenate([own[per * i + j] for j in range(per)], axis=1)
        react = []
        for c in range(3):
            s = jnp.sum(got[c * ADJ:(c + 1) * ADJ] * plane[i, ROWS:ADJ_ROWS], axis=0, keepdims=True)
            s = 2.0 * s * vals[6:7]
            react.append(vals[3 + c:4 + c] - s)
            for j in range(per):
                acc[per * i + j, c:c + 1] = acc[per * i + j, c:c + 1] + s[:, j * OWN:(j + 1) * OWN]
        spread(plane[i], react, zz)
        return carry

    own_block(0, 0)
    start_copy.wait()
    n_own = starts[8, 0, 9].astype(jnp.int32)

    lane = lax.broadcasted_iota(jnp.int32, (8, 128), 1)
    sub = lax.broadcasted_iota(jnp.int32, (8, 128), 0)
    total = jnp.int32(0)
    puts, rest = [], []
    for d, lo, hi in RANGES:
        a = starts[d, 0, lo].astype(jnp.int32)
        b = starts[d, 0, hi].astype(jnp.int32)
        sx, sy = SIDES[d]
        moved = jnp.where(sub == 0, float(sx * CX), jnp.where(sub == 1, float(sy * CY), 0.0))
        by = (total - a) & 127
        upper = lane >= by

        def taken(t, d=d, a=a, b=b, by=by, moved=moved):
            at = t * 128 + lane
            v = jnp.where((at >= a) & (at < b), lists[d, jnp.minimum(t, LANE_TILES - 1)] + moved, 0.0)
            return pltpu.roll(v, by, 1)

        t0 = lax.shift_right_logical(a, 7)
        tile = lax.shift_right_logical(total - a + t0 * 128 + 1024, 7) - 8
        v0, v1 = taken(t0), taken(t0 + 1)
        puts.append((jnp.maximum(tile, 0), jnp.where(upper, v0, 0.0)))
        puts.append((tile + 1, jnp.where(upper, v1, v0)))
        puts.append((tile + 2, jnp.where(upper, 0.0, v1)))

        def more(t, carry, taken=taken, upper=upper, shift=tile - t0):
            v = taken(t)
            ghosts[t + shift] = ghosts[t + shift] + jnp.where(upper, v, 0.0)
            ghosts[t + shift + 1] = ghosts[t + shift + 1] + jnp.where(upper, 0.0, v)
            return carry

        rest.append((t0 + 2, lax.shift_right_logical(b + 127, 7), more))
        total = total + (b - a)
    for at, v in puts:
        ghosts[at] = ghosts[at] + v
    for lo, hi, more in rest:
        lax.fori_loop(lo, hi, more, 0)

    slot = lax.broadcasted_iota(jnp.int32, (1, GHOSTS), 1)
    tiles = lax.shift_right_logical(total + 127, 7)
    ahead = GHOSTS // 128

    def ghost_columns(t, carry):
        g = jnp.where((sub == 0) & (lane + t * 128 >= total), FAR, ghosts[t])
        turned = jnp.transpose(g)
        at = t * 128 if isinstance(t, int) else pl.multiple_of(t * 128, 128)
        for c in range(3):
            cols[c, pl.ds(at, 128)] = jnp.broadcast_to(turned[:, c:c + 1], (128, 128))
        return carry

    def ghost_block(i, carry):
        vals = jnp.concatenate([ghosts[ahead * i + j] for j in range(ahead)], axis=1)
        live = (slot + i * GHOSTS < total).astype(F32)
        zh, zl = z_weights(vals[2:3])
        weights = plane_weights(vals[0:1], vals[1:2], True)
        gi = sample(inner[...], zh, zl)
        gn = sample(near[...], zh, zl)
        gf = sample(outer[...], zh, zl)
        react = []
        for c in range(3):
            s = (jnp.sum(gi[c * ROWS:(c + 1) * ROWS] * weights[0:ROWS], axis=0, keepdims=True)
                 + jnp.sum(gn[c * ADJ:(c + 1) * ADJ] * weights[ROWS:ADJ_ROWS], axis=0, keepdims=True)
                 + jnp.sum(gf[c * FAR_ROWS:(c + 1) * FAR_ROWS] * weights[ADJ_ROWS:], axis=0, keepdims=True))
            react.append((vals[3 + c:4 + c] - 2.0 * s) * live)
        spread(weights[0:ADJ_ROWS], react, jnp.concatenate([zh, zl], axis=0))
        return carry

    for t in range(ahead):
        ghost_columns(t, 0)
    ghost_block(0, 0)
    lax.fori_loop(ahead, tiles, ghost_columns, 0)
    lax.fori_loop(1, lax.div(total + GHOSTS - 1, GHOSTS), ghost_block, 0)
    lax.fori_loop(1, lax.shift_right_logical(n_own + BLOCK - 1, 9), own_block, 0)

    own_left = jnp.where(starts[8, 0, 10] > 0.5, 0, n_own)

    def ghost_pairs(i, carry):
        mine = [jnp.broadcast_to(own[i, c:c + 1], (8, OWN)) for c in range(3)]
        got = tuple(jnp.zeros((8, OWN), F32) for _ in range(3))
        for source, n in ((own_cols, own_left), (cols, total)):
            one = pair_step(source, mine, OWN)

            def four(n, got, one=one):
                for k in range(4):
                    got = one(4 * n + k, got)
                return got

            got = lax.fori_loop(0, lax.shift_right_logical(n + 31, 5), four, got)
        live = own[i, 6:7]
        for c in range(3):
            acc[i, c:c + 1] = acc[i, c:c + 1] + 0.24 * live * jnp.sum(got[c], axis=0, keepdims=True)
        return carry

    lax.fori_loop(0, lax.shift_right_logical(n_own + OWN - 1, 8), ghost_pairs, 0)
    for i in range(SW // OWN):
        for c in range(3):
            for j in range(2):
                r = c * LANE_TILES + 2 * i + j
                force_v[r:r + 1] = acc[i, c:c + 1, j * 128:(j + 1) * 128]
    force_copy = pltpu.make_async_copy(force_v, force_out, force_sem)
    force_copy.start()

    def prepare(rho, u0, half, g):
        u = [u0[c] + half * g[c] for c in range(3)]
        uu = u[0] * u[0] + u[1] * u[1] + u[2] * u[2]
        ug = u[0] * g[0] + u[1] * g[1] + u[2] * g[2]
        k0 = 1.25 * rho * (1.0 - 1.5 * uu) - 1.125 * ug
        return k0, 3.75 * rho, 5.625 * rho, u, [1.125 * v for v in g]

    def along(q, v):
        out = None
        for c in range(3):
            s = DIRS[q][c]
            if s:
                out = (v[c] if s > 0 else -v[c]) if out is None else (out + v[c] if s > 0 else out - v[c])
        return out

    def post(q, f, prep):
        k0, r1, r2, u, g = prep
        if q == 0:
            return -0.25 * f + WEIGHTS[0] * k0
        a, p = along(q, u), along(q, g)
        return -0.25 * f + WEIGHTS[q] * (k0 + a * (r1 + r2 * a + 3.0 * p) + p)

    def side_prep(rho, u0, lo, n):
        g = [force[c, lo:lo + n] for c in range(3)]
        return prepare(rho, u0, 0.5 / rho, g)

    k0, r1, r2, u, g = side_prep(mom[0], [mom[1 + c] for c in range(3)], 0, ROWS)
    node[0] = k0
    for c in range(3):
        node[1 + c] = u[c]
        node[4 + c] = g[c]
    xs = [side_prep(halo_x[s, 0], [halo_x[s, 1 + c] for c in range(3)], ROWS + s * CY, CY) for s in range(2)]
    ys = [side_prep(halo_y[s, 0], [halo_y[s, 1 + c] for c in range(3)], ROWS + 2 * CY + s * CX, CX)
          for s in range(2)]
    cs = []
    for i in range(4):
        sx, sy = SIDES[4 + i]
        r = ADJ_ROWS - 16 + (1 if sx < 0 else 2) * 4 + (1 if sy < 0 else 2)
        cs.append(side_prep(halo_c[i, 0:1], [halo_c[i, 1 + c:2 + c] for c in range(3)], r, 1))
    stores = []
    for q in range(19):
        dx, dy, dz = DIRS[q]
        rho_q = mom[0]
        prep = (node[0], 3.75 * rho_q, 5.625 * rho_q, [node[1 + c] for c in range(3)], [node[4 + c] for c in range(3)])

        def turned(v, dz=dz):
            return pltpu.roll(v, dz % NZ, 1) if dz else v

        v = turned(post(q, pops[q], prep))
        if dy:
            v = pltpu.roll(v, dy % ROWS, 0)
        if dx == 0:
            out_v[q] = v
        else:
            s = 0 if dx > 0 else 1
            e = turned(post(q, halo_x[s, 7 + facing(0, dx).index(q)], xs[s]))
            if dy:
                e = pltpu.roll(e, dy % CY, 0)
            if dx > 0:
                out_v[q, CY:ROWS] = v[0:ROWS - CY]
                out_v[q, 0:CY] = e
            else:
                out_v[q, 0:ROWS - CY] = v[CY:ROWS]
                out_v[q, ROWS - CY:ROWS] = e
        if dy:
            s = 0 if dy > 0 else 1
            at = 0 if dy > 0 else CY - 1
            e = turned(post(q, halo_y[s, 7 + facing(1, dy).index(q)], ys[s]))
            if dx:
                e = pltpu.roll(e, dx % CX, 0)
            out_v[q, pl.ds(at, CX, stride=CY)] = e
            if dx:
                i = SIDES.index((-dx, -dy)) - 4
                r = at + (0 if dx > 0 else (CX - 1) * CY)
                out_v[q, r:r + 1] = post(q, halo_c[i, 4:5], cs[i])
        c = pltpu.make_async_copy(out_v.at[q], next_out.at[q], out_sem.at[q])
        c.start()
        stores.append(c)
    force_copy.wait()
    for c in stores:
        c.wait()


def body(n_gx, n_gy, populations, anchor, offsets, heading, velocity, live_count):
    pops = populations.reshape(19, ROWS, NZ)
    tiles = LANE_TILES
    vmem = pl.BlockSpec(memory_space=pltpu.VMEM)
    hbm = pl.BlockSpec(memory_space=pltpu.HBM)
    dma = pltpu.SemaphoreType.DMA
    held = (
        pltpu.VMEM((19, ROWS, NZ), F32),
        pltpu.VMEM((2, 12, CY, 128), F32),
        pltpu.VMEM((2, 12, CX, 128), F32),
        pltpu.VMEM((4, 16, 128), F32),
        pltpu.VMEM((8, LANE_TILES, 8, 128), F32),
        pltpu.VMEM((9, 1, 128), F32),
        pltpu.VMEM((SW // OWN, 8, OWN), F32),
        pltpu.VMEM((SW // OWN, 8, OWN), F32),
        pltpu.VMEM((4, ROWS, NZ), F32),
        pltpu.VMEM((3 * ROWS, 2 * NZ), BF16),
        pltpu.VMEM((BLOCKS, 2 * NZ, BLOCK), BF16),
        pltpu.VMEM((BLOCKS, ADJ_ROWS, BLOCK), F32),
        pltpu.VMEM((3, SW, 128), F32),
    )
    pops, halo_x, halo_y, halo_c, lists, starts, own, base, mom, inner, zhl, plane, own_cols = pl.pallas_call(
        functools.partial(exchange_kernel, n_gx, n_gy),
        out_shape=held,
        in_specs=[hbm] * 6,
        out_specs=[vmem] * 13,
        scratch_shapes=[
            pltpu.VMEM((tiles, 128), jnp.int32),
            pltpu.VMEM((3 * tiles, 128), F32),
            pltpu.VMEM((2 * tiles, 128), F32),
            pltpu.VMEM((3 * tiles, 128), F32),
            pltpu.SMEM((1,), jnp.int32),
            pltpu.VMEM((8 * tiles, 128), F32),
            pltpu.VMEM((2, 7, CY, 128), F32),
            pltpu.VMEM((2, 12, CX, 128), F32),
            pltpu.VMEM((4, 16, 128), F32),
            pltpu.VMEM((LANE_TILES, 8, 128), F32),
            pltpu.VMEM((1, 128), F32),
            dma((9,)), dma((24,)), dma((24,)), dma((10,)), dma((10,)),
            pltpu.SemaphoreType.REGULAR, pltpu.SemaphoreType.REGULAR,
        ],
        compiler_params=pltpu.CompilerParams(collective_id=0, has_side_effects=True, vmem_limit_bytes=20 << 20),
        name="exchange",
    )(*[pltpu.with_memory_space_constraint(v, pltpu.HBM) for v in (
        pops, anchor.reshape(tiles, 128), offsets.reshape(3 * tiles, 128),
        jnp.swapaxes(heading.reshape(2, tiles, 128), 0, 1).reshape(2 * tiles, 128),
        velocity.reshape(3 * tiles, 128))], live_count.reshape(1))
    moved, force = pl.pallas_call(
        fluid_kernel,
        out_shape=(jax.ShapeDtypeStruct((19, ROWS, NZ), F32), jax.ShapeDtypeStruct((3 * tiles, 128), F32)),
        in_specs=[vmem] * 13,
        out_specs=[hbm, hbm],
        scratch_shapes=[
            pltpu.VMEM((SW // OWN, 8, OWN), F32),
            pltpu.VMEM((19, ROWS, NZ), F32),
            pltpu.VMEM((3 * tiles, 128), F32),
            pltpu.SMEM((9, 1, 128), F32),
            pltpu.VMEM((7, ROWS, NZ), F32),
            pltpu.VMEM((3 * ADJ, 2 * NZ), BF16),
            pltpu.VMEM((3 * FAR_ROWS, 2 * NZ), BF16),
            pltpu.VMEM((3, ADJ_ROWS, NZ), F32),
            pltpu.VMEM((GHOST_TILES, 8, 128), F32),
            pltpu.VMEM((3, GHOST_TILES * 128, 128), F32),
            dma((19,)), dma, dma,
        ],
        compiler_params=pltpu.CompilerParams(vmem_limit_bytes=32 << 20),
        name="fluid",
    )(pops, own, base, halo_x, halo_y, halo_c, lists, starts, mom, inner, zhl, plane, own_cols)
    return (moved.reshape(populations.shape), force.reshape(1, 1, 3, SW))


def solution(mesh):
    return jax.shard_map(
        functools.partial(body, mesh.shape["gx"], mesh.shape["gy"]),
        mesh=mesh,
        in_specs=(
            P(None, "gx", "gy", None),
            P("gx", "gy", None),
            P("gx", "gy", None, None),
            P("gx", "gy", None, None),
            P("gx", "gy", None, None),
            P("gx", "gy"),
        ),
        out_specs=(P(None, "gx", "gy", None), P("gx", "gy", None, None)),
        check_vma=False,
    )
```
